32 devices in a mesh: expert: 8 (over z, y), tensor: 4 (over x, core).
Axes of the slice: x: 2, y: 2, z: 4, core: 2. Of those that a mesh axis runs over, the one named last changes fastest.
Arguments:
- tokens: bfloat16 [2048, 2048], P('expert'), may hold values from -6 to 6
- seq_length: int32 [8], P('expert'), may hold values from 256 to 256, as said below
- expert_routes: int32 [2048, 8], P('expert'), may hold values from 0 to 15, all different within a row; in each aligned block of 256 rows (0 to 255, 256 to 511, ...) at most 160 rows name the same one
- attention_gain: float32 [2048], replicated, may hold values from 0.5 to 1.5
- query_weight: bfloat16 [2048, 4096], P(None, 'tensor'), may hold values from -0.125 to 0.125
- key_weight: bfloat16 [2048, 512], P(None, 'tensor'), may hold values from -0.125 to 0.125
- value_weight: bfloat16 [2048, 512], P(None, 'tensor'), may hold values from -0.125 to 0.125
- query_gain: float32 [128], replicated, may hold values from 0.5 to 1.5
- key_gain: float32 [128], replicated, may hold values from 0.5 to 1.5
- output_weight: bfloat16 [2048, 4096], P(None, 'tensor'), may hold values from -0.5 to 0.5
- routing_gain: float32 [2048], replicated, may hold values from 0.5 to 1.5
- router_weight: bfloat16 [2048, 16], replicated, may hold values from -0.26367188 to 0.26367188
- gate_weight: bfloat16 [16, 2048, 768], P('expert', None, 'tensor'), may hold values from -0.125 to 0.125
- up_weight: bfloat16 [16, 2048, 768], P('expert', None, 'tensor'), may hold values from -0.125 to 0.125
- down_weight: bfloat16 [16, 768, 2048], P('expert', 'tensor'), may hold values from -0.625 to 0.625
- cotangent: bfloat16 [2048, 2048], P('expert'), may hold values from -6 to 6
Outputs:
- mixed: bfloat16 [2048, 2048], P('expert')
- tokens_grad: bfloat16 [2048, 2048], P('expert')
- attention_gain_grad: float32 [2048], P('expert')
- query_weight_grad: float32 [2048, 4096], P('expert', 'tensor')
- key_weight_grad: float32 [2048, 512], P('expert', 'tensor')
- value_weight_grad: float32 [2048, 512], P('expert', 'tensor')
- query_gain_grad: float32 [128], P('expert')
- key_gain_grad: float32 [128], P('expert')
- output_weight_grad: float32 [2048, 4096], P('expert', 'tensor')
- routing_gain_grad: float32 [2048], P('expert')
- router_weight_grad: float32 [2048, 16], P('expert')
- gate_weight_grad: float32 [16, 2048, 768], P('expert', None, 'tensor')
- up_weight_grad: float32 [16, 2048, 768], P('expert', None, 'tensor')
- down_weight_grad: float32 [16, 768, 2048], P('expert', 'tensor')
The draws below stay inside these ranges and needn't reach their ends.
Inputs may be any that keep to these rules, and one draw needn't show every extreme that they name: `seq_length`: each group holds one sequence starting at its first row; some group's sequence fills all 256 rows. `expert_routes`: each row names 8 different experts; within the rows of one group no expert is named more than 160 times.
All inputs are finite; a program needn't handle non-finite values.
Results may differ from the reference program's by a relative error of at most 0.025.
Values may be sent and summed in bfloat16 or wider, within the bound.
A program may use at most 192 MiB of HBM per device.

```python
import math
import jax
import jax.numpy as jnp
import numpy as np
from jax import lax

D = 2048
HEADS = 32
KV_HEADS = 4
HD = 128
FF_E = 768
TOP = 8
TOK_DEV = 256
MIN_LEN = 256
GROUPS = 8
TOKENS = 2048
EXPERTS = 16
CAP = 160


def draw_seq_length(key, part):
    first, second = jax.random.split(key)
    drawn = jax.random.randint(first, (GROUPS,), MIN_LEN, TOK_DEV + 1)
    longest = jax.random.randint(second, (), 0, GROUPS)
    return jnp.where(jnp.arange(GROUPS) == longest, TOK_DEV, drawn).astype(jnp.int32)


def spiked(array, stream_key, source, target, blocks, factor):
    owner, partner = [(jnp.arange(array.shape[dim]) // (array.shape[dim] // blocks)).reshape([-1 if axis == dim else 1 for axis in range(array.ndim)]) for dim in (source, target)]
    chosen = jax.random.permutation(stream_key, blocks)[partner]
    strong = (owner == chosen) | (owner == (partner + blocks // 2) % blocks)
    return jnp.where(strong, factor * array, array)


def shard_levels(stream_key, shape, pieces, least, high):
    gain = 1.0
    for axis_at, blocks in pieces:
        draws = jax.random.uniform(jax.random.fold_in(jax.random.fold_in(stream_key, 6), axis_at), (blocks,), jnp.float32, least / len(pieces), high / len(pieces))
        gain = gain * jnp.repeat(jnp.exp(draws), shape[axis_at] // blocks).reshape((-1,) + (1,) * (len(shape) - 1 - axis_at))
    return gain


def shared_out(key, own, number, rows, count, top, limit, lean):
    order = jax.random.permutation(key, count)
    crowded, common = shares(count, rows * top, limit, lean, True), shares(count, rows * top, limit, lean, False)
    places = jnp.arange(count)

    def named(lengths, turn):
        used = int((lengths > 0).sum())
        fixed = max(1, used // 4)
        passed = fixed + (places - fixed + turn * (used - fixed)) % max(1, count - fixed)
        return jnp.zeros((count,), jnp.int32).at[order[jnp.where(places < fixed, places, passed)]].set(jnp.asarray(lengths, jnp.int32))

    lengths = jnp.where(number % 4 == 0, named(crowded, number // 4), named(common, number - number // 4 - 1))
    mixed = jax.random.permutation(jax.random.fold_in(own, 3), count)
    source_of, taker = mixed[0:count // 2 * 2:2], mixed[1:count // 2 * 2:2]
    room = jnp.minimum(lengths[source_of] - 1, limit - lengths[taker]) // 2
    room = jnp.where((source_of == order[0]) | (taker == order[0]) | (lengths[taker] == 0), 0, jnp.maximum(room, 0))
    passed = jax.random.randint(jax.random.fold_in(own, 4), (count // 2,), 0, 1 << 20) % (room + 1)
    lengths = lengths.at[source_of].add(-passed).at[taker].add(passed)
    labels = jnp.searchsorted(jnp.cumsum(lengths), jnp.arange(rows * top), side="right").astype(jnp.int32)
    grid = labels.reshape(top, rows).T
    grid = grid[jax.random.permutation(jax.random.fold_in(own, 1), rows)]
    turn = jax.random.randint(jax.random.fold_in(own, 2), (rows, 1), 0, top)
    return jnp.take_along_axis(grid, (jnp.arange(top)[None, :] + turn) % top, axis=1)


def shares(amount, total, most, skew, full):
    weights = [(1 << 20) // math.isqrt(rank ** skew) + 1 for rank in range(1, amount + 1)]
    largest = most if full else min(most, max(-(-total // amount), total * weights[0] // sum(weights)))
    least = 1 if total - largest >= amount - 1 else 0
    counts, spare = [largest] + [least] * (amount - 1), total - largest - least * (amount - 1)
    while spare > 0:
        candidates = [i for i in range(1, amount) if counts[i] < largest] or [i for i in range(1, amount) if counts[i] < most]
        pool, budget = sum([weights[i] for i in candidates]), spare
        for i in candidates:
            extra = min(most - counts[i], max(1, budget * weights[i] // pool), spare)
            counts[i] = counts[i] + extra
            spare = spare - extra
    return np.array(counts)


def scatter_about(stream_key, dims, scale, reach, shards=(), held_as=jnp.bfloat16):
    factor_of = shard_levels(stream_key, dims, shards, -0.22, 0.18) if shards else 1.0
    entries = jax.random.normal(stream_key, dims, jnp.float32) * scale * factor_of
    return jnp.minimum(jnp.maximum(entries, -reach), reach).astype(held_as)


def heavy_noise(rng, shape, spread, reach, cuts, heavy, held_as=jnp.bfloat16):
    values = spread * jax.random.normal(rng, shape, jnp.float32)
    if cuts:
        values = values * shard_levels(rng, shape, cuts, -0.22, 0.18)
    return jnp.clip(spiked(values, jax.random.fold_in(rng, 3), *heavy), -reach, reach).astype(held_as)


def setup_inputs(seed: int = 0) -> dict:
    splits = jax.random.split(jax.random.key(seed), 17)
    tokens = heavy_noise(splits[0], (TOKENS, D), 1.0, 6.0, ((0, 8),), (0, 1, 8, 2.0))
    seq_length = draw_seq_length(jax.random.fold_in(splits[16], 71), 0)
    expert_routes_keys = jax.random.split(jax.random.fold_in(splits[2], 1), TOKENS // TOK_DEV)
    expert_routes_turns = jax.random.permutation(jax.random.fold_in(splits[2], 3), TOKENS // TOK_DEV)
    expert_routes = jax.vmap(lambda own, number: shared_out(jax.random.fold_in(splits[2], 2), own, number, TOK_DEV, EXPERTS, TOP, CAP, 1))(expert_routes_keys, expert_routes_turns).reshape((TOKENS, TOP))
    attention_gain = jnp.clip(1.0 + 0.1 * jax.random.normal(splits[3], (D,), jnp.float32), 0.5, 1.5)
    query_weight = scatter_about(splits[4], (D, HEADS * HD), D ** -0.5, 0.125, ((1, 4),))
    key_weight = scatter_about(splits[5], (D, KV_HEADS * HD), D ** -0.5, 0.125, ((1, 4),))
    value_weight = scatter_about(splits[6], (D, KV_HEADS * HD), D ** -0.5, 0.125, ((1, 4),))
    query_gain = jnp.clip(1.0 + 0.1 * jax.random.normal(splits[7], (HD,), jnp.float32), 0.5, 1.5)
    key_gain = jnp.clip(1.0 + 0.1 * jax.random.normal(splits[8], (HD,), jnp.float32), 0.5, 1.5)
    output_weight = scatter_about(splits[9], (D, HEADS * HD), (HEADS * HD // 32) ** -0.5, 0.5, ((1, 4),))
    routing_gain = jnp.clip(1.0 + 0.1 * jax.random.normal(splits[10], (D,), jnp.float32), 0.5, 1.5)
    router_weight = scatter_about(splits[11], (D, EXPERTS), (2.0 / D ** 0.5), 0.26367188)
    gate_weight = scatter_about(splits[12], (EXPERTS, D, FF_E), D ** -0.5, 0.125, ((0, 8), (2, 4)))
    up_weight = scatter_about(splits[13], (EXPERTS, D, FF_E), D ** -0.5, 0.125, ((0, 8), (2, 4)))
    down_weight = scatter_about(splits[14], (EXPERTS, FF_E, D), (FF_E // 8) ** -0.5, 0.625, ((0, 8), (1, 4)))
    cotangent = heavy_noise(splits[15], (TOKENS, D), 1.0, 6.0, ((0, 8),), (0, 1, 8, 2.0))
    return dict(tokens=tokens, seq_length=seq_length, expert_routes=expert_routes, attention_gain=attention_gain, query_weight=query_weight, key_weight=key_weight, value_weight=value_weight, query_gain=query_gain, key_gain=key_gain, output_weight=output_weight, routing_gain=routing_gain, router_weight=router_weight, gate_weight=gate_weight, up_weight=up_weight, down_weight=down_weight, cotangent=cotangent)


EPSILON = 1e-06
THETA = 1000000.0
NEGATIVE = -1e+30

@jax.custom_vjp
def low(v):
    return lax.optimization_barrier(v.astype(jnp.bfloat16)).astype(jnp.float32)

@jax.custom_vjp
def low_back(v):
    return v

def low_keep(v):
    return (low(v), None)

def low_pass(kept, grad):
    return (grad,)

def back_keep(v):
    return (v, None)

def back_low(kept, grad):
    return (low(grad),)
low.defvjp(low_keep, low_pass)
low_back.defvjp(back_keep, back_low)

def rms_scale(values):
    return lax.rsqrt(lax.optimization_barrier(jnp.mean(values * values, axis=-1, keepdims=True)) + EPSILON)

def rope_tables(count, width):
    half = width // 2
    freqs = THETA ** (-(jnp.arange(half, dtype=jnp.float32) * 2.0 / width))
    angles = jnp.arange(count, dtype=jnp.float32)[:, None] * freqs[None, :]
    cosine = jnp.concatenate([jnp.cos(angles), jnp.cos(angles)], axis=1)
    sine = jnp.concatenate([jnp.sin(angles), jnp.sin(angles)], axis=1)
    return (cosine, sine)

def rotate(values, cosine, sine):
    half = values.shape[-1] // 2
    turned = jnp.concatenate([-values[..., half:], values[..., :half]], axis=-1)
    return values * cosine[:, None, :] + turned * sine[:, None, :]

def layer(inputs, length, routes, params):
    attention_gain, query_weight, key_weight, value_weight, query_gain, key_gain, output_weight, routing_gain, router_weight, gate_weight, up_weight, down_weight = params
    highest = lax.Precision.HIGHEST
    count = inputs.shape[0]
    ratio = HEADS // KV_HEADS
    xnorm1 = low(inputs * rms_scale(inputs) * attention_gain)
    query = low_back(jnp.dot(xnorm1, query_weight, precision=highest)).reshape(count, HEADS, HD)
    key = low_back(jnp.dot(xnorm1, key_weight, precision=highest)).reshape(count, KV_HEADS, HD)
    value = low(low_back(jnp.dot(xnorm1, value_weight, precision=highest))).reshape(count, KV_HEADS, HD)
    query_normed = query * rms_scale(query) * query_gain
    key_normed = key * rms_scale(key) * key_gain
    cosine, sine = rope_tables(count, HD)
    query_rot = low(rotate(query_normed, cosine, sine)).reshape(count, KV_HEADS, ratio, HD)
    key_rot = low(rotate(key_normed, cosine, sine))
    block = min(512, count)
    blocks = count // block
    columns = jnp.arange(count, dtype=jnp.int32)

    def attend(item):
        qblock, start = item
        rows = start + jnp.arange(block, dtype=jnp.int32)
        allowed = (columns[None, :] <= rows[:, None]) & (columns[None, :] < length)
        scores = low_back(jnp.einsum('qagh,kah->agqk', qblock, key_rot, precision=highest) * HD ** (-0.5))
        scores = jnp.where(allowed[None, None, :, :], scores, NEGATIVE)
        probs = low(jax.nn.softmax(scores, axis=-1))
        return jnp.einsum('agqk,kah->qagh', probs, value, precision=highest)
    starts = jnp.arange(blocks, dtype=jnp.int32) * block
    outputs = lax.map(jax.checkpoint(attend), (query_rot.reshape(blocks, block, KV_HEADS, ratio, HD), starts))
    valid = (columns < length).astype(jnp.float32)[:, None]
    heads = low_back(low(outputs.reshape(count, HEADS * HD) * valid))
    attention = low_back(jnp.dot(heads, output_weight.T, precision=highest))
    hidden = inputs + attention
    xnorm2 = low(hidden * rms_scale(hidden) * routing_gain)
    logits = low_back(jnp.dot(xnorm2, router_weight, precision=highest))
    router = jax.nn.softmax(logits, axis=-1)
    onehot = routes[:, :, None] == jnp.arange(EXPERTS, dtype=jnp.int32)[None, None, :]
    chosen = lax.optimization_barrier(jnp.sum(jnp.where(onehot, router[:, None, :], 0.0), axis=-1))
    route_weight = chosen / lax.optimization_barrier(jnp.sum(chosen, axis=1, keepdims=True))
    flat_routes = routes.reshape(-1)
    hits = (flat_routes[:, None] == jnp.arange(EXPERTS, dtype=jnp.int32)[None, :]).astype(jnp.int32)
    ranks = lax.optimization_barrier(jnp.sum((jnp.cumsum(hits, axis=0) - 1) * hits, axis=1))
    slot = flat_routes * CAP + ranks
    table = jnp.full((EXPERTS * CAP,), count * TOP, jnp.int32).at[slot].set(jnp.arange(count * TOP, dtype=jnp.int32))
    slot_token = table // TOP
    slot_rows = low_back(jnp.take(xnorm2, slot_token, axis=0, mode='fill', fill_value=0.0)).reshape(EXPERTS, CAP, D)
    gate = low_back(jnp.einsum('ecd,edf->ecf', slot_rows, gate_weight, precision=highest))
    up = low_back(jnp.einsum('ecd,edf->ecf', slot_rows, up_weight, precision=highest))
    inner = low(jax.nn.silu(gate) * up)
    expert_out = low_back(low(jnp.einsum('ecf,efd->ecd', inner, down_weight, precision=highest)))
    picked = jnp.take(expert_out.reshape(EXPERTS * CAP, D), slot, axis=0).reshape(count, TOP, D)
    return hidden + lax.optimization_barrier(jnp.sum(route_weight[:, :, None] * picked, axis=1))

def reference(tokens, seq_length, expert_routes, attention_gain, query_weight, key_weight, value_weight, query_gain, key_gain, output_weight, routing_gain, router_weight, gate_weight, up_weight, down_weight, cotangent):
    params = tuple((item.astype(jnp.float32) for item in (attention_gain, query_weight, key_weight, value_weight, query_gain, key_gain, output_weight, routing_gain, router_weight, gate_weight, up_weight, down_weight)))
    inputs = tokens.astype(jnp.float32).reshape(GROUPS, TOK_DEV, D)
    routes = expert_routes.reshape(GROUPS, TOK_DEV, TOP)
    upstream = cotangent.astype(jnp.float32).reshape(GROUPS, TOK_DEV, D)

    def step(totals, item):
        group_inputs, group_length, group_routes, group_upstream = item
        result, pullback = jax.vjp(lambda values, weights: layer(values, group_length, group_routes, weights), group_inputs, params)
        inputs_grad, params_grad = pullback(group_upstream)
        totals = jax.tree.map(lambda left, right: left + right, totals, params_grad)
        return (totals, (result, inputs_grad))
    zeros = jax.tree.map(jnp.zeros_like, params)
    totals, (results, grads) = lax.scan(step, zeros, (inputs, seq_length, routes, upstream))
    mixed = results.reshape(TOKENS, D).astype(jnp.bfloat16)
    tokens_grad = grads.reshape(TOKENS, D).astype(jnp.bfloat16)
    return (mixed, tokens_grad, totals[0], totals[1], totals[2], totals[3], totals[4], totals[5], totals[6], totals[7], totals[8], totals[9], totals[10], totals[11])
```

```python
import functools

import jax
import jax.numpy as jnp
from jax import lax
from jax.experimental import pallas as pl
from jax.experimental.pallas import tpu as pltpu
from jax.sharding import PartitionSpec as P

EPSILON = 1e-06
THETA = 1000000.0
NEGATIVE = -1e30


def rms_scale(values):
    return lax.rsqrt(jnp.mean(values * values, axis=-1, keepdims=True) + EPSILON)


def rope_tables(count, width):
    half = width // 2
    freqs = THETA ** (-(jnp.arange(half, dtype=jnp.float32) * 2.0 / width))
    angles = jnp.arange(count, dtype=jnp.float32)[:, None] * freqs[None, :]
    cosine = jnp.concatenate([jnp.cos(angles), jnp.cos(angles)], axis=1)
    sine = jnp.concatenate([jnp.sin(angles), jnp.sin(angles)], axis=1)
    return (cosine, sine)


def rotate(values, cosine, sine):
    half = values.shape[-1] // 2
    turned = jnp.concatenate([-values[..., half:], values[..., :half]], axis=-1)
    return values * cosine[:, None, :] + turned * sine[:, None, :]


def rotate_back(grads, cosine, sine):
    half = grads.shape[-1] // 2
    scaled = grads * sine[:, None, :]
    turned = jnp.concatenate([scaled[..., half:], -scaled[..., :half]], axis=-1)
    return grads * cosine[:, None, :] + turned


def head_norm(values, gain):
    scale = rms_scale(values)
    normed = values * scale
    return (normed * gain, normed, scale)


def head_norm_back(grads, normed, scale, gain):
    gain_grad = jnp.sum(grads * normed, axis=(0, 1))
    inner = grads * gain
    values_grad = scale * (inner - normed * jnp.mean(inner * normed, axis=-1, keepdims=True))
    return (values_grad, gain_grad)


def contract(left, right, left_dim, right_dim):
    return lax.dot_general(
        left, right, (((left_dim,), (right_dim,)), ((), ())), preferred_element_type=jnp.float32
    )


def block_scores(qblock, start, keys, length):
    block = qblock.shape[0]
    count = keys.shape[0]
    factor = qblock.shape[-1] ** (-0.5)
    rows = start + jnp.arange(block, dtype=jnp.int32)
    columns = jnp.arange(count, dtype=jnp.int32)
    allowed = (columns[None, :] <= rows[:, None]) & (columns[None, :] < length)
    scores = jnp.einsum("qagh,kah->agqk", qblock, keys, preferred_element_type=jnp.float32) * factor
    return (jnp.where(allowed[None, None, :, :], scores, NEGATIVE), factor)


def attend_block(qblock, start, keys, values, length):
    scores, factor = block_scores(qblock, start, keys, length)
    peak = jnp.max(scores, axis=-1, keepdims=True)
    expo = jnp.exp(scores - peak)
    total = jnp.sum(expo, axis=-1, keepdims=True)
    probs_low = (expo / total).astype(jnp.bfloat16)
    output = jnp.einsum("agqk,kah->qagh", probs_low, values, preferred_element_type=jnp.float32)
    return (output, (peak + jnp.log(total))[..., 0])


def attend_back(qblock, dblock, lse_block, start, keys, values, length):
    scores, factor = block_scores(qblock, start, keys, length)
    probs = jnp.exp(scores - lse_block[..., None])
    probs_grad = jnp.einsum("qagh,kah->agqk", dblock, values, preferred_element_type=jnp.float32)
    delta = jnp.sum(probs * probs_grad, axis=-1, keepdims=True)
    score_grad = (probs * (probs_grad - delta)).astype(jnp.bfloat16)
    query_grad = (
        jnp.einsum("agqk,kah->qagh", score_grad, keys, preferred_element_type=jnp.float32) * factor
    )
    key_grad = (
        jnp.einsum("agqk,qagh->kah", score_grad, qblock, preferred_element_type=jnp.float32)
        * factor
    )
    value_grad = jnp.einsum(
        "agqk,qagh->kah", probs.astype(jnp.bfloat16), dblock, preferred_element_type=jnp.float32
    )
    return (query_grad, key_grad, value_grad)


def routed_shards(
    tokens,
    seq_length,
    expert_routes,
    attention_gain,
    query_weight,
    key_weight,
    value_weight,
    query_gain,
    key_gain,
    output_weight,
    routing_gain,
    router_weight,
    gate_weight,
    up_weight,
    down_weight,
    cotangent,
):
    count = tokens.shape[0]
    width = tokens.shape[1]
    head_size = query_gain.shape[0]
    local_heads = query_weight.shape[1] // head_size
    local_groups = key_weight.shape[1] // head_size
    ratio = local_heads // local_groups
    length = seq_length[0]
    experts = router_weight.shape[1]
    top = expert_routes.shape[1]
    owned = gate_weight.shape[0]
    sources = experts // owned
    parts = lax.axis_size("tensor")
    part = lax.axis_index("tensor")
    quarter = (count * top * 5 + 16 * experts - 1) // (16 * experts)
    inputs = tokens.astype(jnp.float32)
    scale1 = rms_scale(inputs)
    normed1 = inputs * scale1
    xnorm1 = (normed1 * attention_gain).astype(jnp.bfloat16)
    query_raw = jnp.dot(xnorm1, query_weight, preferred_element_type=jnp.float32).reshape(
        count, local_heads, head_size
    )
    key_raw = jnp.dot(xnorm1, key_weight, preferred_element_type=jnp.float32).reshape(
        count, local_groups, head_size
    )
    value_low = (
        jnp.dot(xnorm1, value_weight, preferred_element_type=jnp.float32)
        .astype(jnp.bfloat16)
        .reshape(count, local_groups, head_size)
    )
    query_gained, query_normed, query_scale = head_norm(query_raw, query_gain)
    key_gained, key_normed, key_scale = head_norm(key_raw, key_gain)
    cosine, sine = rope_tables(count, head_size)
    query_low = rotate(query_gained, cosine, sine).astype(jnp.bfloat16)
    key_low = rotate(key_gained, cosine, sine).astype(jnp.bfloat16)
    block = min(512, count)
    blocks = count // block
    starts = jnp.arange(blocks, dtype=jnp.int32) * block
    query_blocks = query_low.reshape(blocks, block, local_groups, ratio, head_size)

    def forward_block(item):
        qblock, start = item
        return attend_block(qblock, start, key_low, value_low, length)

    outputs, lse = lax.map(forward_block, (query_blocks, starts))
    valid = (jnp.arange(count, dtype=jnp.int32) < length)[:, None]
    heads_low = jnp.where(valid, outputs.reshape(count, local_heads * head_size), 0.0).astype(
        jnp.bfloat16
    )
    attention_part = contract(heads_low, output_weight, 1, 1)
    attention_full = lax.psum(attention_part, "tensor")
    hidden = inputs + attention_full
    scale2 = rms_scale(hidden)
    normed2 = hidden * scale2
    xnorm2 = (normed2 * routing_gain).astype(jnp.bfloat16)
    logits = jnp.dot(xnorm2, router_weight, preferred_element_type=jnp.float32)
    peak = jnp.max(logits, axis=1, keepdims=True)
    expo = jnp.exp(logits - peak)
    router = expo / jnp.sum(expo, axis=1, keepdims=True)
    onehot = expert_routes[:, :, None] == jnp.arange(experts, dtype=jnp.int32)[None, None, :]
    chosen = jnp.sum(jnp.where(onehot, router[:, None, :], 0.0), axis=-1)
    chosen_total = jnp.sum(chosen, axis=1, keepdims=True)
    route_weight = chosen / chosen_total
    flat_routes = expert_routes.reshape(-1)
    hits = (flat_routes[:, None] == jnp.arange(experts, dtype=jnp.int32)[None, :]).astype(jnp.int32)
    ranks = jnp.sum((jnp.cumsum(hits, axis=0) - 1) * hits, axis=1)
    mine = ranks % parts == part
    slot_index = jnp.where(mine, ranks // parts * experts + flat_routes, quarter * experts)
    table = (
        jnp.full((quarter * experts,), count * top, jnp.int32)
        .at[slot_index]
        .set(jnp.arange(count * top, dtype=jnp.int32), mode="drop")
    )
    slot_token = table // top
    send_rows = jnp.take(xnorm2, slot_token, axis=0, mode="fill", fill_value=0).reshape(
        quarter, experts, width
    )
    arrived = lax.all_to_all(send_rows, "expert", split_axis=1, concat_axis=1, tiled=True)
    gate_full, up_full, down_full = (
        lax.all_gather(gate_weight, "tensor", axis=2, tiled=True),
        lax.all_gather(up_weight, "tensor", axis=2, tiled=True),
        lax.all_gather(down_weight, "tensor", axis=1, tiled=True),
    )
    rows_own = arrived.reshape(quarter, sources, owned, width)
    gate_val = jnp.einsum("csjd,jdf->csjf", rows_own, gate_full, preferred_element_type=jnp.float32)
    up_val = jnp.einsum("csjd,jdf->csjf", rows_own, up_full, preferred_element_type=jnp.float32)
    sigmoid_gate = jax.nn.sigmoid(gate_val)
    activated = gate_val * sigmoid_gate
    inner_low = (activated * up_val).astype(jnp.bfloat16)
    expert_total = jnp.einsum(
        "csjf,jfd->csjd", inner_low, down_full, preferred_element_type=jnp.float32
    )
    expert_low = expert_total.astype(jnp.bfloat16).reshape(quarter, experts, width)
    returned = lax.all_to_all(
        expert_low, "expert", split_axis=1, concat_axis=1, tiled=True
    ).reshape(quarter * experts, width)
    picked = jnp.take(returned, slot_index, axis=0, mode="fill", fill_value=0).reshape(
        count, top, width
    )
    mine_rows = mine.reshape(count, top)
    mine_weight = jnp.where(mine_rows, route_weight, 0.0)
    moe_part = jnp.sum(mine_weight[:, :, None] * picked, axis=1)
    moe_full = lax.psum(moe_part.astype(jnp.bfloat16), "tensor").astype(jnp.float32)
    mixed = (hidden + moe_full).astype(jnp.bfloat16)
    upstream = cotangent.astype(jnp.float32)
    route_grad_part = jnp.where(mine_rows, jnp.sum(picked * upstream[:, None, :], axis=-1), 0.0)
    slot_weight = jnp.take(route_weight.reshape(-1), table, mode="fill", fill_value=0.0)
    grad_send = (
        jnp.take(cotangent, slot_token, axis=0, mode="fill", fill_value=0) * slot_weight[:, None]
    ).astype(jnp.bfloat16)
    grad_arrived = lax.all_to_all(
        grad_send.reshape(quarter, experts, width),
        "expert",
        split_axis=1,
        concat_axis=1,
        tiled=True,
    )
    grad_own = grad_arrived.reshape(quarter, sources, owned, width)
    down_part = jnp.einsum(
        "csjf,csjd->jfd", inner_low, grad_own, preferred_element_type=jnp.float32
    )
    inner_grad = jnp.einsum(
        "csjd,jfd->csjf", grad_own, down_full, preferred_element_type=jnp.float32
    )
    gate_grad_low = (
        inner_grad * up_val * sigmoid_gate * (1.0 + gate_val * (1.0 - sigmoid_gate))
    ).astype(jnp.bfloat16)
    up_grad_low = (inner_grad * activated).astype(jnp.bfloat16)
    gate_part = jnp.einsum(
        "csjd,csjf->jdf", rows_own, gate_grad_low, preferred_element_type=jnp.float32
    )
    up_part = jnp.einsum(
        "csjd,csjf->jdf", rows_own, up_grad_low, preferred_element_type=jnp.float32
    )
    rows_grad = jnp.einsum(
        "csjf,jdf->csjd", gate_grad_low, gate_full, preferred_element_type=jnp.float32
    )
    rows_grad = rows_grad + jnp.einsum(
        "csjf,jdf->csjd", up_grad_low, up_full, preferred_element_type=jnp.float32
    )
    gate_grad, up_grad, down_grad = (
        lax.psum_scatter(
            gate_part.astype(jnp.bfloat16), "tensor", scatter_dimension=2, tiled=True
        ).astype(jnp.float32),
        lax.psum_scatter(
            up_part.astype(jnp.bfloat16), "tensor", scatter_dimension=2, tiled=True
        ).astype(jnp.float32),
        lax.psum_scatter(
            down_part.astype(jnp.bfloat16), "tensor", scatter_dimension=1, tiled=True
        ).astype(jnp.float32),
    )
    rows_grad_low = rows_grad.astype(jnp.bfloat16).reshape(quarter, experts, width)
    returned_grad = lax.all_to_all(
        rows_grad_low, "expert", split_axis=1, concat_axis=1, tiled=True
    ).reshape(quarter * experts, width)
    route_rows = jnp.take(returned_grad, slot_index, axis=0, mode="fill", fill_value=0).reshape(
        count, top, width
    )
    xnorm2_part = jnp.sum(route_rows, axis=1, dtype=jnp.float32)
    xnorm2_moe, route_grad = (
        lax.psum(xnorm2_part.astype(jnp.bfloat16), "tensor").astype(jnp.float32),
        lax.psum(route_grad_part.astype(jnp.bfloat16), "tensor").astype(jnp.float32),
    )
    inner_total = jnp.sum(route_grad * route_weight, axis=1, keepdims=True)
    chosen_grad = (route_grad - inner_total) / chosen_total
    prob_grad = jnp.sum(jnp.where(onehot, chosen_grad[:, :, None], 0.0), axis=1)
    logit_low = (router * (prob_grad - jnp.sum(router * prob_grad, axis=1, keepdims=True))).astype(
        jnp.bfloat16
    )
    router_grad = contract(xnorm2, logit_low, 0, 0)
    xnorm2_grad = xnorm2_moe + contract(logit_low, router_weight, 1, 1)
    routing_gain_part = jnp.sum(xnorm2_grad * normed2, axis=0)
    inner2 = xnorm2_grad * routing_gain
    hidden_grad = upstream + scale2 * (
        inner2 - normed2 * jnp.mean(inner2 * normed2, axis=1, keepdims=True)
    )
    hidden_low = hidden_grad.astype(jnp.bfloat16)
    output_grad = contract(hidden_low, heads_low, 0, 0)
    heads_grad = jnp.where(
        valid,
        jnp.dot(hidden_low, output_weight, preferred_element_type=jnp.float32).astype(jnp.bfloat16),
        jnp.zeros((), jnp.bfloat16),
    )
    grad_blocks = heads_grad.reshape(blocks, block, local_groups, ratio, head_size)

    def backward_block(carry, item):
        key_acc, value_acc = carry
        qblock, dblock, lse_block, start = item
        query_piece, key_piece, value_piece = attend_back(
            qblock, dblock, lse_block, start, key_low, value_low, length
        )
        return ((key_acc + key_piece, value_acc + value_piece), query_piece)

    empty = jnp.zeros((count, local_groups, head_size), jnp.float32)
    (key_rot_grad, value_grad), query_rot_grad = lax.scan(
        backward_block, (empty, empty), (query_blocks, grad_blocks, lse, starts)
    )
    query_back, query_gain_part = head_norm_back(
        rotate_back(query_rot_grad.reshape(count, local_heads, head_size), cosine, sine),
        query_normed,
        query_scale,
        query_gain,
    )
    key_back, key_gain_part = head_norm_back(
        rotate_back(key_rot_grad, cosine, sine), key_normed, key_scale, key_gain
    )
    query_grad_low = query_back.reshape(count, local_heads * head_size).astype(jnp.bfloat16)
    key_grad_low = key_back.reshape(count, local_groups * head_size).astype(jnp.bfloat16)
    value_grad_low = value_grad.reshape(count, local_groups * head_size).astype(jnp.bfloat16)
    query_wgrad = contract(xnorm1, query_grad_low, 0, 0)
    key_wgrad = contract(xnorm1, key_grad_low, 0, 0)
    value_wgrad = contract(xnorm1, value_grad_low, 0, 0)
    xnorm1_part = contract(query_grad_low, query_weight, 1, 1) + contract(
        key_grad_low, key_weight, 1, 1
    )
    xnorm1_part = xnorm1_part + contract(value_grad_low, value_weight, 1, 1)
    xnorm1_grad, query_gain_sum, key_gain_sum = (
        lax.psum(xnorm1_part.astype(jnp.bfloat16), "tensor").astype(jnp.float32),
        lax.psum(query_gain_part.astype(jnp.bfloat16), "tensor").astype(jnp.float32),
        lax.psum(key_gain_part.astype(jnp.bfloat16), "tensor").astype(jnp.float32),
    )
    attention_gain_part = jnp.sum(xnorm1_grad * normed1, axis=0)
    inner1 = xnorm1_grad * attention_gain
    tokens_grad = (
        hidden_grad
        + scale1 * (inner1 - normed1 * jnp.mean(inner1 * normed1, axis=1, keepdims=True))
    ).astype(jnp.bfloat16)
    summed = (
        lax.psum_scatter(
            attention_gain_part.astype(jnp.bfloat16), "expert", scatter_dimension=0, tiled=True
        ).astype(jnp.float32),
        lax.psum_scatter(
            query_wgrad.astype(jnp.bfloat16), "expert", scatter_dimension=0, tiled=True
        ).astype(jnp.float32),
        lax.psum_scatter(
            key_wgrad.astype(jnp.bfloat16), "expert", scatter_dimension=0, tiled=True
        ).astype(jnp.float32),
        lax.psum_scatter(
            value_wgrad.astype(jnp.bfloat16), "expert", scatter_dimension=0, tiled=True
        ).astype(jnp.float32),
        lax.psum_scatter(
            query_gain_sum.astype(jnp.bfloat16), "expert", scatter_dimension=0, tiled=True
        ).astype(jnp.float32),
        lax.psum_scatter(
            key_gain_sum.astype(jnp.bfloat16), "expert", scatter_dimension=0, tiled=True
        ).astype(jnp.float32),
        lax.psum_scatter(
            output_grad.astype(jnp.bfloat16), "expert", scatter_dimension=0, tiled=True
        ).astype(jnp.float32),
        lax.psum_scatter(
            routing_gain_part.astype(jnp.bfloat16), "expert", scatter_dimension=0, tiled=True
        ).astype(jnp.float32),
        lax.psum_scatter(
            router_grad.astype(jnp.bfloat16), "expert", scatter_dimension=0, tiled=True
        ).astype(jnp.float32),
    )
    return (
        mixed,
        tokens_grad,
        summed[0],
        summed[1],
        summed[2],
        summed[3],
        summed[4],
        summed[5],
        summed[6],
        summed[7],
        summed[8],
        gate_grad,
        up_grad,
        down_grad,
    )


MESH_ID = pl.DeviceIdType.MESH
DEPTH = 4
F32 = jnp.float32
LOW = jnp.bfloat16


class Place:
    def __init__(self):
        e, t = lax.axis_index("expert"), lax.axis_index("tensor")
        self.e, self.t = e, t
        self.z, self.y, self.x, self.c = e // 2, e % 2, t // 2, t % 2

    def at(self, z=None, y=None, x=None, c=None):
        z, y = self.z if z is None else z, self.y if y is None else y
        x, c = self.x if x is None else x, self.c if c is None else c
        return (z * 2 + y, x * 2 + c)

    def block(self, **where):
        e, t = self.at(**where)
        return e * 4 + t

    def near(self, k):
        table = ((0, 1, 2, 3), (1, 2, 0, 3), (2, 1, 3, 0), (3, 2, 1, 0))
        out = 0
        for z in range(DEPTH):
            if isinstance(k, int):
                column = table[z][k]
            else:
                column = table[z][0]
                for i in range(1, DEPTH):
                    column = jnp.where(k == i, table[z][i], column)
            out = jnp.where(self.z == z, column, out)
        return out

    def peers(self):
        line = [self.at(z=(self.z + d) % DEPTH) for d in range(1, DEPTH)]
        return line + [self.at(x=1 - self.x), self.at(y=1 - self.y), self.at(c=1 - self.c)]


class Copies:
    def __init__(self, send_sems, recv_sems):
        self.send_sems, self.recv_sems, self.used, self.made = send_sems, recv_sems, 0, []

    def make(self, src, dst, to):
        i = self.used
        self.used += 1
        copy = pltpu.make_async_remote_copy(
            src,
            dst,
            self.send_sems.at[i],
            self.recv_sems.at[i],
            device_id=to,
            device_id_type=MESH_ID,
        )
        self.made.append(copy)
        return copy

    def along(self, pieces, to, mine):
        base = self.used
        self.used += DEPTH
        out = []
        for (peer, src, dst), device in zip(pieces, to):
            there = pltpu.make_async_remote_copy(
                src,
                dst,
                self.send_sems.at[base + peer],
                self.recv_sems.at[base + mine],
                device_id=device,
                device_id_type=MESH_ID,
            )
            back = pltpu.make_async_remote_copy(
                src,
                dst,
                self.send_sems.at[base + peer],
                self.recv_sems.at[base + peer],
                device_id=device,
                device_id_type=MESH_ID,
            )
            self.made.append(there)
            out.append((there, back))
        return out

    def finish(self):
        for copy in self.made:
            copy.wait_send()


def enter(peers):
    barrier = pltpu.get_barrier_semaphore()
    for peer in peers:
        pl.semaphore_signal(barrier, inc=1, device_id=peer, device_id_type=MESH_ID)
    pl.semaphore_wait(barrier, len(peers))


def pieces_of(ref, rows):
    half = rows // 2

    def whole(b):
        return ref.at[pl.ds(pl.multiple_of(b * rows, rows), rows)]

    def first(b):
        return ref.at[pl.ds(pl.multiple_of(b * rows, rows), half)]

    def second(b):
        return ref.at[pl.ds(pl.multiple_of(b * rows + half, half), half)]

    return whole, first, second


GATHER_SEMS = DEPTH + 3 * DEPTH + 4 * DEPTH + 2 * DEPTH


def gather_steps(p, copies, rows, own_ref, all_ref, own_copy):
    whole, first, second = pieces_of(all_ref, rows)
    me = p.block()
    xn, yn, cn = p.at(x=1 - p.x), p.at(y=1 - p.y), p.at(c=1 - p.c)
    order = [p.near(k) for k in range(DEPTH)]
    line = copies.along(
        [(z, own_ref, whole(me)) for z in order[1:]], [p.at(z=z) for z in order[1:]], p.z
    )
    to_x, to_y, near, far, diagonal = [], [], [], [], []
    for d in range(DEPTH):
        b = p.block(z=order[d])
        src = own_ref if d == 0 else whole(b)
        to_x.append(copies.make(src, whole(b), xn))
        to_y.append(copies.make(src, whole(b), yn))
        bx, by = p.block(z=order[d], x=1 - p.x), p.block(z=order[d], y=1 - p.y)
        bd = p.block(z=order[d], x=1 - p.x, y=1 - p.y)
        near.append([copies.make(src, whole(b), cn), copies.make(whole(bx), whole(bx), cn)])
        diagonal.append(
            (copies.make(first(bx), first(bx), yn), copies.make(second(by), second(by), xn))
        )
        far.append(
            [
                copies.make(whole(by), whole(by), cn),
                copies.make(first(bd), first(bd), cn),
                copies.make(second(bd), second(bd), cn),
            ]
        )

    def onward(d):
        if d:
            line[d - 1][1].wait_recv()
        to_x[d].start()
        to_y[d].start()
        near[d][0].start()

    def pair(d):
        to_x[d].wait_recv()
        diagonal[d][0].start()
        near[d][1].start()
        to_y[d].wait_recv()
        diagonal[d][1].start()
        far[d][0].start()

    def corner(d):
        for i in range(2):
            diagonal[d][i].wait_recv()
            far[d][1 + i].start()

    def arrived(group):
        for copy in group:
            copy.wait_recv()

    def step0():
        own_copy.start()
        for there, _ in line:
            there.start()
        onward(0)
        onward(1)
        pair(0)
        own_copy.wait()
        arrived(near[0])

    def step1():
        onward(2)
        pair(1)
        corner(0)
        arrived(far[0])

    def step3():
        onward(3)
        pair(2)
        corner(1)
        arrived(far[1])

    def step5():
        pair(3)
        corner(2)
        arrived(far[2])

    def step6():
        corner(3)
        arrived(near[3])

    return [
        step0,
        step1,
        lambda: arrived(near[1]),
        step3,
        lambda: arrived(near[2]),
        step5,
        step6,
        lambda: arrived(far[3]),
    ]


SCATTER_SEMS = 16 + 8 + 8 + DEPTH


def scatter_scratch(rows, width):
    return [
        pltpu.VMEM((16, rows, width), LOW),
        pltpu.VMEM((2, DEPTH, rows // 2, width), LOW),
        pltpu.VMEM((2, DEPTH, rows, width), LOW),
        pltpu.VMEM((DEPTH, rows, width), LOW),
    ]


def scatter_steps(p, copies, rows, part, core_in, diag_in, side_in, line_in, out_ref):
    whole, first, second = pieces_of(part, rows)
    order = [p.near(k) for k in reversed(range(DEPTH))]
    xn, yn, cn = p.at(x=1 - p.x), p.at(y=1 - p.y), p.at(c=1 - p.c)
    kinds = [dict(y=1 - p.y, x=1 - p.x), dict(x=1 - p.x), dict(y=1 - p.y), dict()]
    blocks = [[p.block(z=z, **kind) for kind in kinds] for z in order]
    core = [
        [
            copies.make(whole(p.block(z=z, c=1 - p.c, **kind)), core_in.at[k * 4 + j], cn)
            for j, kind in enumerate(kinds)
        ]
        for k, z in enumerate(order)
    ]
    corners = [
        (
            copies.make(first(blocks[k][0]), diag_in.at[0, k], yn),
            copies.make(second(blocks[k][0]), diag_in.at[1, k], xn),
        )
        for k in range(DEPTH)
    ]
    sides = [
        (
            copies.make(whole(blocks[k][1]), side_in.at[0, k], xn),
            copies.make(whole(blocks[k][2]), side_in.at[1, k], yn),
        )
        for k in range(DEPTH)
    ]
    line = copies.along(
        [(order[k], whole(blocks[k][3]), line_in.at[p.z]) for k in range(DEPTH - 1)],
        [p.at(z=order[k]) for k in range(DEPTH - 1)],
        p.z,
    )

    def add(ref, *more):
        total = ref[...].astype(F32)
        for other in more:
            total = total + other[...].astype(F32)
        ref[...] = total.astype(LOW)

    def corner(k):
        core[k][0].wait_recv()
        add(whole(blocks[k][0]), core_in.at[k * 4])
        for copy in corners[k]:
            copy.start()
        for j in (1, 2):
            core[k][j].wait_recv()
            add(whole(blocks[k][j]), core_in.at[k * 4 + j])

    def side(k):
        corners[k][0].wait_recv()
        add(first(blocks[k][1]), diag_in.at[0, k])
        sides[k][0].start()
        corners[k][1].wait_recv()
        add(second(blocks[k][2]), diag_in.at[1, k])
        sides[k][1].start()
        core[k][3].wait_recv()

    def close(k):
        sides[k][0].wait_recv()
        sides[k][1].wait_recv()
        add(whole(blocks[k][3]), core_in.at[k * 4 + 3], side_in.at[0, k], side_in.at[1, k])
        if k < DEPTH - 1:
            line[k][0].start()

    def step0():
        for row in core:
            for copy in row:
                copy.start()
        corner(0)

    def step1():
        corner(1)
        side(0)

    def step2():
        corner(2)
        side(1)

    def step3():
        corner(3)
        side(2)
        close(0)

    def step4():
        side(3)
        close(1)

    def step7():
        total = whole(blocks[DEPTH - 1][3])[...].astype(F32)
        for k in reversed(range(DEPTH - 1)):
            line[k][1].wait_recv()
            total = total + line_in[order[k]].astype(F32)
        out_ref[...] = total

    return [step0, step1, step2, step3, step4, lambda: close(2), lambda: close(3), step7]


def dot(left, right, left_dim, right_dim):
    return lax.dot_general(
        left, right, (((left_dim,), (right_dim,)), ((), ())), preferred_element_type=F32
    )


def semaphores(*counts):
    return [pltpu.SemaphoreType.DMA((n,)) for n in counts]


VMEM_SPEC = pl.BlockSpec(memory_space=pltpu.VMEM)
ANY_SPEC = pl.BlockSpec(memory_space=pl.ANY)


def gather_kernel(rows, own_ref, all_ref, local_sem, send_sems, recv_sems):
    p = Place()
    enter(p.peers())
    copies = Copies(send_sems, recv_sems)
    whole, _, _ = pieces_of(all_ref, rows)
    own_copy = pltpu.make_async_copy(own_ref, whole(p.block()), local_sem.at[0])
    for step in gather_steps(p, copies, rows, own_ref, all_ref, own_copy):
        step()
    copies.finish()


def gather_rows(own, collective_id):
    rows, width = own.shape
    devices = lax.axis_size("expert") * lax.axis_size("tensor")
    return pl.pallas_call(
        functools.partial(gather_kernel, rows),
        out_shape=jax.ShapeDtypeStruct((devices * rows, width), own.dtype),
        in_specs=[ANY_SPEC],
        out_specs=ANY_SPEC,
        scratch_shapes=semaphores(1, GATHER_SEMS, GATHER_SEMS),
        compiler_params=pltpu.CompilerParams(collective_id=collective_id, has_side_effects=True),
        name="gather_rows",
    )(own)


def scatter_kernel(
    rows, part_ref, out_ref, part, core_in, diag_in, side_in, line_in, local_sem, ss, rs
):
    p = Place()
    fetch = pltpu.make_async_copy(part_ref, part, local_sem.at[0])
    fetch.start()
    enter(p.peers())
    fetch.wait()
    copies = Copies(ss, rs)
    for step in scatter_steps(p, copies, rows, part, core_in, diag_in, side_in, line_in, out_ref):
        step()
    copies.finish()


def scatter_rows(part, collective_id):
    total, width = part.shape
    rows = total // (lax.axis_size("expert") * lax.axis_size("tensor"))
    return pl.pallas_call(
        functools.partial(scatter_kernel, rows),
        out_shape=jax.ShapeDtypeStruct((rows, width), F32),
        in_specs=[ANY_SPEC],
        out_specs=VMEM_SPEC,
        scratch_shapes=[pltpu.VMEM(part.shape, LOW)]
        + scatter_scratch(rows, width)
        + semaphores(1, SCATTER_SEMS, SCATTER_SEMS),
        compiler_params=pltpu.CompilerParams(collective_id=collective_id, has_side_effects=True),
        name="scatter_rows",
    )(part)


def experts_kernel(
    rows,
    width,
    experts,
    owned,
    own_ref,
    upstream_ref,
    gate_up_ref,
    down_ref,
    grad_ref,
    moe_ref,
    columns_ref,
    gate_up_grad_ref,
    down_grad_ref,
    all_ref,
    upstream,
    outgoing,
    part,
    back_rows,
    core_in,
    diag_in,
    side_in,
    line_in,
    local_sems,
    gather_send,
    gather_recv,
    scatter_send,
    scatter_recv,
):
    p = Place()
    group = rows * 4
    units = down_ref.shape[0]
    hidden = units // owned
    extra = all_ref.shape[1] - width
    enter(p.peers())
    whole, _, _ = pieces_of(all_ref, rows)
    own_copy = pltpu.make_async_copy(own_ref, whole(p.block()), local_sems.at[0])
    gather_copies = Copies(gather_send, gather_recv)
    scatter_copies = Copies(scatter_send, scatter_recv)
    gathering = gather_steps(p, gather_copies, rows, own_ref, all_ref, own_copy)
    scattering = scatter_steps(
        p, scatter_copies, rows, part, core_in, diag_in, side_in, line_in, grad_ref
    )
    count = 2 * DEPTH

    def rows_of(i):
        side = jnp.where(i % 2 == 0, p.y, 1 - p.y)
        return pl.ds(pl.multiple_of((p.near(i // 2) * 2 + side) * group, group), group)

    def fetch(i):
        return pltpu.make_async_copy(
            upstream_ref.at[rows_of(i)], upstream.at[i % 2], local_sems.at[1 + i % 2]
        )

    def store(i):
        return pltpu.make_async_copy(
            outgoing.at[i % 2], moe_ref.at[rows_of(i)], local_sems.at[3 + i % 2]
        )

    fetch(0).start()
    down_grad_ref[...] = jnp.zeros_like(down_grad_ref)
    first = p.e * owned
    lane = lax.broadcasted_iota(jnp.int32, (group, extra), 1)
    unit = lax.broadcasted_iota(jnp.int32, (group, units), 1)

    @pl.loop(0, count)
    def _(i):
        for k, step in enumerate(gathering):
            pl.when(i == k)(step)
        at = rows_of(i)
        hid = dot(all_ref[at, :width], gate_up_ref[...], 1, 0)
        gate, up = hid[:, :units], hid[:, units:]
        tail = all_ref[at, width:].astype(F32)
        weights = [
            jnp.sum(
                jnp.where((lane == first + j) | (lane == experts + first + j), tail, 0.0),
                axis=1,
                keepdims=True,
            )
            for j in range(owned)
        ]
        weight = weights[0]
        for j in range(1, owned):
            weight = jnp.where(unit >= j * hidden, weights[j], weight)
        sigmoid = 1.0 / (1.0 + jnp.exp(-gate))
        activated = gate * sigmoid
        inner = activated * up
        weighted = (inner * weight).astype(LOW)

        @pl.when(i >= 2)
        def _():
            store(i - 2).wait()

        outgoing[i % 2] = dot(weighted, down_ref[...], 1, 0).astype(LOW)
        store(i).start()
        fetch(i).wait()

        @pl.when(i + 1 < count)
        def _():
            fetch(i + 1).start()

        u = upstream[i % 2]
        down_back = dot(u, down_ref[...], 1, 1)
        down_grad_ref[...] += dot(weighted, u, 0, 0)
        product = inner * down_back
        note = jnp.zeros((group, extra), F32)
        for j in range(owned):
            mine = (unit >= j * hidden) & (unit < (j + 1) * hidden)
            route_grad = jnp.sum(jnp.where(mine, product, 0.0), axis=1, keepdims=True)
            note = jnp.where(lane == first + j, route_grad, note)
        inner_grad = down_back * weight
        gate_back = (inner_grad * up * sigmoid * (1.0 + gate * (1.0 - sigmoid))).astype(LOW)
        up_back = (inner_grad * activated).astype(LOW)
        back_rows[at, :units] = gate_back
        back_rows[at, units:] = up_back
        part[at, :width] = (
            dot(gate_back, gate_up_ref[:, :units], 1, 1) + dot(up_back, gate_up_ref[:, units:], 1, 1)
        ).astype(LOW)
        part[at, width:] = note.astype(LOW)

    share = columns_ref.shape[1]
    columns = pltpu.make_async_copy(
        all_ref.at[:, pl.ds(pl.multiple_of(p.e * share, share), share)],
        columns_ref,
        local_sems.at[0],
    )
    columns.start()
    tile = width // count

    @pl.loop(0, count)
    def _(i):
        for k, step in enumerate(scattering):
            pl.when(i == k)(step)
        at = pl.ds(pl.multiple_of(i * tile, tile), tile)
        gate_up_grad_ref[at, :] = dot(all_ref[:, at], back_rows[...], 0, 0)

    gather_copies.finish()
    scatter_copies.finish()
    store(count - 2).wait()
    store(count - 1).wait()
    columns.wait()


def run_experts(own, upstream_all, gate_up, down, owned, experts, width, collective_id):
    rows, full = own.shape
    total = upstream_all.shape[0]
    units = down.shape[0]
    owners = lax.axis_size("expert")
    group = rows * lax.axis_size("tensor")
    return pl.pallas_call(
        functools.partial(experts_kernel, rows, width, experts, owned),
        out_shape=(
            jax.ShapeDtypeStruct((rows, full), F32),
            jax.ShapeDtypeStruct((total, width), LOW),
            jax.ShapeDtypeStruct((total, width // owners), LOW),
            jax.ShapeDtypeStruct((width, 2 * units), F32),
            jax.ShapeDtypeStruct((units, width), F32),
        ),
        in_specs=[VMEM_SPEC, ANY_SPEC, VMEM_SPEC, VMEM_SPEC],
        out_specs=(VMEM_SPEC, ANY_SPEC, ANY_SPEC, VMEM_SPEC, VMEM_SPEC),
        scratch_shapes=[
            pltpu.VMEM((total, full), LOW),
            pltpu.VMEM((2, group, width), LOW),
            pltpu.VMEM((2, group, width), LOW),
            pltpu.VMEM((total, full), LOW),
            pltpu.VMEM((total, 2 * units), LOW),
        ]
        + scatter_scratch(rows, full)
        + semaphores(6, GATHER_SEMS, GATHER_SEMS, SCATTER_SEMS, SCATTER_SEMS),
        compiler_params=pltpu.CompilerParams(
            collective_id=collective_id, has_side_effects=True, vmem_limit_bytes=64000000
        ),
        name="experts",
    )(own, upstream_all, gate_up, down)


def gathered_shards(
    tokens,
    seq_length,
    expert_routes,
    attention_gain,
    query_weight,
    key_weight,
    value_weight,
    query_gain,
    key_gain,
    output_weight,
    routing_gain,
    router_weight,
    gate_weight,
    up_weight,
    down_weight,
    cotangent,
):
    count, width = tokens.shape
    head_size = query_gain.shape[0]
    local_heads = query_weight.shape[1] // head_size
    local_groups = key_weight.shape[1] // head_size
    ratio = local_heads // local_groups
    length = seq_length[0]
    experts = router_weight.shape[1]
    owned = gate_weight.shape[0]
    parts = lax.axis_size("tensor")
    part = lax.axis_index("tensor")
    owner = lax.axis_index("expert")
    rows = count // parts
    everywhere = ("expert", "tensor")
    low = jnp.bfloat16

    def own_rows(values):
        return lax.dynamic_slice_in_dim(values, part * rows, rows, 0)

    upstream_all = gather_rows(own_rows(cotangent), 0)
    inputs = tokens.astype(jnp.float32)
    scale1 = rms_scale(inputs)
    normed1 = inputs * scale1
    xnorm1 = (normed1 * attention_gain).astype(low)
    xnorm1_columns = lax.all_to_all(xnorm1, "expert", split_axis=1, concat_axis=0, tiled=True)
    query_raw = jnp.dot(xnorm1, query_weight, preferred_element_type=jnp.float32).reshape(
        count, local_heads, head_size
    )
    key_raw = jnp.dot(xnorm1, key_weight, preferred_element_type=jnp.float32).reshape(
        count, local_groups, head_size
    )
    value_low = (
        jnp.dot(xnorm1, value_weight, preferred_element_type=jnp.float32)
        .astype(low)
        .reshape(count, local_groups, head_size)
    )
    query_gained, query_normed, query_scale = head_norm(query_raw, query_gain)
    key_gained, key_normed, key_scale = head_norm(key_raw, key_gain)
    cosine, sine = rope_tables(count, head_size)
    query_low = rotate(query_gained, cosine, sine).astype(low)
    key_low = rotate(key_gained, cosine, sine).astype(low)
    query_block = query_low.reshape(count, local_groups, ratio, head_size)
    outputs, lse = attend_block(query_block, 0, key_low, value_low, length)
    valid = (jnp.arange(count, dtype=jnp.int32) < length)[:, None]
    heads_low = jnp.where(valid, outputs.reshape(count, local_heads * head_size), 0.0).astype(low)
    attention_part = contract(heads_low, output_weight, 1, 1)
    attention = lax.psum_scatter(
        attention_part.astype(low), "tensor", scatter_dimension=0, tiled=True
    ).astype(jnp.float32)
    heads_all = lax.all_gather(heads_low, "expert", axis=0, tiled=True)

    hidden = own_rows(inputs) + attention
    scale2 = rms_scale(hidden)
    normed2 = hidden * scale2
    xnorm2 = (normed2 * routing_gain).astype(low)
    logits = jnp.dot(xnorm2, router_weight, preferred_element_type=jnp.float32)
    peak = jnp.max(logits, axis=1, keepdims=True)
    expo = jnp.exp(logits - peak)
    router = expo / jnp.sum(expo, axis=1, keepdims=True)
    routes = own_rows(expert_routes)
    named = jnp.any(
        routes[:, :, None] == jnp.arange(experts, dtype=jnp.int32)[None, None, :], axis=1
    )
    chosen = jnp.where(named, router, 0.0)
    chosen_total = jnp.sum(chosen, axis=1, keepdims=True)
    route_weight = chosen / chosen_total

    high = route_weight.astype(low)
    rest = (route_weight - high.astype(jnp.float32)).astype(low)
    spare = jnp.zeros((rows, 128 - 2 * experts), low)
    own = jnp.concatenate([xnorm2, high, rest, spare], axis=1)
    gate_up = jnp.concatenate([*gate_weight, *up_weight], axis=1)
    summed, moe_part, columns, gate_up_grad, down_grad = run_experts(
        own, upstream_all, gate_up, down_weight.reshape(-1, width), owned, experts, width, 1
    )
    units = gate_up.shape[1] // (2 * owned)
    split = [gate_up_grad[:, j * units : (j + 1) * units] for j in range(2 * owned)]
    gate_grad, up_grad = jnp.stack(split[:owned]), jnp.stack(split[owned:])
    down_grad = down_grad.reshape(down_weight.shape)
    moe = scatter_rows(moe_part, 2)
    mixed = lax.all_gather((hidden + moe).astype(low), "tensor", axis=0, tiled=True)
    xnorm2_moe, route_grad = summed[:, :width], summed[:, width : width + experts]

    upstream = own_rows(cotangent).astype(jnp.float32)
    inner_total = jnp.sum(route_grad * route_weight, axis=1, keepdims=True)
    prob_grad = jnp.where(named, (route_grad - inner_total) / chosen_total, 0.0)
    logit_low = (router * (prob_grad - jnp.sum(router * prob_grad, axis=1, keepdims=True))).astype(
        low
    )
    logit_all = lax.all_gather(logit_low, everywhere, axis=0, tiled=True)
    router_grad = contract(columns, logit_all, 0, 0)
    xnorm2_grad = xnorm2_moe + contract(logit_low, router_weight, 1, 1)
    routing_gain_part = jnp.sum(xnorm2_grad * normed2, axis=0)
    inner2 = xnorm2_grad * routing_gain
    hidden_grad = upstream + scale2 * (
        inner2 - normed2 * jnp.mean(inner2 * normed2, axis=1, keepdims=True)
    )
    hidden_low = lax.all_gather(hidden_grad.astype(low), "tensor", axis=0, tiled=True)
    hidden_columns = lax.all_to_all(hidden_low, "expert", split_axis=1, concat_axis=0, tiled=True)
    output_grad = contract(hidden_columns, heads_all, 0, 0)
    heads_grad = jnp.where(
        valid,
        jnp.dot(hidden_low, output_weight, preferred_element_type=jnp.float32).astype(low),
        jnp.zeros((), low),
    ).reshape(count, local_groups, ratio, head_size)
    query_rot_grad, key_rot_grad, value_grad = attend_back(
        query_block, heads_grad, lse, 0, key_low, value_low, length
    )
    query_back, query_gain_part = head_norm_back(
        rotate_back(query_rot_grad.reshape(count, local_heads, head_size), cosine, sine),
        query_normed,
        query_scale,
        query_gain,
    )
    key_back, key_gain_part = head_norm_back(
        rotate_back(key_rot_grad, cosine, sine), key_normed, key_scale, key_gain
    )
    query_grad_low = query_back.reshape(count, local_heads * head_size).astype(low)
    key_grad_low = key_back.reshape(count, local_groups * head_size).astype(low)
    value_grad_low = value_grad.reshape(count, local_groups * head_size).astype(low)
    packed = jnp.concatenate([query_grad_low, key_grad_low, value_grad_low], axis=1)
    packed_all = lax.all_gather(packed, "expert", axis=0, tiled=True)
    packed_grad = contract(xnorm1_columns, packed_all, 0, 0)
    query_end = local_heads * head_size
    key_end = query_end + local_groups * head_size
    xnorm1_part = contract(query_grad_low, query_weight, 1, 1) + contract(
        key_grad_low, key_weight, 1, 1
    )
    xnorm1_part = xnorm1_part + contract(value_grad_low, value_weight, 1, 1)
    xnorm1_grad = lax.psum_scatter(
        xnorm1_part.astype(low), "tensor", scatter_dimension=0, tiled=True
    ).astype(jnp.float32)
    normed1_own = own_rows(normed1)
    attention_gain_part = jnp.sum(xnorm1_grad * normed1_own, axis=0)
    inner1 = xnorm1_grad * attention_gain
    tokens_grad = (
        hidden_grad
        + own_rows(scale1)
        * (inner1 - normed1_own * jnp.mean(inner1 * normed1_own, axis=1, keepdims=True))
    ).astype(low)
    tokens_grad = lax.all_gather(tokens_grad, "tensor", axis=0, tiled=True)
    gains = lax.psum(
        jnp.concatenate([attention_gain_part, routing_gain_part, query_gain_part, key_gain_part]),
        everywhere,
    )

    def own_share(start, size):
        share = size // lax.axis_size("expert")
        return lax.dynamic_slice_in_dim(gains, start + owner * share, share, 0)

    return (
        mixed,
        tokens_grad,
        own_share(0, width),
        packed_grad[:, :query_end],
        packed_grad[:, query_end:key_end],
        packed_grad[:, key_end:],
        own_share(2 * width, head_size),
        own_share(2 * width + head_size, head_size),
        output_grad,
        own_share(width, width),
        router_grad,
        gate_grad,
        up_grad,
        down_grad,
    )

def solution(mesh):
    sizes = dict(mesh.shape)
    fits = sizes["expert"] == 2 * DEPTH and sizes["tensor"] == 4
    return jax.shard_map(
        gathered_shards if fits else routed_shards,
        mesh=mesh,
        in_specs=(
            P("expert", None),
            P("expert"),
            P("expert", None),
            P(),
            P(None, "tensor"),
            P(None, "tensor"),
            P(None, "tensor"),
            P(),
            P(),
            P(None, "tensor"),
            P(),
            P(),
            P("expert", None, "tensor"),
            P("expert", None, "tensor"),
            P("expert", "tensor", None),
            P("expert", None),
        ),
        out_specs=(
            P("expert", None),
            P("expert", None),
            P("expert"),
            P("expert", "tensor"),
            P("expert", "tensor"),
            P("expert", "tensor"),
            P("expert"),
            P("expert"),
            P("expert", "tensor"),
            P("expert"),
            P("expert", None),
            P("expert", None, "tensor"),
            P("expert", None, "tensor"),
            P("expert", "tensor", None),
        ),
        check_vma=False,
    )
```

```python
import functools

import jax
import jax.numpy as jnp
from jax import lax
from jax.experimental import pallas as pl
from jax.experimental.pallas import tpu as pltpu
from jax.sharding import PartitionSpec as P

EPSILON = 1e-06
THETA = 1000000.0
NEGATIVE = -1e30


def rms_scale(values):
    return lax.rsqrt(jnp.mean(values * values, axis=-1, keepdims=True) + EPSILON)


def rope_tables(count, width):
    half = width // 2
    freqs = THETA ** (-(jnp.arange(half, dtype=jnp.float32) * 2.0 / width))
    angles = jnp.arange(count, dtype=jnp.float32)[:, None] * freqs[None, :]
    cosine = jnp.concatenate([jnp.cos(angles), jnp.cos(angles)], axis=1)
    sine = jnp.concatenate([jnp.sin(angles), jnp.sin(angles)], axis=1)
    return (cosine, sine)


def rotate(values, cosine, sine):
    half = values.shape[-1] // 2
    turned = jnp.concatenate([-values[..., half:], values[..., :half]], axis=-1)
    return values * cosine[:, None, :] + turned * sine[:, None, :]


def rotate_back(grads, cosine, sine):
    half = grads.shape[-1] // 2
    scaled = grads * sine[:, None, :]
    turned = jnp.concatenate([scaled[..., half:], -scaled[..., :half]], axis=-1)
    return grads * cosine[:, None, :] + turned


def head_norm(values, gain):
    scale = rms_scale(values)
    normed = values * scale
    return (normed * gain, normed, scale)


def head_norm_back(grads, normed, scale, gain):
    gain_grad = jnp.sum(grads * normed, axis=(0, 1))
    inner = grads * gain
    values_grad = scale * (inner - normed * jnp.mean(inner * normed, axis=-1, keepdims=True))
    return (values_grad, gain_grad)


def contract(left, right, left_dim, right_dim):
    return lax.dot_general(
        left, right, (((left_dim,), (right_dim,)), ((), ())), preferred_element_type=jnp.float32
    )


def block_scores(qblock, start, keys, length):
    block = qblock.shape[0]
    count = keys.shape[0]
    factor = qblock.shape[-1] ** (-0.5)
    rows = start + jnp.arange(block, dtype=jnp.int32)
    columns = jnp.arange(count, dtype=jnp.int32)
    allowed = (columns[None, :] <= rows[:, None]) & (columns[None, :] < length)
    scores = jnp.einsum("qagh,kah->agqk", qblock, keys, preferred_element_type=jnp.float32) * factor
    return (jnp.where(allowed[None, None, :, :], scores, NEGATIVE), factor)


def attend_block(qblock, start, keys, values, length):
    scores, factor = block_scores(qblock, start, keys, length)
    peak = jnp.max(scores, axis=-1, keepdims=True)
    expo = jnp.exp(scores - peak)
    total = jnp.sum(expo, axis=-1, keepdims=True)
    probs_low = (expo / total).astype(jnp.bfloat16)
    output = jnp.einsum("agqk,kah->qagh", probs_low, values, preferred_element_type=jnp.float32)
    return (output, (peak + jnp.log(total))[..., 0])


def attend_back(qblock, dblock, lse_block, start, keys, values, length):
    scores, factor = block_scores(qblock, start, keys, length)
    probs = jnp.exp(scores - lse_block[..., None])
    probs_grad = jnp.einsum("qagh,kah->agqk", dblock, values, preferred_element_type=jnp.float32)
    delta = jnp.sum(probs * probs_grad, axis=-1, keepdims=True)
    score_grad = (probs * (probs_grad - delta)).astype(jnp.bfloat16)
    query_grad = (
        jnp.einsum("agqk,kah->qagh", score_grad, keys, preferred_element_type=jnp.float32) * factor
    )
    key_grad = (
        jnp.einsum("agqk,qagh->kah", score_grad, qblock, preferred_element_type=jnp.float32)
        * factor
    )
    value_grad = jnp.einsum(
        "agqk,qagh->kah", probs.astype(jnp.bfloat16), dblock, preferred_element_type=jnp.float32
    )
    return (query_grad, key_grad, value_grad)


def routed_shards(
    tokens,
    seq_length,
    expert_routes,
    attention_gain,
    query_weight,
    key_weight,
    value_weight,
    query_gain,
    key_gain,
    output_weight,
    routing_gain,
    router_weight,
    gate_weight,
    up_weight,
    down_weight,
    cotangent,
):
    count = tokens.shape[0]
    width = tokens.shape[1]
    head_size = query_gain.shape[0]
    local_heads = query_weight.shape[1] // head_size
    local_groups = key_weight.shape[1] // head_size
    ratio = local_heads // local_groups
    length = seq_length[0]
    experts = router_weight.shape[1]
    top = expert_routes.shape[1]
    owned = gate_weight.shape[0]
    sources = experts // owned
    parts = lax.axis_size("tensor")
    part = lax.axis_index("tensor")
    quarter = (count * top * 5 + 16 * experts - 1) // (16 * experts)
    inputs = tokens.astype(jnp.float32)
    scale1 = rms_scale(inputs)
    normed1 = inputs * scale1
    xnorm1 = (normed1 * attention_gain).astype(jnp.bfloat16)
    query_raw = jnp.dot(xnorm1, query_weight, preferred_element_type=jnp.float32).reshape(
        count, local_heads, head_size
    )
    key_raw = jnp.dot(xnorm1, key_weight, preferred_element_type=jnp.float32).reshape(
        count, local_groups, head_size
    )
    value_low = (
        jnp.dot(xnorm1, value_weight, preferred_element_type=jnp.float32)
        .astype(jnp.bfloat16)
        .reshape(count, local_groups, head_size)
    )
    query_gained, query_normed, query_scale = head_norm(query_raw, query_gain)
    key_gained, key_normed, key_scale = head_norm(key_raw, key_gain)
    cosine, sine = rope_tables(count, head_size)
    query_low = rotate(query_gained, cosine, sine).astype(jnp.bfloat16)
    key_low = rotate(key_gained, cosine, sine).astype(jnp.bfloat16)
    block = min(512, count)
    blocks = count // block
    starts = jnp.arange(blocks, dtype=jnp.int32) * block
    query_blocks = query_low.reshape(blocks, block, local_groups, ratio, head_size)

    def forward_block(item):
        qblock, start = item
        return attend_block(qblock, start, key_low, value_low, length)

    outputs, lse = lax.map(forward_block, (query_blocks, starts))
    valid = (jnp.arange(count, dtype=jnp.int32) < length)[:, None]
    heads_low = jnp.where(valid, outputs.reshape(count, local_heads * head_size), 0.0).astype(
        jnp.bfloat16
    )
    attention_part = contract(heads_low, output_weight, 1, 1)
    attention_full = lax.psum(attention_part, "tensor")
    hidden = inputs + attention_full
    scale2 = rms_scale(hidden)
    normed2 = hidden * scale2
    xnorm2 = (normed2 * routing_gain).astype(jnp.bfloat16)
    logits = jnp.dot(xnorm2, router_weight, preferred_element_type=jnp.float32)
    peak = jnp.max(logits, axis=1, keepdims=True)
    expo = jnp.exp(logits - peak)
    router = expo / jnp.sum(expo, axis=1, keepdims=True)
    onehot = expert_routes[:, :, None] == jnp.arange(experts, dtype=jnp.int32)[None, None, :]
    chosen = jnp.sum(jnp.where(onehot, router[:, None, :], 0.0), axis=-1)
    chosen_total = jnp.sum(chosen, axis=1, keepdims=True)
    route_weight = chosen / chosen_total
    flat_routes = expert_routes.reshape(-1)
    hits = (flat_routes[:, None] == jnp.arange(experts, dtype=jnp.int32)[None, :]).astype(jnp.int32)
    ranks = jnp.sum((jnp.cumsum(hits, axis=0) - 1) * hits, axis=1)
    mine = ranks % parts == part
    slot_index = jnp.where(mine, ranks // parts * experts + flat_routes, quarter * experts)
    table = (
        jnp.full((quarter * experts,), count * top, jnp.int32)
        .at[slot_index]
        .set(jnp.arange(count * top, dtype=jnp.int32), mode="drop")
    )
    slot_token = table // top
    send_rows = jnp.take(xnorm2, slot_token, axis=0, mode="fill", fill_value=0).reshape(
        quarter, experts, width
    )
    arrived = lax.all_to_all(send_rows, "expert", split_axis=1, concat_axis=1, tiled=True)
    gate_full, up_full, down_full = (
        lax.all_gather(gate_weight, "tensor", axis=2, tiled=True),
        lax.all_gather(up_weight, "tensor", axis=2, tiled=True),
        lax.all_gather(down_weight, "tensor", axis=1, tiled=True),
    )
    rows_own = arrived.reshape(quarter, sources, owned, width)
    gate_val = jnp.einsum("csjd,jdf->csjf", rows_own, gate_full, preferred_element_type=jnp.float32)
    up_val = jnp.einsum("csjd,jdf->csjf", rows_own, up_full, preferred_element_type=jnp.float32)
    sigmoid_gate = jax.nn.sigmoid(gate_val)
    activated = gate_val * sigmoid_gate
    inner_low = (activated * up_val).astype(jnp.bfloat16)
    expert_total = jnp.einsum(
        "csjf,jfd->csjd", inner_low, down_full, preferred_element_type=jnp.float32
    )
    expert_low = expert_total.astype(jnp.bfloat16).reshape(quarter, experts, width)
    returned = lax.all_to_all(
        expert_low, "expert", split_axis=1, concat_axis=1, tiled=True
    ).reshape(quarter * experts, width)
    picked = jnp.take(returned, slot_index, axis=0, mode="fill", fill_value=0).reshape(
        count, top, width
    )
    mine_rows = mine.reshape(count, top)
    mine_weight = jnp.where(mine_rows, route_weight, 0.0)
    moe_part = jnp.sum(mine_weight[:, :, None] * picked, axis=1)
    moe_full = lax.psum(moe_part.astype(jnp.bfloat16), "tensor").astype(jnp.float32)
    mixed = (hidden + moe_full).astype(jnp.bfloat16)
    upstream = cotangent.astype(jnp.float32)
    route_grad_part = jnp.where(mine_rows, jnp.sum(picked * upstream[:, None, :], axis=-1), 0.0)
    slot_weight = jnp.take(route_weight.reshape(-1), table, mode="fill", fill_value=0.0)
    grad_send = (
        jnp.take(cotangent, slot_token, axis=0, mode="fill", fill_value=0) * slot_weight[:, None]
    ).astype(jnp.bfloat16)
    grad_arrived = lax.all_to_all(
        grad_send.reshape(quarter, experts, width),
        "expert",
        split_axis=1,
        concat_axis=1,
        tiled=True,
    )
    grad_own = grad_arrived.reshape(quarter, sources, owned, width)
    down_part = jnp.einsum(
        "csjf,csjd->jfd", inner_low, grad_own, preferred_element_type=jnp.float32
    )
    inner_grad = jnp.einsum(
        "csjd,jfd->csjf", grad_own, down_full, preferred_element_type=jnp.float32
    )
    gate_grad_low = (
        inner_grad * up_val * sigmoid_gate * (1.0 + gate_val * (1.0 - sigmoid_gate))
    ).astype(jnp.bfloat16)
    up_grad_low = (inner_grad * activated).astype(jnp.bfloat16)
    gate_part = jnp.einsum(
        "csjd,csjf->jdf", rows_own, gate_grad_low, preferred_element_type=jnp.float32
    )
    up_part = jnp.einsum(
        "csjd,csjf->jdf", rows_own, up_grad_low, preferred_element_type=jnp.float32
    )
    rows_grad = jnp.einsum(
        "csjf,jdf->csjd", gate_grad_low, gate_full, preferred_element_type=jnp.float32
    )
    rows_grad = rows_grad + jnp.einsum(
        "csjf,jdf->csjd", up_grad_low, up_full, preferred_element_type=jnp.float32
    )
    gate_grad, up_grad, down_grad = (
        lax.psum_scatter(
            gate_part.astype(jnp.bfloat16), "tensor", scatter_dimension=2, tiled=True
        ).astype(jnp.float32),
        lax.psum_scatter(
            up_part.astype(jnp.bfloat16), "tensor", scatter_dimension=2, tiled=True
        ).astype(jnp.float32),
        lax.psum_scatter(
            down_part.astype(jnp.bfloat16), "tensor", scatter_dimension=1, tiled=True
        ).astype(jnp.float32),
    )
    rows_grad_low = rows_grad.astype(jnp.bfloat16).reshape(quarter, experts, width)
    returned_grad = lax.all_to_all(
        rows_grad_low, "expert", split_axis=1, concat_axis=1, tiled=True
    ).reshape(quarter * experts, width)
    route_rows = jnp.take(returned_grad, slot_index, axis=0, mode="fill", fill_value=0).reshape(
        count, top, width
    )
    xnorm2_part = jnp.sum(route_rows, axis=1, dtype=jnp.float32)
    xnorm2_moe, route_grad = (
        lax.psum(xnorm2_part.astype(jnp.bfloat16), "tensor").astype(jnp.float32),
        lax.psum(route_grad_part.astype(jnp.bfloat16), "tensor").astype(jnp.float32),
    )
    inner_total = jnp.sum(route_grad * route_weight, axis=1, keepdims=True)
    chosen_grad = (route_grad - inner_total) / chosen_total
    prob_grad = jnp.sum(jnp.where(onehot, chosen_grad[:, :, None], 0.0), axis=1)
    logit_low = (router * (prob_grad - jnp.sum(router * prob_grad, axis=1, keepdims=True))).astype(
        jnp.bfloat16
    )
    router_grad = contract(xnorm2, logit_low, 0, 0)
    xnorm2_grad = xnorm2_moe + contract(logit_low, router_weight, 1, 1)
    routing_gain_part = jnp.sum(xnorm2_grad * normed2, axis=0)
    inner2 = xnorm2_grad * routing_gain
    hidden_grad = upstream + scale2 * (
        inner2 - normed2 * jnp.mean(inner2 * normed2, axis=1, keepdims=True)
    )
    hidden_low = hidden_grad.astype(jnp.bfloat16)
    output_grad = contract(hidden_low, heads_low, 0, 0)
    heads_grad = jnp.where(
        valid,
        jnp.dot(hidden_low, output_weight, preferred_element_type=jnp.float32).astype(jnp.bfloat16),
        jnp.zeros((), jnp.bfloat16),
    )
    grad_blocks = heads_grad.reshape(blocks, block, local_groups, ratio, head_size)

    def backward_block(carry, item):
        key_acc, value_acc = carry
        qblock, dblock, lse_block, start = item
        query_piece, key_piece, value_piece = attend_back(
            qblock, dblock, lse_block, start, key_low, value_low, length
        )
        return ((key_acc + key_piece, value_acc + value_piece), query_piece)

    empty = jnp.zeros((count, local_groups, head_size), jnp.float32)
    (key_rot_grad, value_grad), query_rot_grad = lax.scan(
        backward_block, (empty, empty), (query_blocks, grad_blocks, lse, starts)
    )
    query_back, query_gain_part = head_norm_back(
        rotate_back(query_rot_grad.reshape(count, local_heads, head_size), cosine, sine),
        query_normed,
        query_scale,
        query_gain,
    )
    key_back, key_gain_part = head_norm_back(
        rotate_back(key_rot_grad, cosine, sine), key_normed, key_scale, key_gain
    )
    query_grad_low = query_back.reshape(count, local_heads * head_size).astype(jnp.bfloat16)
    key_grad_low = key_back.reshape(count, local_groups * head_size).astype(jnp.bfloat16)
    value_grad_low = value_grad.reshape(count, local_groups * head_size).astype(jnp.bfloat16)
    query_wgrad = contract(xnorm1, query_grad_low, 0, 0)
    key_wgrad = contract(xnorm1, key_grad_low, 0, 0)
    value_wgrad = contract(xnorm1, value_grad_low, 0, 0)
    xnorm1_part = contract(query_grad_low, query_weight, 1, 1) + contract(
        key_grad_low, key_weight, 1, 1
    )
    xnorm1_part = xnorm1_part + contract(value_grad_low, value_weight, 1, 1)
    xnorm1_grad, query_gain_sum, key_gain_sum = (
        lax.psum(xnorm1_part.astype(jnp.bfloat16), "tensor").astype(jnp.float32),
        lax.psum(query_gain_part.astype(jnp.bfloat16), "tensor").astype(jnp.float32),
        lax.psum(key_gain_part.astype(jnp.bfloat16), "tensor").astype(jnp.float32),
    )
    attention_gain_part = jnp.sum(xnorm1_grad * normed1, axis=0)
    inner1 = xnorm1_grad * attention_gain
    tokens_grad = (
        hidden_grad
        + scale1 * (inner1 - normed1 * jnp.mean(inner1 * normed1, axis=1, keepdims=True))
    ).astype(jnp.bfloat16)
    summed = (
        lax.psum_scatter(
            attention_gain_part.astype(jnp.bfloat16), "expert", scatter_dimension=0, tiled=True
        ).astype(jnp.float32),
        lax.psum_scatter(
            query_wgrad.astype(jnp.bfloat16), "expert", scatter_dimension=0, tiled=True
        ).astype(jnp.float32),
        lax.psum_scatter(
            key_wgrad.astype(jnp.bfloat16), "expert", scatter_dimension=0, tiled=True
        ).astype(jnp.float32),
        lax.psum_scatter(
            value_wgrad.astype(jnp.bfloat16), "expert", scatter_dimension=0, tiled=True
        ).astype(jnp.float32),
        lax.psum_scatter(
            query_gain_sum.astype(jnp.bfloat16), "expert", scatter_dimension=0, tiled=True
        ).astype(jnp.float32),
        lax.psum_scatter(
            key_gain_sum.astype(jnp.bfloat16), "expert", scatter_dimension=0, tiled=True
        ).astype(jnp.float32),
        lax.psum_scatter(
            output_grad.astype(jnp.bfloat16), "expert", scatter_dimension=0, tiled=True
        ).astype(jnp.float32),
        lax.psum_scatter(
            routing_gain_part.astype(jnp.bfloat16), "expert", scatter_dimension=0, tiled=True
        ).astype(jnp.float32),
        lax.psum_scatter(
            router_grad.astype(jnp.bfloat16), "expert", scatter_dimension=0, tiled=True
        ).astype(jnp.float32),
    )
    return (
        mixed,
        tokens_grad,
        summed[0],
        summed[1],
        summed[2],
        summed[3],
        summed[4],
        summed[5],
        summed[6],
        summed[7],
        summed[8],
        gate_grad,
        up_grad,
        down_grad,
    )


MESH_ID = pl.DeviceIdType.MESH
DEPTH = 4
F32 = jnp.float32
LOW = jnp.bfloat16


class Place:
    def __init__(self):
        e, t = lax.axis_index("expert"), lax.axis_index("tensor")
        self.e, self.t = e, t
        self.z, self.y, self.x, self.c = e // 2, e % 2, t // 2, t % 2

    def at(self, z=None, y=None, x=None, c=None):
        z, y = self.z if z is None else z, self.y if y is None else y
        x, c = self.x if x is None else x, self.c if c is None else c
        return (z * 2 + y, x * 2 + c)

    def block(self, **where):
        e, t = self.at(**where)
        return e * 4 + t

    def near(self, k):
        table = ((0, 1, 2, 3), (1, 2, 0, 3), (2, 1, 3, 0), (3, 2, 1, 0))
        out = 0
        for z in range(DEPTH):
            if isinstance(k, int):
                column = table[z][k]
            else:
                column = table[z][0]
                for i in range(1, DEPTH):
                    column = jnp.where(k == i, table[z][i], column)
            out = jnp.where(self.z == z, column, out)
        return out

    def peers(self):
        line = [self.at(z=(self.z + d) % DEPTH) for d in range(1, DEPTH)]
        return line + [self.at(x=1 - self.x), self.at(y=1 - self.y), self.at(c=1 - self.c)]


class Copies:
    def __init__(self, send_sems, recv_sems):
        self.send_sems, self.recv_sems, self.used, self.made = send_sems, recv_sems, 0, []

    def make(self, src, dst, to):
        i = self.used
        self.used += 1
        copy = pltpu.make_async_remote_copy(
            src,
            dst,
            self.send_sems.at[i],
            self.recv_sems.at[i],
            device_id=to,
            device_id_type=MESH_ID,
        )
        self.made.append(copy)
        return copy

    def along(self, pieces, to, mine):
        base = self.used
        self.used += DEPTH
        out = []
        for (peer, src, dst), device in zip(pieces, to):
            there = pltpu.make_async_remote_copy(
                src,
                dst,
                self.send_sems.at[base + peer],
                self.recv_sems.at[base + mine],
                device_id=device,
                device_id_type=MESH_ID,
            )
            back = pltpu.make_async_remote_copy(
                src,
                dst,
                self.send_sems.at[base + peer],
                self.recv_sems.at[base + peer],
                device_id=device,
                device_id_type=MESH_ID,
            )
            self.made.append(there)
            out.append((there, back))
        return out

    def finish(self):
        for copy in self.made:
            copy.wait_send()


def enter(peers):
    barrier = pltpu.get_barrier_semaphore()
    for peer in peers:
        pl.semaphore_signal(barrier, inc=1, device_id=peer, device_id_type=MESH_ID)
    pl.semaphore_wait(barrier, len(peers))


def pieces_of(ref, rows):
    half = rows // 2

    def whole(b):
        return ref.at[pl.ds(pl.multiple_of(b * rows, rows), rows)]

    def first(b):
        return ref.at[pl.ds(pl.multiple_of(b * rows, rows), half)]

    def second(b):
        return ref.at[pl.ds(pl.multiple_of(b * rows + half, half), half)]

    return whole, first, second


GATHER_SEMS = DEPTH + 3 * DEPTH + 4 * DEPTH + 2 * DEPTH


def gather_steps(p, copies, rows, own_ref, all_ref, own_copy):
    whole, first, second = pieces_of(all_ref, rows)
    me = p.block()
    xn, yn, cn = p.at(x=1 - p.x), p.at(y=1 - p.y), p.at(c=1 - p.c)
    order = [p.near(k) for k in range(DEPTH)]
    line = copies.along(
        [(z, own_ref, whole(me)) for z in order[1:]], [p.at(z=z) for z in order[1:]], p.z
    )
    to_x, to_y, near, far, diagonal = [], [], [], [], []
    for d in range(DEPTH):
        b = p.block(z=order[d])
        src = own_ref if d == 0 else whole(b)
        to_x.append(copies.make(src, whole(b), xn))
        to_y.append(copies.make(src, whole(b), yn))
        bx, by = p.block(z=order[d], x=1 - p.x), p.block(z=order[d], y=1 - p.y)
        bd = p.block(z=order[d], x=1 - p.x, y=1 - p.y)
        near.append([copies.make(src, whole(b), cn), copies.make(whole(bx), whole(bx), cn)])
        diagonal.append(
            (copies.make(first(bx), first(bx), yn), copies.make(second(by), second(by), xn))
        )
        far.append(
            [
                copies.make(whole(by), whole(by), cn),
                copies.make(first(bd), first(bd), cn),
                copies.make(second(bd), second(bd), cn),
            ]
        )

    def onward(d):
        if d:
            line[d - 1][1].wait_recv()
        to_x[d].start()
        to_y[d].start()
        near[d][0].start()

    def pair(d):
        to_x[d].wait_recv()
        diagonal[d][0].start()
        near[d][1].start()
        to_y[d].wait_recv()
        diagonal[d][1].start()
        far[d][0].start()

    def corner(d):
        for i in range(2):
            diagonal[d][i].wait_recv()
            far[d][1 + i].start()

    def arrived(group):
        for copy in group:
            copy.wait_recv()

    def step0():
        own_copy.start()
        for there, _ in line:
            there.start()
        onward(0)
        onward(1)
        pair(0)
        own_copy.wait()
        arrived(near[0])

    def step1():
        onward(2)
        pair(1)
        corner(0)
        arrived(far[0])

    def step3():
        onward(3)
        pair(2)
        corner(1)
        arrived(far[1])

    def step5():
        pair(3)
        corner(2)
        arrived(far[2])

    def step6():
        corner(3)
        arrived(near[3])

    return [
        step0,
        step1,
        lambda: arrived(near[1]),
        step3,
        lambda: arrived(near[2]),
        step5,
        step6,
        lambda: arrived(far[3]),
    ]


SCATTER_SEMS = 16 + 8 + 8 + DEPTH


def scatter_scratch(rows, width):
    return [
        pltpu.VMEM((16, rows, width), LOW),
        pltpu.VMEM((2, DEPTH, rows // 2, width), LOW),
        pltpu.VMEM((2, DEPTH, rows, width), LOW),
        pltpu.VMEM((DEPTH, rows, width), LOW),
    ]


def scatter_steps(p, copies, rows, part, core_in, diag_in, side_in, line_in, out_ref):
    whole, first, second = pieces_of(part, rows)
    order = [p.near(k) for k in reversed(range(DEPTH))]
    xn, yn, cn = p.at(x=1 - p.x), p.at(y=1 - p.y), p.at(c=1 - p.c)
    kinds = [dict(y=1 - p.y, x=1 - p.x), dict(x=1 - p.x), dict(y=1 - p.y), dict()]
    blocks = [[p.block(z=z, **kind) for kind in kinds] for z in order]
    core = [
        [
            copies.make(whole(p.block(z=z, c=1 - p.c, **kind)), core_in.at[k * 4 + j], cn)
            for j, kind in enumerate(kinds)
        ]
        for k, z in enumerate(order)
    ]
    corners = [
        (
            copies.make(first(blocks[k][0]), diag_in.at[0, k], yn),
            copies.make(second(blocks[k][0]), diag_in.at[1, k], xn),
        )
        for k in range(DEPTH)
    ]
    sides = [
        (
            copies.make(whole(blocks[k][1]), side_in.at[0, k], xn),
            copies.make(whole(blocks[k][2]), side_in.at[1, k], yn),
        )
        for k in range(DEPTH)
    ]
    line = copies.along(
        [(order[k], whole(blocks[k][3]), line_in.at[p.z]) for k in range(DEPTH - 1)],
        [p.at(z=order[k]) for k in range(DEPTH - 1)],
        p.z,
    )

    def add(ref, *more):
        total = ref[...].astype(F32)
        for other in more:
            total = total + other[...].astype(F32)
        ref[...] = total.astype(LOW)

    def corner(k):
        core[k][0].wait_recv()
        add(whole(blocks[k][0]), core_in.at[k * 4])
        for copy in corners[k]:
            copy.start()
        for j in (1, 2):
            core[k][j].wait_recv()
            add(whole(blocks[k][j]), core_in.at[k * 4 + j])

    def side(k):
        corners[k][0].wait_recv()
        add(first(blocks[k][1]), diag_in.at[0, k])
        sides[k][0].start()
        corners[k][1].wait_recv()
        add(second(blocks[k][2]), diag_in.at[1, k])
        sides[k][1].start()
        core[k][3].wait_recv()

    def close(k):
        sides[k][0].wait_recv()
        sides[k][1].wait_recv()
        add(whole(blocks[k][3]), core_in.at[k * 4 + 3], side_in.at[0, k], side_in.at[1, k])
        if k < DEPTH - 1:
            line[k][0].start()

    def step0():
        for row in core:
            for copy in row:
                copy.start()
        corner(0)

    def step1():
        corner(1)
        side(0)

    def step2():
        corner(2)
        side(1)

    def step3():
        corner(3)
        side(2)
        close(0)

    def step4():
        side(3)
        close(1)

    def step7():
        total = whole(blocks[DEPTH - 1][3])[...].astype(F32)
        for k in reversed(range(DEPTH - 1)):
            line[k][1].wait_recv()
            total = total + line_in[order[k]].astype(F32)
        out_ref[...] = total

    return [step0, step1, step2, step3, step4, lambda: close(2), lambda: close(3), step7]


def dot(left, right, left_dim, right_dim):
    return lax.dot_general(
        left, right, (((left_dim,), (right_dim,)), ((), ())), preferred_element_type=F32
    )


def semaphores(*counts):
    return [pltpu.SemaphoreType.DMA((n,)) for n in counts]


VMEM_SPEC = pl.BlockSpec(memory_space=pltpu.VMEM)
ANY_SPEC = pl.BlockSpec(memory_space=pl.ANY)


def gather_kernel(rows, own_ref, all_ref, local_sem, send_sems, recv_sems):
    p = Place()
    enter(p.peers())
    copies = Copies(send_sems, recv_sems)
    whole, _, _ = pieces_of(all_ref, rows)
    own_copy = pltpu.make_async_copy(own_ref, whole(p.block()), local_sem.at[0])
    for step in gather_steps(p, copies, rows, own_ref, all_ref, own_copy):
        step()
    copies.finish()


def gather_rows(own, collective_id):
    rows, width = own.shape
    devices = lax.axis_size("expert") * lax.axis_size("tensor")
    return pl.pallas_call(
        functools.partial(gather_kernel, rows),
        out_shape=jax.ShapeDtypeStruct((devices * rows, width), own.dtype),
        in_specs=[ANY_SPEC],
        out_specs=ANY_SPEC,
        scratch_shapes=semaphores(1, GATHER_SEMS, GATHER_SEMS),
        compiler_params=pltpu.CompilerParams(collective_id=collective_id, has_side_effects=True),
        name="gather_rows",
    )(own)


def scatter_kernel(
    rows, part_ref, out_ref, part, core_in, diag_in, side_in, line_in, local_sem, ss, rs
):
    p = Place()
    fetch = pltpu.make_async_copy(part_ref, part, local_sem.at[0])
    fetch.start()
    enter(p.peers())
    fetch.wait()
    copies = Copies(ss, rs)
    for step in scatter_steps(p, copies, rows, part, core_in, diag_in, side_in, line_in, out_ref):
        step()
    copies.finish()


def scatter_rows(part, collective_id):
    total, width = part.shape
    rows = total // (lax.axis_size("expert") * lax.axis_size("tensor"))
    return pl.pallas_call(
        functools.partial(scatter_kernel, rows),
        out_shape=jax.ShapeDtypeStruct((rows, width), F32),
        in_specs=[ANY_SPEC],
        out_specs=VMEM_SPEC,
        scratch_shapes=[pltpu.VMEM(part.shape, LOW)]
        + scatter_scratch(rows, width)
        + semaphores(1, SCATTER_SEMS, SCATTER_SEMS),
        compiler_params=pltpu.CompilerParams(collective_id=collective_id, has_side_effects=True),
        name="scatter_rows",
    )(part)


def experts_kernel(
    rows,
    width,
    experts,
    owned,
    own_ref,
    upstream_ref,
    gate_up_ref,
    down_ref,
    heads_ref,
    grad_ref,
    moe_ref,
    line_heads_ref,
    gate_up_grad_ref,
    down_grad_ref,
    all_ref,
    upstream,
    outgoing,
    part,
    back_rows,
    core_in,
    diag_in,
    side_in,
    line_in,
    local_sems,
    gather_send,
    gather_recv,
    scatter_send,
    scatter_recv,
    heads_send,
    heads_recv,
):
    p = Place()
    group = rows * 4
    units = down_ref.shape[0]
    hidden = units // owned
    extra = all_ref.shape[1] - width
    enter(p.peers())
    whole, _, _ = pieces_of(all_ref, rows)
    own_copy = pltpu.make_async_copy(own_ref, whole(p.block()), local_sems.at[0])
    gather_copies = Copies(gather_send, gather_recv)
    scatter_copies = Copies(scatter_send, scatter_recv)
    gathering = gather_steps(p, gather_copies, rows, own_ref, all_ref, own_copy)
    scattering = scatter_steps(
        p, scatter_copies, rows, part, core_in, diag_in, side_in, line_in, grad_ref
    )
    heads_copies = Copies(heads_send, heads_recv)
    others = [p.near(k) for k in range(1, DEPTH)]
    heads_line = heads_copies.along(
        [(z, heads_ref, line_heads_ref.at[p.z]) for z in others], [p.at(z=z) for z in others], p.z
    )
    count = 2 * DEPTH

    def rows_of(i):
        side = jnp.where(i % 2 == 0, p.y, 1 - p.y)
        return pl.ds(pl.multiple_of((p.near(i // 2) * 2 + side) * group, group), group)

    def fetch(i):
        return pltpu.make_async_copy(
            upstream_ref.at[rows_of(i)], upstream.at[i % 2], local_sems.at[1 + i % 2]
        )

    def store(i):
        return pltpu.make_async_copy(
            outgoing.at[i % 2], moe_ref.at[rows_of(i)], local_sems.at[3 + i % 2]
        )

    fetch(0).start()
    down_grad_ref[...] = jnp.zeros_like(down_grad_ref)
    first = p.e * owned
    lane = lax.broadcasted_iota(jnp.int32, (group, extra), 1)
    unit = lax.broadcasted_iota(jnp.int32, (group, units), 1)

    @pl.loop(0, count)
    def _(i):
        for k, step in enumerate(gathering):
            pl.when(i == k)(step)
        at = rows_of(i)
        hid = dot(all_ref[at, :width], gate_up_ref[...], 1, 0)
        gate, up = hid[:, :units], hid[:, units:]
        tail = all_ref[at, width:].astype(F32)
        weights = [
            jnp.sum(
                jnp.where((lane == first + j) | (lane == experts + first + j), tail, 0.0),
                axis=1,
                keepdims=True,
            )
            for j in range(owned)
        ]
        weight = weights[0]
        for j in range(1, owned):
            weight = jnp.where(unit >= j * hidden, weights[j], weight)
        sigmoid = 1.0 / (1.0 + jnp.exp(-gate))
        activated = gate * sigmoid
        inner = activated * up
        weighted = (inner * weight).astype(LOW)

        @pl.when(i >= 2)
        def _():
            store(i - 2).wait()

        outgoing[i % 2] = dot(weighted, down_ref[...], 1, 0).astype(LOW)
        store(i).start()
        fetch(i).wait()

        @pl.when(i + 1 < count)
        def _():
            fetch(i + 1).start()

        u = upstream[i % 2]
        down_back = dot(u, down_ref[...], 1, 1)
        down_grad_ref[...] += dot(weighted, u, 0, 0)
        product = inner * down_back
        note = jnp.zeros((group, extra), F32)
        for j in range(owned):
            mine = (unit >= j * hidden) & (unit < (j + 1) * hidden)
            route_grad = jnp.sum(jnp.where(mine, product, 0.0), axis=1, keepdims=True)
            note = jnp.where(lane == first + j, route_grad, note)
        inner_grad = down_back * weight
        gate_back = (inner_grad * up * sigmoid * (1.0 + gate * (1.0 - sigmoid))).astype(LOW)
        up_back = (inner_grad * activated).astype(LOW)
        back_rows[at, :units] = gate_back
        back_rows[at, units:] = up_back
        part[at, :width] = (
            dot(gate_back, gate_up_ref[:, :units], 1, 1) + dot(up_back, gate_up_ref[:, units:], 1, 1)
        ).astype(LOW)
        part[at, width:] = note.astype(LOW)

    for there, _ in heads_line:
        there.start()
    tile = width // count

    @pl.loop(0, count)
    def _(i):
        for k, step in enumerate(scattering):
            pl.when(i == k)(step)
        at = pl.ds(pl.multiple_of(i * tile, tile), tile)
        gate_up_grad_ref[at, :] = dot(all_ref[:, at], back_rows[...], 0, 0)

    gather_copies.finish()
    scatter_copies.finish()
    store(count - 2).wait()
    store(count - 1).wait()
    for _, back in heads_line:
        back.wait_recv()
    heads_copies.finish()


def run_experts(own, upstream_all, gate_up, down, heads, owned, experts, width, collective_id):
    rows, full = own.shape
    total = upstream_all.shape[0]
    units = down.shape[0]
    group = rows * lax.axis_size("tensor")
    return pl.pallas_call(
        functools.partial(experts_kernel, rows, width, experts, owned),
        out_shape=(
            jax.ShapeDtypeStruct((rows, full), F32),
            jax.ShapeDtypeStruct((total, width), LOW),
            jax.ShapeDtypeStruct((DEPTH, *heads.shape), LOW),
            jax.ShapeDtypeStruct((width, 2 * units), F32),
            jax.ShapeDtypeStruct((units, width), F32),
        ),
        in_specs=[VMEM_SPEC, ANY_SPEC, VMEM_SPEC, VMEM_SPEC, ANY_SPEC],
        out_specs=(VMEM_SPEC, ANY_SPEC, ANY_SPEC, VMEM_SPEC, VMEM_SPEC),
        scratch_shapes=[
            pltpu.VMEM((total, full), LOW),
            pltpu.VMEM((2, group, width), LOW),
            pltpu.VMEM((2, group, width), LOW),
            pltpu.VMEM((total, full), LOW),
            pltpu.VMEM((total, 2 * units), LOW),
        ]
        + scatter_scratch(rows, full)
        + semaphores(5, GATHER_SEMS, GATHER_SEMS, SCATTER_SEMS, SCATTER_SEMS, DEPTH, DEPTH),
        compiler_params=pltpu.CompilerParams(
            collective_id=collective_id, has_side_effects=True, vmem_limit_bytes=64000000
        ),
        name="experts",
    )(own, upstream_all, gate_up, down, heads)


def normed_rows(values):
    scale = lax.rsqrt(jnp.mean(values * values, axis=-1, keepdims=True) + EPSILON)
    return values * scale, scale


def turned(values):
    return pltpu.roll(values, values.shape[-1] // 2, values.ndim - 1)


def allowed_keys(count, length):
    row = lax.broadcasted_iota(jnp.int32, (count, count), 0)
    column = lax.broadcasted_iota(jnp.int32, (count, count), 1)
    return (column <= row) & (column < length)


def attention_probs(query, key, allowed):
    factor = query.shape[-1] ** (-0.5)
    scores = jnp.where(allowed, dot(query, key, 1, 1) * factor, NEGATIVE)
    expo = jnp.exp(scores - jnp.max(scores, axis=-1, keepdims=True))
    return expo / jnp.sum(expo, axis=-1, keepdims=True)


class Spread:
    def __init__(self, p, copies, slot):
        other = (1 - p.x) * 2 + p.c
        self.to_x = copies.make(slot(p.t), slot(p.t), p.at(x=1 - p.x))
        self.to_c = copies.make(slot(p.t), slot(p.t), p.at(c=1 - p.c))
        self.onward = copies.make(slot(other), slot(other), p.at(c=1 - p.c))

    def start(self):
        self.to_x.start()
        self.to_c.start()

    def forward(self):
        self.to_x.wait_recv()
        self.onward.start()

    def finish(self):
        self.to_c.wait_recv()
        self.onward.wait_recv()


SPREAD_SEMS = 3
TAIL_SEMS = 4 * SPREAD_SEMS + DEPTH + DEPTH + 2 + 2 * DEPTH + 1 + 3 + 3 + DEPTH


def tail_kernel(
    rows,
    length_ref,
    hidden_low_ref,
    hidden_grad_ref,
    hidden_ref,
    tokens_ref,
    xnorm1_ref,
    small_ref,
    moe_ref,
    heads_ref,
    line_heads_ref,
    query_ref,
    key_ref,
    value_ref,
    cosine_ref,
    sine_ref,
    attention_gain_ref,
    query_gain_ref,
    key_gain_ref,
    query_weight_ref,
    key_weight_ref,
    value_weight_ref,
    output_weight_ref,
    mixed_ref,
    tokens_grad_ref,
    output_grad_ref,
    packed_grad_ref,
    small_out_ref,
    hidden_all,
    hidden_line,
    line_heads,
    heads_grad,
    packed,
    packed_in,
    xnorm_in,
    weight_out,
    weight_in,
    output_out,
    output_in,
    key_sum,
    value_sum,
    back_part,
    back_in,
    moe,
    moe_own,
    small,
    small_in,
    small_side,
    small_line,
    core_in,
    diag_in,
    side_in,
    line_in,
    local_sems,
    send_sems,
    recv_sems,
    scatter_send,
    scatter_recv,
):
    p = Place()
    group, width = xnorm1_ref.shape
    units = query_ref.shape[1]
    size = cosine_ref.shape[1]
    count = units // size
    packed_width = packed.shape[1]
    share = width // (2 * DEPTH)
    length = length_ref[0]
    fetch = [
        pltpu.make_async_copy(moe_ref, moe, local_sems.at[0]),
        *[
            pltpu.make_async_copy(
                line_heads_ref.at[p.near(k)], line_heads.at[p.near(k)], local_sems.at[k]
            )
            for k in range(1, DEPTH)
        ],
    ]
    for copy in fetch:
        copy.start()
    enter(p.peers())
    copies = Copies(send_sems, recv_sems)
    scatter_copies = Copies(scatter_send, scatter_recv)
    scattering = scatter_steps(
        p, scatter_copies, rows, moe, core_in, diag_in, side_in, line_in, moe_own
    )
    xn, yn, cn = p.at(x=1 - p.x), p.at(y=1 - p.y), p.at(c=1 - p.c)
    order = [p.near(k) for k in reversed(range(DEPTH))]
    along = [p.at(z=z) for z in order[: DEPTH - 1]]

    def columns(z, y):
        return pl.ds(pl.multiple_of((z * 2 + y) * share, share), share)

    def block(ref, t):
        return ref.at[pl.ds(pl.multiple_of(t * rows, rows), rows)]

    hidden_spread = Spread(p, copies, lambda t: block(hidden_all, t))
    line_spread = Spread(p, copies, lambda t: hidden_line.at[t])
    hidden_to = copies.along(
        [
            (
                z,
                hidden_low_ref.at[:, pl.ds(pl.multiple_of(z * 2 * share, share), 2 * share)],
                hidden_line.at[p.t, p.z],
            )
            for z in order[: DEPTH - 1]
        ],
        along,
        p.z,
    )
    xnorm_to = [
        copies.make(xnorm1_ref.at[:, columns(z, 1 - p.y)], xnorm_in.at[z], yn) for z in range(DEPTH)
    ]
    cuts = [(0, units // 2), (units // 2, packed_width)]
    packed_to = [copies.make(packed.at[:, a:b], packed_in.at[:, a:b], yn) for a, b in cuts]
    weight_to = [
        copies.along(
            [
                (order[k], weight_out.at[k, :, a:b], weight_in.at[p.z, :, a:b])
                for k in range(DEPTH - 1)
            ],
            along,
            p.z,
        )
        for a, b in cuts
    ]
    output_to = copies.make(output_out, output_in, yn)
    other = (1 - p.x) * 2 + p.c
    back_to_c = [
        copies.make(block(back_part, (1 - p.x) * 2 + 1 - p.c), back_in.at[0], cn),
        copies.make(block(back_part, p.x * 2 + 1 - p.c), back_in.at[1], cn),
    ]
    back_to_x = copies.make(block(back_part, other), back_in.at[2], xn)
    tokens_spread = Spread(p, copies, lambda t: block(tokens_grad_ref, t))
    mixed_spread = Spread(p, copies, lambda t: block(mixed_ref, t))
    small_to_c = copies.make(small, small_in.at[0], cn)
    small_to_x = copies.make(small, small_in.at[1], xn)
    small_to_y = copies.make(small_side.at[0], small_side.at[1], yn)
    small_to = copies.along(
        [(z, small_side.at[2, z], small_line.at[p.z]) for z in order[: DEPTH - 1]], along, p.z
    )

    block(hidden_all, p.t)[...] = hidden_low_ref[...]
    hidden_line[p.t, p.z] = hidden_low_ref[
        :, pl.ds(pl.multiple_of(p.z * 2 * share, share), 2 * share)
    ]
    for there, _ in hidden_to:
        there.start()
    hidden_spread.start()
    for copy in xnorm_to:
        copy.start()
    small[...] = small_ref[...]
    key_sum[...] = jnp.zeros_like(key_sum)
    value_sum[...] = jnp.zeros_like(value_sum)
    fetch[0].wait()
    scattering[0]()
    hidden_spread.forward()
    scattering[1]()
    hidden_spread.finish()

    valid = lax.broadcasted_iota(jnp.int32, (group, 1), 0) < length
    allowed = allowed_keys(group, length)
    heads_grad[...] = jnp.where(
        valid, dot(hidden_all[...], output_weight_ref[...], 1, 0), 0.0
    ).astype(LOW)
    cosine, sine = cosine_ref[...], sine_ref[...]
    query_gain, key_gain = query_gain_ref[...], key_gain_ref[...]
    factor = size ** (-0.5)
    key_hat, key_scale = normed_rows(key_ref[...])
    key_gained = key_hat * key_gain
    key_low = (key_gained * cosine + turned(key_gained) * sine).astype(LOW)
    gain_row = 2 * DEPTH * 2 + 2

    def norm_back(grad, hat, scale, gain):
        grad = grad * cosine - turned(grad) * sine
        gain_part = jnp.sum(grad * hat, axis=0, keepdims=True)
        inner = grad * gain
        return scale * (inner - hat * jnp.mean(inner * hat, axis=-1, keepdims=True)), gain_part

    def one_head(h):
        at = pl.ds(pl.multiple_of(h * size, size), size)
        hat, scale = normed_rows(query_ref[:, at])
        gained = hat * query_gain
        query_low = (gained * cosine + turned(gained) * sine).astype(LOW)
        probs = attention_probs(query_low, key_low, allowed)
        grad = heads_grad[:, at]
        probs_grad = dot(grad, value_ref[...], 1, 1)
        delta = jnp.sum(probs * probs_grad, axis=-1, keepdims=True)
        score_grad = (probs * (probs_grad - delta)).astype(LOW)
        key_sum[...] += dot(score_grad, query_low, 0, 0)
        value_sum[...] += dot(probs.astype(LOW), grad, 0, 0)
        back, gain_part = norm_back(
            dot(score_grad, key_low, 1, 0) * factor, hat, scale, query_gain
        )
        packed[:, at] = back.astype(LOW)
        small[gain_row : gain_row + 1, :size] += gain_part

    pl.loop(0, count // 2)(one_head)
    packed_to[0].start()
    scattering[2]()
    for _, back in hidden_to:
        back.wait_recv()
    line_spread.start()
    pl.loop(count // 2, count)(one_head)
    key_back, key_part = norm_back(key_sum[...] * factor, key_hat, key_scale, key_gain)
    packed[:, units : units + size] = key_back.astype(LOW)
    packed[:, units + size :] = value_sum[...].astype(LOW)
    packed_to[1].start()
    small[gain_row + 1 : gain_row + 2, :size] = key_part
    for row in (gain_row, gain_row + 1):
        part = small[row : row + 1, :size]
        for i in range(1, width // size):
            small[row : row + 1, i * size : (i + 1) * size] = part
    line_spread.forward()
    scattering[3]()
    back_part[...] = (
        dot(packed[:, :units], query_weight_ref[...], 1, 1)
        + dot(packed[:, units : units + size], key_weight_ref[...], 1, 1)
        + dot(packed[:, units + size :], value_weight_ref[...], 1, 1)
    ).astype(LOW)
    for copy in back_to_c:
        copy.start()
    for copy in xnorm_to:
        copy.wait_recv()

    def weight_piece(i):
        a, b = cuts[i]
        packed_to[i].wait_recv()
        for k, z in enumerate(order):
            grad = dot(xnorm1_ref[:, columns(z, p.y)], packed[:, a:b], 0, 0) + dot(
                xnorm_in[z], packed_in[:, a:b], 0, 0
            )
            if k < DEPTH - 1:
                weight_out[k, :, a:b] = grad.astype(LOW)
                weight_to[i][k][0].start()
            else:
                packed_grad_ref[:, a:b] = grad

    weight_piece(0)
    back_to_c[0].wait_recv()
    there = block(back_part, other)
    there[...] = (there[...].astype(F32) + back_in[0].astype(F32)).astype(LOW)
    back_to_x.start()
    scattering[4]()
    weight_piece(1)
    scattering[5]()

    back_to_c[1].wait_recv()
    back_to_x.wait_recv()
    xnorm1_grad = (
        block(back_part, p.t)[...].astype(F32) + back_in[1].astype(F32) + back_in[2].astype(F32)
    )
    normed1, scale1 = normed_rows(tokens_ref[...].astype(F32))
    small[gain_row - 1 : gain_row, :] = jnp.sum(xnorm1_grad * normed1, axis=0, keepdims=True)
    small_to_c.start()
    inner = xnorm1_grad * attention_gain_ref[...]
    block(tokens_grad_ref, p.t)[...] = (
        hidden_grad_ref[...]
        + scale1 * (inner - normed1 * jnp.mean(inner * normed1, axis=-1, keepdims=True))
    ).astype(LOW)
    tokens_spread.start()

    line_spread.finish()
    for copy in fetch[1:]:
        copy.wait()

    def output_piece(y):
        at = pl.ds(pl.multiple_of(y * share, share), share)
        grad = dot(hidden_line[:, p.z, :, at].reshape(group, share), heads_ref[...], 0, 0)
        for k in range(1, DEPTH):
            z = p.near(k)
            grad += dot(hidden_line[:, z, :, at].reshape(group, share), line_heads[z], 0, 0)
        return grad

    output_out[...] = output_piece(1 - p.y).astype(LOW)
    output_to.start()
    output_grad_ref[...] = output_piece(p.y)
    scattering[6]()
    small_to_c.wait_recv()
    small_to_c.wait_send()
    small[...] += small_in[0]
    small_to_x.start()
    tokens_spread.forward()
    scattering[7]()
    block(mixed_ref, p.t)[...] = (hidden_ref[...] + moe_own[...]).astype(LOW)
    mixed_spread.start()
    small_to_x.wait_recv()
    small_to_x.wait_send()
    small[...] += small_in[1]
    for z in range(DEPTH):
        small_side[0, z] = small[:, columns(z, 1 - p.y)]
        small_side[2, z] = small[:, columns(z, p.y)]
    small_to_y.start()
    output_to.wait_recv()
    output_grad_ref[...] += output_in[...].astype(F32)
    small_to_y.wait_recv()
    small_side[2] += small_side[1]
    for there, _ in small_to:
        there.start()
    mixed_spread.forward()
    tokens_spread.finish()
    small_total = small_side[2, p.z]
    for (_, back), z in zip(small_to, order):
        back.wait_recv()
        small_total += small_line[z]
    small_out_ref[...] = small_total
    mixed_spread.finish()
    for i, (a, b) in enumerate(cuts):
        grad = packed_grad_ref[:, a:b]
        for (_, back), z in zip(weight_to[i], order):
            back.wait_recv()
            grad += weight_in[z, :, a:b].astype(F32)
        packed_grad_ref[:, a:b] = grad
    for copy in copies.made:
        if copy is not small_to_c and copy is not small_to_x:
            copy.wait_send()
    scatter_copies.finish()


def run_tail(
    length,
    hidden_low,
    hidden_grad,
    hidden,
    tokens,
    xnorm1,
    small,
    moe,
    heads,
    line_heads,
    query,
    key,
    value,
    cosine,
    sine,
    attention_gain,
    query_gain,
    key_gain,
    query_weight,
    key_weight,
    value_weight,
    output_weight,
    collective_id,
):
    group, width = xnorm1.shape
    rows = hidden_low.shape[0]
    units, size = query.shape[1], cosine.shape[1]
    packed_width = units + 2 * size
    share = width // (2 * DEPTH)
    tensors = group // rows
    vmem = pltpu.VMEM
    return pl.pallas_call(
        functools.partial(tail_kernel, rows),
        out_shape=(
            jax.ShapeDtypeStruct((group, width), LOW),
            jax.ShapeDtypeStruct((group, width), LOW),
            jax.ShapeDtypeStruct((share, units), F32),
            jax.ShapeDtypeStruct((share, packed_width), F32),
            jax.ShapeDtypeStruct((small.shape[0], share), F32),
        ),
        in_specs=[pl.BlockSpec(memory_space=pltpu.SMEM)]
        + [VMEM_SPEC] * 6
        + [ANY_SPEC, VMEM_SPEC, ANY_SPEC]
        + [VMEM_SPEC] * 12,
        out_specs=[VMEM_SPEC] * 5,
        scratch_shapes=[
            vmem((group, width), LOW),
            vmem((tensors, DEPTH, rows, 2 * share), LOW),
            vmem((DEPTH, group, units), LOW),
            vmem((group, units), LOW),
            vmem((group, packed_width), LOW),
            vmem((group, packed_width), LOW),
            vmem((DEPTH, group, share), LOW),
            vmem((DEPTH - 1, share, packed_width), LOW),
            vmem((DEPTH, share, packed_width), LOW),
            vmem((share, units), LOW),
            vmem((share, units), LOW),
            vmem((group, size), F32),
            vmem((group, size), F32),
            vmem((group, width), LOW),
            vmem((3, rows, width), LOW),
            vmem(moe.shape, LOW),
            vmem((rows, width), F32),
            vmem(small.shape, F32),
            vmem((2, *small.shape), F32),
            vmem((3, DEPTH, small.shape[0], share), F32),
            vmem((DEPTH, small.shape[0], share), F32),
        ]
        + scatter_scratch(rows, width)
        + semaphores(DEPTH, TAIL_SEMS, TAIL_SEMS, SCATTER_SEMS, SCATTER_SEMS),
        compiler_params=pltpu.CompilerParams(
            collective_id=collective_id, has_side_effects=True, vmem_limit_bytes=64000000
        ),
        name="tail",
    )(
        length,
        hidden_low,
        hidden_grad,
        hidden,
        tokens,
        xnorm1,
        small,
        moe,
        heads,
        line_heads,
        query,
        key,
        value,
        cosine,
        sine,
        attention_gain,
        query_gain,
        key_gain,
        query_weight,
        key_weight,
        value_weight,
        output_weight,
    )


def gathered_shards(
    tokens,
    seq_length,
    expert_routes,
    attention_gain,
    query_weight,
    key_weight,
    value_weight,
    query_gain,
    key_gain,
    output_weight,
    routing_gain,
    router_weight,
    gate_weight,
    up_weight,
    down_weight,
    cotangent,
):
    count, width = tokens.shape
    head_size = query_gain.shape[0]
    local_heads = query_weight.shape[1] // head_size
    local_groups = key_weight.shape[1] // head_size
    ratio = local_heads // local_groups
    length = seq_length[0]
    experts = router_weight.shape[1]
    owned = gate_weight.shape[0]
    parts = lax.axis_size("tensor")
    part = lax.axis_index("tensor")
    owner = lax.axis_index("expert")
    rows = count // parts
    everywhere = ("expert", "tensor")
    low = jnp.bfloat16

    def own_rows(values):
        return lax.dynamic_slice_in_dim(values, part * rows, rows, 0)

    upstream_all = gather_rows(own_rows(cotangent), 0)
    inputs = tokens.astype(jnp.float32)
    scale1 = rms_scale(inputs)
    normed1 = inputs * scale1
    xnorm1 = (normed1 * attention_gain).astype(low)
    query_flat = jnp.dot(xnorm1, query_weight, preferred_element_type=jnp.float32)
    key_flat = jnp.dot(xnorm1, key_weight, preferred_element_type=jnp.float32)
    value_flat = jnp.dot(xnorm1, value_weight, preferred_element_type=jnp.float32).astype(low)
    query_raw = query_flat.reshape(count, local_heads, head_size)
    key_raw = key_flat.reshape(count, local_groups, head_size)
    value_low = value_flat.reshape(count, local_groups, head_size)
    query_gained, query_normed, query_scale = head_norm(query_raw, query_gain)
    key_gained, key_normed, key_scale = head_norm(key_raw, key_gain)
    cosine, sine = rope_tables(count, head_size)
    query_low = rotate(query_gained, cosine, sine).astype(low)
    key_low = rotate(key_gained, cosine, sine).astype(low)
    query_block = query_low.reshape(count, local_groups, ratio, head_size)
    outputs, _ = attend_block(query_block, 0, key_low, value_low, length)
    valid = (jnp.arange(count, dtype=jnp.int32) < length)[:, None]
    heads_low = jnp.where(valid, outputs.reshape(count, local_heads * head_size), 0.0).astype(low)
    attention_part = contract(heads_low, output_weight, 1, 1)
    attention = lax.psum_scatter(
        attention_part.astype(low), "tensor", scatter_dimension=0, tiled=True
    ).astype(jnp.float32)

    hidden = own_rows(inputs) + attention
    scale2 = rms_scale(hidden)
    normed2 = hidden * scale2
    xnorm2 = (normed2 * routing_gain).astype(low)
    logits = jnp.dot(xnorm2, router_weight, preferred_element_type=jnp.float32)
    peak = jnp.max(logits, axis=1, keepdims=True)
    expo = jnp.exp(logits - peak)
    router = expo / jnp.sum(expo, axis=1, keepdims=True)
    routes = own_rows(expert_routes)
    named = jnp.any(
        routes[:, :, None] == jnp.arange(experts, dtype=jnp.int32)[None, None, :], axis=1
    )
    chosen = jnp.where(named, router, 0.0)
    chosen_total = jnp.sum(chosen, axis=1, keepdims=True)
    route_weight = chosen / chosen_total

    high = route_weight.astype(low)
    rest = (route_weight - high.astype(jnp.float32)).astype(low)
    spare = jnp.zeros((rows, 128 - 2 * experts), low)
    own = jnp.concatenate([xnorm2, high, rest, spare], axis=1)
    gate_up = jnp.concatenate([*gate_weight, *up_weight], axis=1)
    summed, moe_part, line_heads, gate_up_grad, down_grad = run_experts(
        own,
        upstream_all,
        gate_up,
        down_weight.reshape(-1, width),
        heads_low,
        owned,
        experts,
        width,
        1,
    )
    units = gate_up.shape[1] // (2 * owned)
    split = [gate_up_grad[:, j * units : (j + 1) * units] for j in range(2 * owned)]
    gate_grad, up_grad = jnp.stack(split[:owned]), jnp.stack(split[owned:])
    down_grad = down_grad.reshape(down_weight.shape)
    xnorm2_moe, route_grad = summed[:, :width], summed[:, width : width + experts]

    upstream = own_rows(cotangent).astype(jnp.float32)
    inner_total = jnp.sum(route_grad * route_weight, axis=1, keepdims=True)
    prob_grad = jnp.where(named, (route_grad - inner_total) / chosen_total, 0.0)
    logit_low = (router * (prob_grad - jnp.sum(router * prob_grad, axis=1, keepdims=True))).astype(
        low
    )
    router_part = contract(logit_low, xnorm2, 0, 0)
    xnorm2_grad = xnorm2_moe + contract(logit_low, router_weight, 1, 1)
    routing_gain_part = jnp.sum(xnorm2_grad * normed2, axis=0)
    inner2 = xnorm2_grad * routing_gain
    hidden_grad = upstream + scale2 * (
        inner2 - normed2 * jnp.mean(inner2 * normed2, axis=1, keepdims=True)
    )
    small = jnp.concatenate(
        [router_part, routing_gain_part[None], jnp.zeros((7, width), jnp.float32)], axis=0
    )
    half = head_size // 2
    mixed, tokens_grad, output_grad, packed_grad, small_sum = run_tail(
        seq_length,
        hidden_grad.astype(low),
        hidden_grad,
        hidden,
        own_rows(tokens),
        xnorm1,
        small,
        moe_part,
        heads_low,
        line_heads,
        query_flat,
        key_flat,
        value_flat,
        cosine,
        jnp.concatenate([-sine[:, :half], sine[:, half:]], axis=1),
        attention_gain[None],
        query_gain[None],
        key_gain[None],
        query_weight,
        key_weight,
        value_weight,
        output_weight,
        2,
    )
    query_end = local_heads * head_size
    key_end = query_end + local_groups * head_size
    share = head_size // lax.axis_size("expert")

    def own_gain(row):
        return lax.dynamic_slice_in_dim(small_sum[row], owner * share, share, 0)

    return (
        mixed,
        tokens_grad,
        small_sum[experts + 1],
        packed_grad[:, :query_end],
        packed_grad[:, query_end:key_end],
        packed_grad[:, key_end:],
        own_gain(experts + 2),
        own_gain(experts + 3),
        output_grad,
        small_sum[experts],
        small_sum[:experts].T,
        gate_grad,
        up_grad,
        down_grad,
    )


def solution(mesh):
    sizes = dict(mesh.shape)
    fits = sizes["expert"] == 2 * DEPTH and sizes["tensor"] == 4
    return jax.shard_map(
        gathered_shards if fits else routed_shards,
        mesh=mesh,
        in_specs=(
            P("expert", None),
            P("expert"),
            P("expert", None),
            P(),
            P(None, "tensor"),
            P(None, "tensor"),
            P(None, "tensor"),
            P(),
            P(),
            P(None, "tensor"),
            P(),
            P(),
            P("expert", None, "tensor"),
            P("expert", None, "tensor"),
            P("expert", "tensor", None),
            P("expert", None),
        ),
        out_specs=(
            P("expert", None),
            P("expert", None),
            P("expert"),
            P("expert", "tensor"),
            P("expert", "tensor"),
            P("expert", "tensor"),
            P("expert"),
            P("expert"),
            P("expert", "tensor"),
            P("expert"),
            P("expert", None),
            P("expert", None, "tensor"),
            P("expert", None, "tensor"),
            P("expert", "tensor", None),
        ),
        check_vma=False,
    )
```

```python
import functools

import jax
import jax.numpy as jnp
from jax import lax
from jax.experimental import pallas as pl
from jax.experimental.pallas import tpu as pltpu
from jax.sharding import PartitionSpec as P

EPSILON = 1e-06
THETA = 1000000.0
NEGATIVE = -1e30


def rms_scale(values):
    return lax.rsqrt(jnp.mean(values * values, axis=-1, keepdims=True) + EPSILON)


def rope_tables(count, width):
    half = width // 2
    freqs = THETA ** (-(jnp.arange(half, dtype=jnp.float32) * 2.0 / width))
    angles = jnp.arange(count, dtype=jnp.float32)[:, None] * freqs[None, :]
    cosine = jnp.concatenate([jnp.cos(angles), jnp.cos(angles)], axis=1)
    sine = jnp.concatenate([jnp.sin(angles), jnp.sin(angles)], axis=1)
    return (cosine, sine)


def rotate(values, cosine, sine):
    half = values.shape[-1] // 2
    turned = jnp.concatenate([-values[..., half:], values[..., :half]], axis=-1)
    return values * cosine[:, None, :] + turned * sine[:, None, :]


def rotate_back(grads, cosine, sine):
    half = grads.shape[-1] // 2
    scaled = grads * sine[:, None, :]
    turned = jnp.concatenate([scaled[..., half:], -scaled[..., :half]], axis=-1)
    return grads * cosine[:, None, :] + turned


def head_norm(values, gain):
    scale = rms_scale(values)
    normed = values * scale
    return (normed * gain, normed, scale)


def head_norm_back(grads, normed, scale, gain):
    gain_grad = jnp.sum(grads * normed, axis=(0, 1))
    inner = grads * gain
    values_grad = scale * (inner - normed * jnp.mean(inner * normed, axis=-1, keepdims=True))
    return (values_grad, gain_grad)


def contract(left, right, left_dim, right_dim):
    return lax.dot_general(
        left, right, (((left_dim,), (right_dim,)), ((), ())), preferred_element_type=jnp.float32
    )


def block_scores(qblock, start, keys, length):
    block = qblock.shape[0]
    count = keys.shape[0]
    factor = qblock.shape[-1] ** (-0.5)
    rows = start + jnp.arange(block, dtype=jnp.int32)
    columns = jnp.arange(count, dtype=jnp.int32)
    allowed = (columns[None, :] <= rows[:, None]) & (columns[None, :] < length)
    scores = jnp.einsum("qagh,kah->agqk", qblock, keys, preferred_element_type=jnp.float32) * factor
    return (jnp.where(allowed[None, None, :, :], scores, NEGATIVE), factor)


def attend_block(qblock, start, keys, values, length):
    scores, factor = block_scores(qblock, start, keys, length)
    peak = jnp.max(scores, axis=-1, keepdims=True)
    expo = jnp.exp(scores - peak)
    total = jnp.sum(expo, axis=-1, keepdims=True)
    probs_low = (expo / total).astype(jnp.bfloat16)
    output = jnp.einsum("agqk,kah->qagh", probs_low, values, preferred_element_type=jnp.float32)
    return (output, (peak + jnp.log(total))[..., 0])


def attend_back(qblock, dblock, lse_block, start, keys, values, length):
    scores, factor = block_scores(qblock, start, keys, length)
    probs = jnp.exp(scores - lse_block[..., None])
    probs_grad = jnp.einsum("qagh,kah->agqk", dblock, values, preferred_element_type=jnp.float32)
    delta = jnp.sum(probs * probs_grad, axis=-1, keepdims=True)
    score_grad = (probs * (probs_grad - delta)).astype(jnp.bfloat16)
    query_grad = (
        jnp.einsum("agqk,kah->qagh", score_grad, keys, preferred_element_type=jnp.float32) * factor
    )
    key_grad = (
        jnp.einsum("agqk,qagh->kah", score_grad, qblock, preferred_element_type=jnp.float32)
        * factor
    )
    value_grad = jnp.einsum(
        "agqk,qagh->kah", probs.astype(jnp.bfloat16), dblock, preferred_element_type=jnp.float32
    )
    return (query_grad, key_grad, value_grad)


def routed_shards(
    tokens,
    seq_length,
    expert_routes,
    attention_gain,
    query_weight,
    key_weight,
    value_weight,
    query_gain,
    key_gain,
    output_weight,
    routing_gain,
    router_weight,
    gate_weight,
    up_weight,
    down_weight,
    cotangent,
):
    count = tokens.shape[0]
    width = tokens.shape[1]
    head_size = query_gain.shape[0]
    local_heads = query_weight.shape[1] // head_size
    local_groups = key_weight.shape[1] // head_size
    ratio = local_heads // local_groups
    length = seq_length[0]
    experts = router_weight.shape[1]
    top = expert_routes.shape[1]
    owned = gate_weight.shape[0]
    sources = experts // owned
    parts = lax.axis_size("tensor")
    part = lax.axis_index("tensor")
    quarter = (count * top * 5 + 16 * experts - 1) // (16 * experts)
    inputs = tokens.astype(jnp.float32)
    scale1 = rms_scale(inputs)
    normed1 = inputs * scale1
    xnorm1 = (normed1 * attention_gain).astype(jnp.bfloat16)
    query_raw = jnp.dot(xnorm1, query_weight, preferred_element_type=jnp.float32).reshape(
        count, local_heads, head_size
    )
    key_raw = jnp.dot(xnorm1, key_weight, preferred_element_type=jnp.float32).reshape(
        count, local_groups, head_size
    )
    value_low = (
        jnp.dot(xnorm1, value_weight, preferred_element_type=jnp.float32)
        .astype(jnp.bfloat16)
        .reshape(count, local_groups, head_size)
    )
    query_gained, query_normed, query_scale = head_norm(query_raw, query_gain)
    key_gained, key_normed, key_scale = head_norm(key_raw, key_gain)
    cosine, sine = rope_tables(count, head_size)
    query_low = rotate(query_gained, cosine, sine).astype(jnp.bfloat16)
    key_low = rotate(key_gained, cosine, sine).astype(jnp.bfloat16)
    block = min(512, count)
    blocks = count // block
    starts = jnp.arange(blocks, dtype=jnp.int32) * block
    query_blocks = query_low.reshape(blocks, block, local_groups, ratio, head_size)

    def forward_block(item):
        qblock, start = item
        return attend_block(qblock, start, key_low, value_low, length)

    outputs, lse = lax.map(forward_block, (query_blocks, starts))
    valid = (jnp.arange(count, dtype=jnp.int32) < length)[:, None]
    heads_low = jnp.where(valid, outputs.reshape(count, local_heads * head_size), 0.0).astype(
        jnp.bfloat16
    )
    attention_part = contract(heads_low, output_weight, 1, 1)
    attention_full = lax.psum(attention_part, "tensor")
    hidden = inputs + attention_full
    scale2 = rms_scale(hidden)
    normed2 = hidden * scale2
    xnorm2 = (normed2 * routing_gain).astype(jnp.bfloat16)
    logits = jnp.dot(xnorm2, router_weight, preferred_element_type=jnp.float32)
    peak = jnp.max(logits, axis=1, keepdims=True)
    expo = jnp.exp(logits - peak)
    router = expo / jnp.sum(expo, axis=1, keepdims=True)
    onehot = expert_routes[:, :, None] == jnp.arange(experts, dtype=jnp.int32)[None, None, :]
    chosen = jnp.sum(jnp.where(onehot, router[:, None, :], 0.0), axis=-1)
    chosen_total = jnp.sum(chosen, axis=1, keepdims=True)
    route_weight = chosen / chosen_total
    flat_routes = expert_routes.reshape(-1)
    hits = (flat_routes[:, None] == jnp.arange(experts, dtype=jnp.int32)[None, :]).astype(jnp.int32)
    ranks = jnp.sum((jnp.cumsum(hits, axis=0) - 1) * hits, axis=1)
    mine = ranks % parts == part
    slot_index = jnp.where(mine, ranks // parts * experts + flat_routes, quarter * experts)
    table = (
        jnp.full((quarter * experts,), count * top, jnp.int32)
        .at[slot_index]
        .set(jnp.arange(count * top, dtype=jnp.int32), mode="drop")
    )
    slot_token = table // top
    send_rows = jnp.take(xnorm2, slot_token, axis=0, mode="fill", fill_value=0).reshape(
        quarter, experts, width
    )
    arrived = lax.all_to_all(send_rows, "expert", split_axis=1, concat_axis=1, tiled=True)
    gate_full, up_full, down_full = (
        lax.all_gather(gate_weight, "tensor", axis=2, tiled=True),
        lax.all_gather(up_weight, "tensor", axis=2, tiled=True),
        lax.all_gather(down_weight, "tensor", axis=1, tiled=True),
    )
    rows_own = arrived.reshape(quarter, sources, owned, width)
    gate_val = jnp.einsum("csjd,jdf->csjf", rows_own, gate_full, preferred_element_type=jnp.float32)
    up_val = jnp.einsum("csjd,jdf->csjf", rows_own, up_full, preferred_element_type=jnp.float32)
    sigmoid_gate = jax.nn.sigmoid(gate_val)
    activated = gate_val * sigmoid_gate
    inner_low = (activated * up_val).astype(jnp.bfloat16)
    expert_total = jnp.einsum(
        "csjf,jfd->csjd", inner_low, down_full, preferred_element_type=jnp.float32
    )
    expert_low = expert_total.astype(jnp.bfloat16).reshape(quarter, experts, width)
    returned = lax.all_to_all(
        expert_low, "expert", split_axis=1, concat_axis=1, tiled=True
    ).reshape(quarter * experts, width)
    picked = jnp.take(returned, slot_index, axis=0, mode="fill", fill_value=0).reshape(
        count, top, width
    )
    mine_rows = mine.reshape(count, top)
    mine_weight = jnp.where(mine_rows, route_weight, 0.0)
    moe_part = jnp.sum(mine_weight[:, :, None] * picked, axis=1)
    moe_full = lax.psum(moe_part.astype(jnp.bfloat16), "tensor").astype(jnp.float32)
    mixed = (hidden + moe_full).astype(jnp.bfloat16)
    upstream = cotangent.astype(jnp.float32)
    route_grad_part = jnp.where(mine_rows, jnp.sum(picked * upstream[:, None, :], axis=-1), 0.0)
    slot_weight = jnp.take(route_weight.reshape(-1), table, mode="fill", fill_value=0.0)
    grad_send = (
        jnp.take(cotangent, slot_token, axis=0, mode="fill", fill_value=0) * slot_weight[:, None]
    ).astype(jnp.bfloat16)
    grad_arrived = lax.all_to_all(
        grad_send.reshape(quarter, experts, width),
        "expert",
        split_axis=1,
        concat_axis=1,
        tiled=True,
    )
    grad_own = grad_arrived.reshape(quarter, sources, owned, width)
    down_part = jnp.einsum(
        "csjf,csjd->jfd", inner_low, grad_own, preferred_element_type=jnp.float32
    )
    inner_grad = jnp.einsum(
        "csjd,jfd->csjf", grad_own, down_full, preferred_element_type=jnp.float32
    )
    gate_grad_low = (
        inner_grad * up_val * sigmoid_gate * (1.0 + gate_val * (1.0 - sigmoid_gate))
    ).astype(jnp.bfloat16)
    up_grad_low = (inner_grad * activated).astype(jnp.bfloat16)
    gate_part = jnp.einsum(
        "csjd,csjf->jdf", rows_own, gate_grad_low, preferred_element_type=jnp.float32
    )
    up_part = jnp.einsum(
        "csjd,csjf->jdf", rows_own, up_grad_low, preferred_element_type=jnp.float32
    )
    rows_grad = jnp.einsum(
        "csjf,jdf->csjd", gate_grad_low, gate_full, preferred_element_type=jnp.float32
    )
    rows_grad = rows_grad + jnp.einsum(
        "csjf,jdf->csjd", up_grad_low, up_full, preferred_element_type=jnp.float32
    )
    gate_grad, up_grad, down_grad = (
        lax.psum_scatter(
            gate_part.astype(jnp.bfloat16), "tensor", scatter_dimension=2, tiled=True
        ).astype(jnp.float32),
        lax.psum_scatter(
            up_part.astype(jnp.bfloat16), "tensor", scatter_dimension=2, tiled=True
        ).astype(jnp.float32),
        lax.psum_scatter(
            down_part.astype(jnp.bfloat16), "tensor", scatter_dimension=1, tiled=True
        ).astype(jnp.float32),
    )
    rows_grad_low = rows_grad.astype(jnp.bfloat16).reshape(quarter, experts, width)
    returned_grad = lax.all_to_all(
        rows_grad_low, "expert", split_axis=1, concat_axis=1, tiled=True
    ).reshape(quarter * experts, width)
    route_rows = jnp.take(returned_grad, slot_index, axis=0, mode="fill", fill_value=0).reshape(
        count, top, width
    )
    xnorm2_part = jnp.sum(route_rows, axis=1, dtype=jnp.float32)
    xnorm2_moe, route_grad = (
        lax.psum(xnorm2_part.astype(jnp.bfloat16), "tensor").astype(jnp.float32),
        lax.psum(route_grad_part.astype(jnp.bfloat16), "tensor").astype(jnp.float32),
    )
    inner_total = jnp.sum(route_grad * route_weight, axis=1, keepdims=True)
    chosen_grad = (route_grad - inner_total) / chosen_total
    prob_grad = jnp.sum(jnp.where(onehot, chosen_grad[:, :, None], 0.0), axis=1)
    logit_low = (router * (prob_grad - jnp.sum(router * prob_grad, axis=1, keepdims=True))).astype(
        jnp.bfloat16
    )
    router_grad = contract(xnorm2, logit_low, 0, 0)
    xnorm2_grad = xnorm2_moe + contract(logit_low, router_weight, 1, 1)
    routing_gain_part = jnp.sum(xnorm2_grad * normed2, axis=0)
    inner2 = xnorm2_grad * routing_gain
    hidden_grad = upstream + scale2 * (
        inner2 - normed2 * jnp.mean(inner2 * normed2, axis=1, keepdims=True)
    )
    hidden_low = hidden_grad.astype(jnp.bfloat16)
    output_grad = contract(hidden_low, heads_low, 0, 0)
    heads_grad = jnp.where(
        valid,
        jnp.dot(hidden_low, output_weight, preferred_element_type=jnp.float32).astype(jnp.bfloat16),
        jnp.zeros((), jnp.bfloat16),
    )
    grad_blocks = heads_grad.reshape(blocks, block, local_groups, ratio, head_size)

    def backward_block(carry, item):
        key_acc, value_acc = carry
        qblock, dblock, lse_block, start = item
        query_piece, key_piece, value_piece = attend_back(
            qblock, dblock, lse_block, start, key_low, value_low, length
        )
        return ((key_acc + key_piece, value_acc + value_piece), query_piece)

    empty = jnp.zeros((count, local_groups, head_size), jnp.float32)
    (key_rot_grad, value_grad), query_rot_grad = lax.scan(
        backward_block, (empty, empty), (query_blocks, grad_blocks, lse, starts)
    )
    query_back, query_gain_part = head_norm_back(
        rotate_back(query_rot_grad.reshape(count, local_heads, head_size), cosine, sine),
        query_normed,
        query_scale,
        query_gain,
    )
    key_back, key_gain_part = head_norm_back(
        rotate_back(key_rot_grad, cosine, sine), key_normed, key_scale, key_gain
    )
    query_grad_low = query_back.reshape(count, local_heads * head_size).astype(jnp.bfloat16)
    key_grad_low = key_back.reshape(count, local_groups * head_size).astype(jnp.bfloat16)
    value_grad_low = value_grad.reshape(count, local_groups * head_size).astype(jnp.bfloat16)
    query_wgrad = contract(xnorm1, query_grad_low, 0, 0)
    key_wgrad = contract(xnorm1, key_grad_low, 0, 0)
    value_wgrad = contract(xnorm1, value_grad_low, 0, 0)
    xnorm1_part = contract(query_grad_low, query_weight, 1, 1) + contract(
        key_grad_low, key_weight, 1, 1
    )
    xnorm1_part = xnorm1_part + contract(value_grad_low, value_weight, 1, 1)
    xnorm1_grad, query_gain_sum, key_gain_sum = (
        lax.psum(xnorm1_part.astype(jnp.bfloat16), "tensor").astype(jnp.float32),
        lax.psum(query_gain_part.astype(jnp.bfloat16), "tensor").astype(jnp.float32),
        lax.psum(key_gain_part.astype(jnp.bfloat16), "tensor").astype(jnp.float32),
    )
    attention_gain_part = jnp.sum(xnorm1_grad * normed1, axis=0)
    inner1 = xnorm1_grad * attention_gain
    tokens_grad = (
        hidden_grad
        + scale1 * (inner1 - normed1 * jnp.mean(inner1 * normed1, axis=1, keepdims=True))
    ).astype(jnp.bfloat16)
    summed = (
        lax.psum_scatter(
            attention_gain_part.astype(jnp.bfloat16), "expert", scatter_dimension=0, tiled=True
        ).astype(jnp.float32),
        lax.psum_scatter(
            query_wgrad.astype(jnp.bfloat16), "expert", scatter_dimension=0, tiled=True
        ).astype(jnp.float32),
        lax.psum_scatter(
            key_wgrad.astype(jnp.bfloat16), "expert", scatter_dimension=0, tiled=True
        ).astype(jnp.float32),
        lax.psum_scatter(
            value_wgrad.astype(jnp.bfloat16), "expert", scatter_dimension=0, tiled=True
        ).astype(jnp.float32),
        lax.psum_scatter(
            query_gain_sum.astype(jnp.bfloat16), "expert", scatter_dimension=0, tiled=True
        ).astype(jnp.float32),
        lax.psum_scatter(
            key_gain_sum.astype(jnp.bfloat16), "expert", scatter_dimension=0, tiled=True
        ).astype(jnp.float32),
        lax.psum_scatter(
            output_grad.astype(jnp.bfloat16), "expert", scatter_dimension=0, tiled=True
        ).astype(jnp.float32),
        lax.psum_scatter(
            routing_gain_part.astype(jnp.bfloat16), "expert", scatter_dimension=0, tiled=True
        ).astype(jnp.float32),
        lax.psum_scatter(
            router_grad.astype(jnp.bfloat16), "expert", scatter_dimension=0, tiled=True
        ).astype(jnp.float32),
    )
    return (
        mixed,
        tokens_grad,
        summed[0],
        summed[1],
        summed[2],
        summed[3],
        summed[4],
        summed[5],
        summed[6],
        summed[7],
        summed[8],
        gate_grad,
        up_grad,
        down_grad,
    )


MESH_ID = pl.DeviceIdType.MESH
DEPTH = 4
F32 = jnp.float32
LOW = jnp.bfloat16


class Place:
    def __init__(self):
        e, t = lax.axis_index("expert"), lax.axis_index("tensor")
        self.e, self.t = e, t
        self.z, self.y, self.x, self.c = e // 2, e % 2, t // 2, t % 2

    def at(self, z=None, y=None, x=None, c=None):
        z, y = self.z if z is None else z, self.y if y is None else y
        x, c = self.x if x is None else x, self.c if c is None else c
        return (z * 2 + y, x * 2 + c)

    def block(self, **where):
        e, t = self.at(**where)
        return e * 4 + t

    def near(self, k):
        table = ((0, 1, 2, 3), (1, 2, 0, 3), (2, 1, 3, 0), (3, 2, 1, 0))
        out = 0
        for z in range(DEPTH):
            if isinstance(k, int):
                column = table[z][k]
            else:
                column = table[z][0]
                for i in range(1, DEPTH):
                    column = jnp.where(k == i, table[z][i], column)
            out = jnp.where(self.z == z, column, out)
        return out

    def peers(self):
        line = [self.at(z=(self.z + d) % DEPTH) for d in range(1, DEPTH)]
        return line + [self.at(x=1 - self.x), self.at(y=1 - self.y), self.at(c=1 - self.c)]


class Copies:
    def __init__(self, send_sems, recv_sems):
        self.send_sems, self.recv_sems, self.used, self.made = send_sems, recv_sems, 0, []

    def make(self, src, dst, to):
        i = self.used
        self.used += 1
        copy = pltpu.make_async_remote_copy(
            src,
            dst,
            self.send_sems.at[i],
            self.recv_sems.at[i],
            device_id=to,
            device_id_type=MESH_ID,
        )
        self.made.append(copy)
        return copy

    def along(self, pieces, to, mine):
        base = self.used
        self.used += DEPTH
        out = []
        for (peer, src, dst), device in zip(pieces, to):
            there = pltpu.make_async_remote_copy(
                src,
                dst,
                self.send_sems.at[base + peer],
                self.recv_sems.at[base + mine],
                device_id=device,
                device_id_type=MESH_ID,
            )
            back = pltpu.make_async_remote_copy(
                src,
                dst,
                self.send_sems.at[base + peer],
                self.recv_sems.at[base + peer],
                device_id=device,
                device_id_type=MESH_ID,
            )
            self.made.append(there)
            out.append((there, back))
        return out

    def finish(self):
        for copy in self.made:
            copy.wait_send()


def enter(peers):
    barrier = pltpu.get_barrier_semaphore()
    for peer in peers:
        pl.semaphore_signal(barrier, inc=1, device_id=peer, device_id_type=MESH_ID)
    pl.semaphore_wait(barrier, len(peers))


def pieces_of(ref, rows):
    half = rows // 2

    def whole(b):
        return ref.at[pl.ds(pl.multiple_of(b * rows, rows), rows)]

    def first(b):
        return ref.at[pl.ds(pl.multiple_of(b * rows, rows), half)]

    def second(b):
        return ref.at[pl.ds(pl.multiple_of(b * rows + half, half), half)]

    return whole, first, second


GATHER_SEMS = DEPTH + 3 * DEPTH + 4 * DEPTH + 2 * DEPTH


def gather_steps(p, copies, rows, own_ref, all_ref, own_copy):
    whole, first, second = pieces_of(all_ref, rows)
    me = p.block()
    xn, yn, cn = p.at(x=1 - p.x), p.at(y=1 - p.y), p.at(c=1 - p.c)
    order = [p.near(k) for k in range(DEPTH)]
    line = copies.along(
        [(z, own_ref, whole(me)) for z in order[1:]], [p.at(z=z) for z in order[1:]], p.z
    )
    to_x, to_y, near, far, diagonal = [], [], [], [], []
    for d in range(DEPTH):
        b = p.block(z=order[d])
        src = own_ref if d == 0 else whole(b)
        to_x.append(copies.make(src, whole(b), xn))
        to_y.append(copies.make(src, whole(b), yn))
        bx, by = p.block(z=order[d], x=1 - p.x), p.block(z=order[d], y=1 - p.y)
        bd = p.block(z=order[d], x=1 - p.x, y=1 - p.y)
        near.append([copies.make(src, whole(b), cn), copies.make(whole(bx), whole(bx), cn)])
        diagonal.append(
            (copies.make(first(bx), first(bx), yn), copies.make(second(by), second(by), xn))
        )
        far.append(
            [
                copies.make(whole(by), whole(by), cn),
                copies.make(first(bd), first(bd), cn),
                copies.make(second(bd), second(bd), cn),
            ]
        )

    def onward(d):
        if d:
            line[d - 1][1].wait_recv()
        to_x[d].start()
        to_y[d].start()
        near[d][0].start()

    def pair(d):
        to_x[d].wait_recv()
        diagonal[d][0].start()
        near[d][1].start()
        to_y[d].wait_recv()
        diagonal[d][1].start()
        far[d][0].start()

    def corner(d):
        for i in range(2):
            diagonal[d][i].wait_recv()
            far[d][1 + i].start()

    def arrived(group):
        for copy in group:
            copy.wait_recv()

    def begin():
        own_copy.start()
        for there, _ in line:
            there.start()
        onward(0)

    def step0():
        onward(1)
        pair(0)
        own_copy.wait()
        arrived(near[0])

    def step1():
        onward(2)
        pair(1)
        corner(0)
        arrived(far[0])

    def step3():
        onward(3)
        pair(2)
        corner(1)
        arrived(far[1])

    def step5():
        pair(3)
        corner(2)
        arrived(far[2])

    def step6():
        corner(3)
        arrived(near[3])

    return [
        begin,
        step0,
        step1,
        lambda: arrived(near[1]),
        step3,
        lambda: arrived(near[2]),
        step5,
        step6,
        lambda: arrived(far[3]),
    ]


SCATTER_SEMS = 16 + 8 + 8 + DEPTH


def scatter_scratch(rows, width):
    return [
        pltpu.VMEM((16, rows, width), LOW),
        pltpu.VMEM((2, DEPTH, rows // 2, width), LOW),
        pltpu.VMEM((2, DEPTH, rows, width), LOW),
        pltpu.VMEM((DEPTH, rows, width), LOW),
    ]


def scatter_steps(p, copies, rows, part, core_in, diag_in, side_in, line_in, out_ref):
    whole, first, second = pieces_of(part, rows)
    order = [p.near(k) for k in reversed(range(DEPTH))]
    xn, yn, cn = p.at(x=1 - p.x), p.at(y=1 - p.y), p.at(c=1 - p.c)
    kinds = [dict(y=1 - p.y, x=1 - p.x), dict(x=1 - p.x), dict(y=1 - p.y), dict()]
    blocks = [[p.block(z=z, **kind) for kind in kinds] for z in order]
    core = [
        [
            copies.make(whole(p.block(z=z, c=1 - p.c, **kind)), core_in.at[k * 4 + j], cn)
            for j, kind in enumerate(kinds)
        ]
        for k, z in enumerate(order)
    ]
    corners = [
        (
            copies.make(first(blocks[k][0]), diag_in.at[0, k], yn),
            copies.make(second(blocks[k][0]), diag_in.at[1, k], xn),
        )
        for k in range(DEPTH)
    ]
    sides = [
        (
            copies.make(whole(blocks[k][1]), side_in.at[0, k], xn),
            copies.make(whole(blocks[k][2]), side_in.at[1, k], yn),
        )
        for k in range(DEPTH)
    ]
    line = copies.along(
        [(order[k], whole(blocks[k][3]), line_in.at[p.z]) for k in range(DEPTH - 1)],
        [p.at(z=order[k]) for k in range(DEPTH - 1)],
        p.z,
    )

    def add(ref, *more):
        total = ref[...].astype(F32)
        for other in more:
            total = total + other[...].astype(F32)
        ref[...] = total.astype(LOW)

    def corner(k):
        core[k][0].wait_recv()
        add(whole(blocks[k][0]), core_in.at[k * 4])
        for copy in corners[k]:
            copy.start()
        for j in (1, 2):
            core[k][j].wait_recv()
            add(whole(blocks[k][j]), core_in.at[k * 4 + j])

    def side(k):
        corners[k][0].wait_recv()
        add(first(blocks[k][1]), diag_in.at[0, k])
        sides[k][0].start()
        corners[k][1].wait_recv()
        add(second(blocks[k][2]), diag_in.at[1, k])
        sides[k][1].start()
        core[k][3].wait_recv()

    def close(k):
        sides[k][0].wait_recv()
        sides[k][1].wait_recv()
        add(whole(blocks[k][3]), core_in.at[k * 4 + 3], side_in.at[0, k], side_in.at[1, k])
        if k < DEPTH - 1:
            line[k][0].start()

    def step0():
        for row in core:
            for copy in row:
                copy.start()
        corner(0)

    def step1():
        corner(1)
        side(0)

    def step2():
        corner(2)
        side(1)

    def step3():
        corner(3)
        side(2)
        close(0)

    def step4():
        side(3)
        close(1)

    def step7():
        total = whole(blocks[DEPTH - 1][3])[...].astype(F32)
        for k in reversed(range(DEPTH - 1)):
            line[k][1].wait_recv()
            total = total + line_in[order[k]].astype(F32)
        out_ref[...] = total

    return [step0, step1, step2, step3, step4, lambda: close(2), lambda: close(3), step7]


def dot(left, right, left_dim, right_dim):
    return lax.dot_general(
        left, right, (((left_dim,), (right_dim,)), ((), ())), preferred_element_type=F32
    )


def semaphores(*counts):
    return [pltpu.SemaphoreType.DMA((n,)) for n in counts]


VMEM_SPEC = pl.BlockSpec(memory_space=pltpu.VMEM)
ANY_SPEC = pl.BlockSpec(memory_space=pl.ANY)


def experts_kernel(
    rows,
    width,
    experts,
    owned,
    own_ref,
    upstream_ref,
    gate_ref,
    up_ref,
    down_ref,
    heads_ref,
    grad_ref,
    moe_ref,
    line_heads_ref,
    gate_grad_ref,
    up_grad_ref,
    down_grad_ref,
    all_ref,
    upstream,
    outgoing,
    part,
    back_rows,
    core_in,
    diag_in,
    side_in,
    line_in,
    local_sems,
    gather_send,
    gather_recv,
    scatter_send,
    scatter_recv,
    heads_send,
    heads_recv,
):
    p = Place()
    group = rows * 4
    units = down_ref.shape[0]
    hidden = units // owned
    extra = all_ref.shape[1] - width
    enter(p.peers())
    whole, _, _ = pieces_of(all_ref, rows)
    own_copy = pltpu.make_async_copy(own_ref, whole(p.block()), local_sems.at[0])
    gather_copies = Copies(gather_send, gather_recv)
    scatter_copies = Copies(scatter_send, scatter_recv)
    gathering = gather_steps(p, gather_copies, rows, own_ref, all_ref, own_copy)
    scattering = scatter_steps(
        p, scatter_copies, rows, part, core_in, diag_in, side_in, line_in, grad_ref
    )
    heads_copies = Copies(heads_send, heads_recv)
    others = [p.near(k) for k in range(1, DEPTH)]
    heads_line = heads_copies.along(
        [(z, heads_ref, line_heads_ref.at[p.z]) for z in others], [p.at(z=z) for z in others], p.z
    )
    count = 2 * DEPTH

    def rows_of(i):
        side = jnp.where(i % 2 == 0, p.y, 1 - p.y)
        return pl.ds(pl.multiple_of((p.near(i // 2) * 2 + side) * group, group), group)

    def fetch(i):
        return pltpu.make_async_copy(
            upstream_ref.at[rows_of(i)], upstream.at[i % 2], local_sems.at[1 + i % 2]
        )

    def store(i):
        return pltpu.make_async_copy(
            outgoing.at[i % 2], moe_ref.at[rows_of(i)], local_sems.at[3 + i % 2]
        )

    fetch(0).start()
    gathering[0]()
    down_grad_ref[...] = jnp.zeros_like(down_grad_ref)
    first = p.e * owned
    lane = lax.broadcasted_iota(jnp.int32, (group, extra), 1)
    unit = lax.broadcasted_iota(jnp.int32, (group, units), 1)

    @pl.loop(0, count)
    def _(i):
        for k, step in enumerate(gathering[1:]):
            pl.when(i == k)(step)
        at = rows_of(i)
        x = all_ref[at, :width]
        gate = dot(x, gate_ref[...], 1, 1)
        up = dot(x, up_ref[...], 1, 1)
        tail = all_ref[at, width:].astype(F32)
        weights = [
            jnp.sum(
                jnp.where((lane == first + j) | (lane == experts + first + j), tail, 0.0),
                axis=1,
                keepdims=True,
            )
            for j in range(owned)
        ]
        weight = weights[0]
        for j in range(1, owned):
            weight = jnp.where(unit >= j * hidden, weights[j], weight)
        sigmoid = 1.0 / (1.0 + jnp.exp(-gate))
        activated = gate * sigmoid
        inner = activated * up
        weighted = (inner * weight).astype(LOW)

        @pl.when(i >= 2)
        def _():
            store(i - 2).wait()

        outgoing[i % 2] = dot(weighted, down_ref[...], 1, 0).astype(LOW)
        store(i).start()
        fetch(i).wait()

        @pl.when(i + 1 < count)
        def _():
            fetch(i + 1).start()

        u = upstream[i % 2]
        down_back = dot(u, down_ref[...], 1, 1)
        down_grad_ref[...] += dot(weighted, u, 0, 0)
        product = inner * down_back
        note = jnp.zeros((group, extra), F32)
        for j in range(owned):
            mine = (unit >= j * hidden) & (unit < (j + 1) * hidden)
            route_grad = jnp.sum(jnp.where(mine, product, 0.0), axis=1, keepdims=True)
            note = jnp.where(lane == first + j, route_grad, note)
        inner_grad = down_back * weight
        gate_back = (inner_grad * up * sigmoid * (1.0 + gate * (1.0 - sigmoid))).astype(LOW)
        up_back = (inner_grad * activated).astype(LOW)
        back_rows[at, :units] = gate_back
        back_rows[at, units:] = up_back
        part[at, :width] = (
            dot(gate_back, gate_ref[...], 1, 0) + dot(up_back, up_ref[...], 1, 0)
        ).astype(LOW)
        part[at, width:] = note.astype(LOW)

    for there, _ in heads_line:
        there.start()
    tile = width // count

    @pl.loop(0, count)
    def _(i):
        for k, step in enumerate(scattering):
            pl.when(i == k)(step)
        at = pl.ds(pl.multiple_of(i * tile, tile), tile)
        x = all_ref[:, at]
        gate_grad_ref[:, at] = dot(back_rows[:, :units], x, 0, 0)
        up_grad_ref[:, at] = dot(back_rows[:, units:], x, 0, 0)

    gather_copies.finish()
    scatter_copies.finish()
    store(count - 2).wait()
    store(count - 1).wait()
    for _, back in heads_line:
        back.wait_recv()
    heads_copies.finish()


def run_experts(own, upstream_all, gate, up, down, heads, owned, experts, width, collective_id):
    rows, full = own.shape
    total = upstream_all.shape[0]
    units = down.shape[0]
    group = rows * lax.axis_size("tensor")
    return pl.pallas_call(
        functools.partial(experts_kernel, rows, width, experts, owned),
        out_shape=(
            jax.ShapeDtypeStruct((rows, full), F32),
            jax.ShapeDtypeStruct((total, width), LOW),
            jax.ShapeDtypeStruct((DEPTH, *heads.shape), LOW),
            *[jax.ShapeDtypeStruct((units, width), F32)] * 3,
        ),
        in_specs=[VMEM_SPEC, ANY_SPEC, VMEM_SPEC, VMEM_SPEC, VMEM_SPEC, ANY_SPEC],
        out_specs=(VMEM_SPEC, ANY_SPEC, ANY_SPEC, VMEM_SPEC, VMEM_SPEC, VMEM_SPEC),
        scratch_shapes=[
            pltpu.VMEM((total, full), LOW),
            pltpu.VMEM((2, group, width), LOW),
            pltpu.VMEM((2, group, width), LOW),
            pltpu.VMEM((total, full), LOW),
            pltpu.VMEM((total, 2 * units), LOW),
        ]
        + scatter_scratch(rows, full)
        + semaphores(5, GATHER_SEMS, GATHER_SEMS, SCATTER_SEMS, SCATTER_SEMS, DEPTH, DEPTH),
        compiler_params=pltpu.CompilerParams(
            collective_id=collective_id, has_side_effects=True, vmem_limit_bytes=64000000
        ),
        name="experts",
    )(own, upstream_all, gate, up, down, heads)


def normed_rows(values):
    scale = lax.rsqrt(jnp.mean(values * values, axis=-1, keepdims=True) + EPSILON)
    return values * scale, scale


def turned(values):
    return pltpu.roll(values, values.shape[-1] // 2, values.ndim - 1)


def allowed_keys(count, length):
    row = lax.broadcasted_iota(jnp.int32, (count, count), 0)
    column = lax.broadcasted_iota(jnp.int32, (count, count), 1)
    return (column <= row) & (column < length)


def attention_probs(query, key, allowed):
    factor = query.shape[-1] ** (-0.5)
    scores = jnp.where(allowed, dot(query, key, 1, 1) * factor, NEGATIVE)
    expo = jnp.exp(scores - jnp.max(scores, axis=-1, keepdims=True))
    return expo / jnp.sum(expo, axis=-1, keepdims=True)


class Spread:
    def __init__(self, p, copies, slot):
        other = (1 - p.x) * 2 + p.c
        self.to_x = copies.make(slot(p.t), slot(p.t), p.at(x=1 - p.x))
        self.to_c = copies.make(slot(p.t), slot(p.t), p.at(c=1 - p.c))
        self.onward = copies.make(slot(other), slot(other), p.at(c=1 - p.c))

    def start(self):
        self.to_x.start()
        self.to_c.start()

    def forward(self):
        self.to_x.wait_recv()
        self.onward.start()

    def finish(self):
        self.to_c.wait_recv()
        self.onward.wait_recv()


class Fold:
    def __init__(self, p, copies, rows, part, arrived):
        def block(t):
            return part.at[pl.ds(pl.multiple_of(t * rows, rows), rows)]

        cn, xn = p.at(c=1 - p.c), p.at(x=1 - p.x)
        self.arrived, self.own, self.other = arrived, block(p.t), block((1 - p.x) * 2 + p.c)
        self.to_c = [
            copies.make(block((1 - p.x) * 2 + 1 - p.c), arrived.at[0], cn),
            copies.make(block(p.x * 2 + 1 - p.c), arrived.at[1], cn),
        ]
        self.to_x = copies.make(self.other, arrived.at[2], xn)

    def start(self):
        for copy in self.to_c:
            copy.start()

    def forward(self):
        self.to_c[0].wait_recv()
        self.other[...] = (self.other[...].astype(F32) + self.arrived[0].astype(F32)).astype(LOW)
        self.to_x.start()

    def finish(self):
        self.to_c[1].wait_recv()
        self.to_x.wait_recv()
        return (
            self.own[...].astype(F32) + self.arrived[1].astype(F32) + self.arrived[2].astype(F32)
        )


FOLD_SEMS = 3


def front_kernel(
    rows,
    experts,
    length_ref,
    tokens_ref,
    cotangent_ref,
    routes_ref,
    attention_gain_ref,
    query_gain_ref,
    key_gain_ref,
    routing_gain_ref,
    cosine_ref,
    sine_ref,
    query_weight_ref,
    key_weight_ref,
    value_weight_ref,
    output_weight_ref,
    router_weight_ref,
    upstream_ref,
    xnorm1_ref,
    query_ref,
    key_ref,
    value_ref,
    heads_ref,
    hidden_ref,
    own_ref,
    router_ref,
    part,
    part_in,
    local_sems,
    gather_send,
    gather_recv,
    send_sems,
    recv_sems,
):
    p = Place()
    group, width = tokens_ref.shape
    units = query_ref.shape[1]
    size = cosine_ref.shape[1]
    count = units // size
    length = length_ref[0]
    enter(p.peers())
    copies = Copies(send_sems, recv_sems)
    gather_copies = Copies(gather_send, gather_recv)
    mine = pl.ds(pl.multiple_of(p.t * rows, rows), rows)
    whole, _, _ = pieces_of(upstream_ref, rows)
    own_cotangent = cotangent_ref.at[mine]
    own_copy = pltpu.make_async_copy(own_cotangent, whole(p.block()), local_sems.at[0])
    gathering = gather_steps(p, gather_copies, rows, own_cotangent, upstream_ref, own_copy)
    fold = Fold(p, copies, rows, part, part_in)
    gathering[0]()

    normed1, _ = normed_rows(tokens_ref[...].astype(F32))
    xnorm1_ref[...] = (normed1 * attention_gain_ref[...]).astype(LOW)
    query_ref[...] = dot(xnorm1_ref[...], query_weight_ref[...], 1, 0)
    key_ref[...] = dot(xnorm1_ref[...], key_weight_ref[...], 1, 0)
    value_ref[...] = dot(xnorm1_ref[...], value_weight_ref[...], 1, 0).astype(LOW)
    gathering[1]()
    cosine, sine = cosine_ref[...], sine_ref[...]
    query_gain = query_gain_ref[...]
    valid = lax.broadcasted_iota(jnp.int32, (group, 1), 0) < length
    allowed = allowed_keys(group, length)
    key_hat, _ = normed_rows(key_ref[...])
    key_gained = key_hat * key_gain_ref[...]
    key_low = (key_gained * cosine + turned(key_gained) * sine).astype(LOW)

    @pl.loop(0, count)
    def _(h):
        for k in (2, 3):
            pl.when(h == 2 * k)(gathering[k])
        at = pl.ds(pl.multiple_of(h * size, size), size)
        hat, _ = normed_rows(query_ref[:, at])
        gained = hat * query_gain
        query_low = (gained * cosine + turned(gained) * sine).astype(LOW)
        probs = attention_probs(query_low, key_low, allowed).astype(LOW)
        heads_ref[:, at] = jnp.where(valid, dot(probs, value_ref[...], 1, 0), 0.0).astype(LOW)

    part[...] = dot(heads_ref[...], output_weight_ref[...], 1, 1).astype(LOW)
    fold.start()
    gathering[4]()
    fold.forward()
    gathering[5]()
    hidden = tokens_ref[mine, :].astype(F32) + fold.finish()
    hidden_ref[...] = hidden
    normed2, _ = normed_rows(hidden)
    xnorm2 = (normed2 * routing_gain_ref[...]).astype(LOW)
    own_ref[:, :width] = xnorm2
    gathering[6]()
    logits = dot(xnorm2, router_weight_ref[...], 1, 1)
    lanes = logits.shape[1]
    lane = lax.broadcasted_iota(jnp.int32, logits.shape, 1)
    peak = jnp.max(jnp.where(lane < experts, logits, NEGATIVE), axis=1, keepdims=True)
    expo = jnp.where(lane < experts, jnp.exp(jnp.minimum(logits - peak, 0.0)), 0.0)
    router = expo / jnp.sum(expo, axis=1, keepdims=True)
    named = jnp.zeros(logits.shape, F32)
    for k in range(routes_ref.shape[1]):
        named = jnp.where(routes_ref[:, k : k + 1] == lane, 1.0, named)
    chosen = router * named
    route_weight = chosen / jnp.sum(chosen, axis=1, keepdims=True)
    high = route_weight.astype(LOW).astype(F32)
    own_ref[:, width:] = (high + pltpu.roll(route_weight - high, experts, 1)).astype(LOW)
    router_ref[:, :lanes] = router
    router_ref[:, lanes : 2 * lanes] = route_weight
    router_ref[:, 2 * lanes :] = named
    for step in gathering[7:]:
        step()
    gather_copies.finish()
    copies.finish()


def run_front(
    length,
    tokens,
    cotangent,
    routes,
    attention_gain,
    query_gain,
    key_gain,
    routing_gain,
    cosine,
    sine,
    query_weight,
    key_weight,
    value_weight,
    output_weight,
    router_weight,
    experts,
    collective_id,
):
    group, width = tokens.shape
    rows = routes.shape[0]
    lanes = router_weight.shape[0]
    total = group * lax.axis_size("expert")
    struct = jax.ShapeDtypeStruct
    return pl.pallas_call(
        functools.partial(front_kernel, rows, experts),
        out_shape=(
            struct((total, width), LOW),
            struct((group, width), LOW),
            struct((group, query_weight.shape[1]), F32),
            struct((group, key_weight.shape[1]), F32),
            struct((group, value_weight.shape[1]), LOW),
            struct((group, query_weight.shape[1]), LOW),
            struct((rows, width), F32),
            struct((rows, width + lanes), LOW),
            struct((rows, 3 * lanes), F32),
        ),
        in_specs=[pl.BlockSpec(memory_space=pltpu.SMEM), VMEM_SPEC, ANY_SPEC] + [VMEM_SPEC] * 12,
        out_specs=[ANY_SPEC] + [VMEM_SPEC] * 8,
        scratch_shapes=[pltpu.VMEM((group, width), LOW), pltpu.VMEM((3, rows, width), LOW)]
        + semaphores(1, GATHER_SEMS, GATHER_SEMS, FOLD_SEMS, FOLD_SEMS),
        compiler_params=pltpu.CompilerParams(
            collective_id=collective_id, has_side_effects=True, vmem_limit_bytes=60000000
        ),
        name="front",
    )(
        length,
        tokens,
        cotangent,
        routes,
        attention_gain,
        query_gain,
        key_gain,
        routing_gain,
        cosine,
        sine,
        query_weight,
        key_weight,
        value_weight,
        output_weight,
        router_weight,
    )


SPREAD_SEMS = 3
TAIL_SEMS = 4 * SPREAD_SEMS + DEPTH + DEPTH + 2 + 2 * DEPTH + 1 + 3 + 3 + DEPTH


def tail_kernel(
    rows,
    experts,
    length_ref,
    summed_ref,
    own_ref,
    router_ref,
    hidden_ref,
    cotangent_ref,
    tokens_ref,
    xnorm1_ref,
    moe_ref,
    heads_ref,
    line_heads_ref,
    query_ref,
    key_ref,
    value_ref,
    cosine_ref,
    sine_ref,
    attention_gain_ref,
    routing_gain_ref,
    query_gain_ref,
    key_gain_ref,
    query_weight_ref,
    key_weight_ref,
    value_weight_ref,
    output_weight_ref,
    router_weight_ref,
    mixed_ref,
    tokens_grad_ref,
    output_grad_ref,
    packed_grad_ref,
    small_out_ref,
    hidden_grad_ref,
    hidden_low_ref,
    hidden_all,
    hidden_line,
    line_heads,
    heads_grad,
    packed,
    packed_in,
    xnorm_in,
    weight_out,
    weight_in,
    output_out,
    output_in,
    key_sum,
    value_sum,
    back_part,
    back_in,
    moe,
    moe_own,
    small,
    small_in,
    small_side,
    small_line,
    core_in,
    diag_in,
    side_in,
    line_in,
    local_sems,
    send_sems,
    recv_sems,
    scatter_send,
    scatter_recv,
):
    p = Place()
    group, width = xnorm1_ref.shape
    units = query_ref.shape[1]
    size = cosine_ref.shape[1]
    count = units // size
    packed_width = packed.shape[1]
    share = width // (2 * DEPTH)
    length = length_ref[0]
    fetch = [
        pltpu.make_async_copy(moe_ref, moe, local_sems.at[0]),
        *[
            pltpu.make_async_copy(
                line_heads_ref.at[p.near(k)], line_heads.at[p.near(k)], local_sems.at[k]
            )
            for k in range(1, DEPTH)
        ],
    ]
    for copy in fetch:
        copy.start()
    enter(p.peers())
    copies = Copies(send_sems, recv_sems)
    scatter_copies = Copies(scatter_send, scatter_recv)
    scattering = scatter_steps(
        p, scatter_copies, rows, moe, core_in, diag_in, side_in, line_in, moe_own
    )
    xn, yn, cn = p.at(x=1 - p.x), p.at(y=1 - p.y), p.at(c=1 - p.c)
    order = [p.near(k) for k in reversed(range(DEPTH))]
    along = [p.at(z=z) for z in order[: DEPTH - 1]]

    def columns(z, y):
        return pl.ds(pl.multiple_of((z * 2 + y) * share, share), share)

    def block(ref, t):
        return ref.at[pl.ds(pl.multiple_of(t * rows, rows), rows)]

    hidden_spread = Spread(p, copies, lambda t: block(hidden_all, t))
    line_spread = Spread(p, copies, lambda t: hidden_line.at[t])
    hidden_to = copies.along(
        [
            (
                z,
                hidden_low_ref.at[:, pl.ds(pl.multiple_of(z * 2 * share, share), 2 * share)],
                hidden_line.at[p.t, p.z],
            )
            for z in order[: DEPTH - 1]
        ],
        along,
        p.z,
    )
    xnorm_to = [
        copies.make(xnorm1_ref.at[:, columns(z, 1 - p.y)], xnorm_in.at[z], yn) for z in range(DEPTH)
    ]
    cuts = [(0, units // 2), (units // 2, packed_width)]
    packed_to = [copies.make(packed.at[:, a:b], packed_in.at[:, a:b], yn) for a, b in cuts]
    weight_to = [
        copies.along(
            [
                (order[k], weight_out.at[k, :, a:b], weight_in.at[p.z, :, a:b])
                for k in range(DEPTH - 1)
            ],
            along,
            p.z,
        )
        for a, b in cuts
    ]
    output_to = copies.make(output_out, output_in, yn)
    fold = Fold(p, copies, rows, back_part, back_in)
    tokens_spread = Spread(p, copies, lambda t: block(tokens_grad_ref, t))
    mixed_spread = Spread(p, copies, lambda t: block(mixed_ref, t))
    small_to_c = copies.make(small, small_in.at[0], cn)
    small_to_x = copies.make(small, small_in.at[1], xn)
    small_to_y = copies.make(small_side.at[0], small_side.at[1], yn)
    small_to = copies.along(
        [(z, small_side.at[2, z], small_line.at[p.z]) for z in order[: DEPTH - 1]], along, p.z
    )

    lanes = router_weight_ref.shape[0]
    gain_row = experts + 2
    route_grad = summed_ref[:, width:]
    router = router_ref[:, :lanes]
    route_weight = router_ref[:, lanes : 2 * lanes]
    named = router_ref[:, 2 * lanes :]
    chosen_total = jnp.sum(router * named, axis=1, keepdims=True)
    inner_total = jnp.sum(route_grad * route_weight, axis=1, keepdims=True)
    prob_grad = named * (route_grad - inner_total) / chosen_total
    logit_low = (router * (prob_grad - jnp.sum(router * prob_grad, axis=1, keepdims=True))).astype(
        LOW
    )
    small[...] = jnp.zeros_like(small)
    small[:experts, :] = dot(logit_low, own_ref[:, :width], 0, 0)[:experts]
    xnorm2_grad = summed_ref[:, :width] + dot(logit_low, router_weight_ref[...], 1, 0)
    normed2, scale2 = normed_rows(hidden_ref[...])
    small[experts : experts + 1, :] = jnp.sum(xnorm2_grad * normed2, axis=0, keepdims=True)
    inner2 = xnorm2_grad * routing_gain_ref[...]
    hidden_grad_ref[...] = cotangent_ref[...].astype(F32) + scale2 * (
        inner2 - normed2 * jnp.mean(inner2 * normed2, axis=-1, keepdims=True)
    )
    hidden_low_ref[...] = hidden_grad_ref[...].astype(LOW)
    block(hidden_all, p.t)[...] = hidden_low_ref[...]
    hidden_line[p.t, p.z] = hidden_low_ref[
        :, pl.ds(pl.multiple_of(p.z * 2 * share, share), 2 * share)
    ]
    for there, _ in hidden_to:
        there.start()
    hidden_spread.start()
    for copy in xnorm_to:
        copy.start()
    key_sum[...] = jnp.zeros_like(key_sum)
    value_sum[...] = jnp.zeros_like(value_sum)
    fetch[0].wait()
    scattering[0]()
    hidden_spread.forward()
    scattering[1]()
    hidden_spread.finish()

    valid = lax.broadcasted_iota(jnp.int32, (group, 1), 0) < length
    allowed = allowed_keys(group, length)
    heads_grad[...] = jnp.where(
        valid, dot(hidden_all[...], output_weight_ref[...], 1, 0), 0.0
    ).astype(LOW)
    cosine, sine = cosine_ref[...], sine_ref[...]
    query_gain, key_gain = query_gain_ref[...], key_gain_ref[...]
    factor = size ** (-0.5)
    key_hat, key_scale = normed_rows(key_ref[...])
    key_gained = key_hat * key_gain
    key_low = (key_gained * cosine + turned(key_gained) * sine).astype(LOW)

    def norm_back(grad, hat, scale, gain):
        grad = grad * cosine - turned(grad) * sine
        gain_part = jnp.sum(grad * hat, axis=0, keepdims=True)
        inner = grad * gain
        return scale * (inner - hat * jnp.mean(inner * hat, axis=-1, keepdims=True)), gain_part

    def one_head(h):
        at = pl.ds(pl.multiple_of(h * size, size), size)
        hat, scale = normed_rows(query_ref[:, at])
        gained = hat * query_gain
        query_low = (gained * cosine + turned(gained) * sine).astype(LOW)
        probs = attention_probs(query_low, key_low, allowed)
        grad = heads_grad[:, at]
        probs_grad = dot(grad, value_ref[...], 1, 1)
        delta = jnp.sum(probs * probs_grad, axis=-1, keepdims=True)
        score_grad = (probs * (probs_grad - delta)).astype(LOW)
        key_sum[...] += dot(score_grad, query_low, 0, 0)
        value_sum[...] += dot(probs.astype(LOW), grad, 0, 0)
        back, gain_part = norm_back(
            dot(score_grad, key_low, 1, 0) * factor, hat, scale, query_gain
        )
        packed[:, at] = back.astype(LOW)
        small[gain_row : gain_row + 1, :size] += gain_part

    pl.loop(0, count // 2)(one_head)
    packed_to[0].start()
    scattering[2]()
    for _, back in hidden_to:
        back.wait_recv()
    line_spread.start()
    pl.loop(count // 2, count)(one_head)
    key_back, key_part = norm_back(key_sum[...] * factor, key_hat, key_scale, key_gain)
    packed[:, units : units + size] = key_back.astype(LOW)
    packed[:, units + size :] = value_sum[...].astype(LOW)
    packed_to[1].start()
    small[gain_row + 1 : gain_row + 2, :size] = key_part
    for row in (gain_row, gain_row + 1):
        part = small[row : row + 1, :size]
        for i in range(1, width // size):
            small[row : row + 1, i * size : (i + 1) * size] = part
    line_spread.forward()
    scattering[3]()
    back_part[...] = (
        dot(packed[:, :units], query_weight_ref[...], 1, 1)
        + dot(packed[:, units : units + size], key_weight_ref[...], 1, 1)
        + dot(packed[:, units + size :], value_weight_ref[...], 1, 1)
    ).astype(LOW)
    fold.start()
    for copy in xnorm_to:
        copy.wait_recv()

    def weight_piece(i):
        a, b = cuts[i]
        packed_to[i].wait_recv()
        for k, z in enumerate(order):
            grad = dot(xnorm1_ref[:, columns(z, p.y)], packed[:, a:b], 0, 0) + dot(
                xnorm_in[z], packed_in[:, a:b], 0, 0
            )
            if k < DEPTH - 1:
                weight_out[k, :, a:b] = grad.astype(LOW)
                weight_to[i][k][0].start()
            else:
                packed_grad_ref[:, a:b] = grad

    weight_piece(0)
    fold.forward()
    scattering[4]()
    weight_piece(1)
    scattering[5]()

    xnorm1_grad = fold.finish()
    normed1, scale1 = normed_rows(tokens_ref[...].astype(F32))
    small[gain_row - 1 : gain_row, :] = jnp.sum(xnorm1_grad * normed1, axis=0, keepdims=True)
    small_to_c.start()
    inner = xnorm1_grad * attention_gain_ref[...]
    block(tokens_grad_ref, p.t)[...] = (
        hidden_grad_ref[...]
        + scale1 * (inner - normed1 * jnp.mean(inner * normed1, axis=-1, keepdims=True))
    ).astype(LOW)
    tokens_spread.start()

    line_spread.finish()
    for copy in fetch[1:]:
        copy.wait()

    def output_piece(y):
        at = pl.ds(pl.multiple_of(y * share, share), share)
        grad = dot(hidden_line[:, p.z, :, at].reshape(group, share), heads_ref[...], 0, 0)
        for k in range(1, DEPTH):
            z = p.near(k)
            grad += dot(hidden_line[:, z, :, at].reshape(group, share), line_heads[z], 0, 0)
        return grad

    output_out[...] = output_piece(1 - p.y).astype(LOW)
    output_to.start()
    output_grad_ref[...] = output_piece(p.y)
    scattering[6]()
    small_to_c.wait_recv()
    small_to_c.wait_send()
    small[...] += small_in[0]
    small_to_x.start()
    tokens_spread.forward()
    scattering[7]()
    block(mixed_ref, p.t)[...] = (hidden_ref[...] + moe_own[...]).astype(LOW)
    mixed_spread.start()
    small_to_x.wait_recv()
    small_to_x.wait_send()
    small[...] += small_in[1]
    for z in range(DEPTH):
        small_side[0, z] = small[:, columns(z, 1 - p.y)]
        small_side[2, z] = small[:, columns(z, p.y)]
    small_to_y.start()
    output_to.wait_recv()
    output_grad_ref[...] += output_in[...].astype(F32)
    small_to_y.wait_recv()
    small_side[2] += small_side[1]
    for there, _ in small_to:
        there.start()
    mixed_spread.forward()
    tokens_spread.finish()
    small_total = small_side[2, p.z]
    for (_, back), z in zip(small_to, order):
        back.wait_recv()
        small_total += small_line[z]
    small_out_ref[...] = small_total
    mixed_spread.finish()
    for i, (a, b) in enumerate(cuts):
        grad = packed_grad_ref[:, a:b]
        for (_, back), z in zip(weight_to[i], order):
            back.wait_recv()
            grad += weight_in[z, :, a:b].astype(F32)
        packed_grad_ref[:, a:b] = grad
    for copy in copies.made:
        if copy is not small_to_c and copy is not small_to_x:
            copy.wait_send()
    scatter_copies.finish()


def run_tail(
    length,
    summed,
    own,
    router,
    hidden,
    cotangent,
    tokens,
    xnorm1,
    moe,
    heads,
    line_heads,
    query,
    key,
    value,
    cosine,
    sine,
    attention_gain,
    routing_gain,
    query_gain,
    key_gain,
    query_weight,
    key_weight,
    value_weight,
    output_weight,
    router_weight,
    experts,
    collective_id,
):
    group, width = xnorm1.shape
    rows = hidden.shape[0]
    units, size = query.shape[1], cosine.shape[1]
    packed_width = units + 2 * size
    share = width // (2 * DEPTH)
    tensors = group // rows
    smalls = (experts + 4 + 7) // 8 * 8
    vmem = pltpu.VMEM
    return pl.pallas_call(
        functools.partial(tail_kernel, rows, experts),
        out_shape=(
            jax.ShapeDtypeStruct((group, width), LOW),
            jax.ShapeDtypeStruct((group, width), LOW),
            jax.ShapeDtypeStruct((share, units), F32),
            jax.ShapeDtypeStruct((share, packed_width), F32),
            jax.ShapeDtypeStruct((smalls, share), F32),
        ),
        in_specs=[pl.BlockSpec(memory_space=pltpu.SMEM)]
        + [VMEM_SPEC] * 7
        + [ANY_SPEC, VMEM_SPEC, ANY_SPEC]
        + [VMEM_SPEC] * 14,
        out_specs=[VMEM_SPEC] * 5,
        scratch_shapes=[
            vmem((rows, width), F32),
            vmem((rows, width), LOW),
            vmem((group, width), LOW),
            vmem((tensors, DEPTH, rows, 2 * share), LOW),
            vmem((DEPTH, group, units), LOW),
            vmem((group, units), LOW),
            vmem((group, packed_width), LOW),
            vmem((group, packed_width), LOW),
            vmem((DEPTH, group, share), LOW),
            vmem((DEPTH - 1, share, packed_width), LOW),
            vmem((DEPTH, share, packed_width), LOW),
            vmem((share, units), LOW),
            vmem((share, units), LOW),
            vmem((group, size), F32),
            vmem((group, size), F32),
            vmem((group, width), LOW),
            vmem((3, rows, width), LOW),
            vmem(moe.shape, LOW),
            vmem((rows, width), F32),
            vmem((smalls, width), F32),
            vmem((2, smalls, width), F32),
            vmem((3, DEPTH, smalls, share), F32),
            vmem((DEPTH, smalls, share), F32),
        ]
        + scatter_scratch(rows, width)
        + semaphores(DEPTH, TAIL_SEMS, TAIL_SEMS, SCATTER_SEMS, SCATTER_SEMS),
        compiler_params=pltpu.CompilerParams(
            collective_id=collective_id, has_side_effects=True, vmem_limit_bytes=64000000
        ),
        name="tail",
    )(
        length,
        summed,
        own,
        router,
        hidden,
        cotangent,
        tokens,
        xnorm1,
        moe,
        heads,
        line_heads,
        query,
        key,
        value,
        cosine,
        sine,
        attention_gain,
        routing_gain,
        query_gain,
        key_gain,
        query_weight,
        key_weight,
        value_weight,
        output_weight,
        router_weight,
    )


def gathered_shards(
    tokens,
    seq_length,
    expert_routes,
    attention_gain,
    query_weight,
    key_weight,
    value_weight,
    query_gain,
    key_gain,
    output_weight,
    routing_gain,
    router_weight,
    gate_weight,
    up_weight,
    down_weight,
    cotangent,
):
    count, width = tokens.shape
    head_size = query_gain.shape[0]
    experts = router_weight.shape[1]
    owned = gate_weight.shape[0]
    part = lax.axis_index("tensor")
    owner = lax.axis_index("expert")
    rows = count // lax.axis_size("tensor")

    def own_rows(values):
        return lax.dynamic_slice_in_dim(values, part * rows, rows, 0)

    cosine, sine = rope_tables(count, head_size)
    half = head_size // 2
    sine = jnp.concatenate([-sine[:, :half], sine[:, half:]], axis=1)
    router_wide = jnp.pad(router_weight.T, ((0, 128 - experts), (0, 0)))
    upstream_all, xnorm1, query, key, value, heads, hidden, own, router = run_front(
        seq_length,
        tokens,
        cotangent,
        own_rows(expert_routes),
        attention_gain[None],
        query_gain[None],
        key_gain[None],
        routing_gain[None],
        cosine,
        sine,
        query_weight,
        key_weight,
        value_weight,
        output_weight,
        router_wide,
        experts,
        0,
    )

    def by_unit(weight):
        return weight.transpose(0, 2, 1).reshape(-1, width)

    def from_units(grad):
        return grad.reshape(owned, -1, width).transpose(0, 2, 1)

    summed, moe_part, line_heads, gate_grad, up_grad, down_grad = run_experts(
        own,
        upstream_all,
        by_unit(gate_weight),
        by_unit(up_weight),
        down_weight.reshape(-1, width),
        heads,
        owned,
        experts,
        width,
        1,
    )
    mixed, tokens_grad, output_grad, packed_grad, small_sum = run_tail(
        seq_length,
        summed,
        own,
        router,
        hidden,
        own_rows(cotangent),
        own_rows(tokens),
        xnorm1,
        moe_part,
        heads,
        line_heads,
        query,
        key,
        value,
        cosine,
        sine,
        attention_gain[None],
        routing_gain[None],
        query_gain[None],
        key_gain[None],
        query_weight,
        key_weight,
        value_weight,
        output_weight,
        router_wide,
        experts,
        2,
    )
    query_end = query_weight.shape[1]
    key_end = query_end + key_weight.shape[1]
    share = head_size // lax.axis_size("expert")

    def own_gain(row):
        return lax.dynamic_slice_in_dim(small_sum[row], owner * share, share, 0)

    return (
        mixed,
        tokens_grad,
        small_sum[experts + 1],
        packed_grad[:, :query_end],
        packed_grad[:, query_end:key_end],
        packed_grad[:, key_end:],
        own_gain(experts + 2),
        own_gain(experts + 3),
        output_grad,
        small_sum[experts],
        small_sum[:experts].T,
        from_units(gate_grad),
        from_units(up_grad),
        down_grad.reshape(down_weight.shape),
    )


def solution(mesh):
    sizes = dict(mesh.shape)
    fits = sizes["expert"] == 2 * DEPTH and sizes["tensor"] == 4
    return jax.shard_map(
        gathered_shards if fits else routed_shards,
        mesh=mesh,
        in_specs=(
            P("expert", None),
            P("expert"),
            P("expert", None),
            P(),
            P(None, "tensor"),
            P(None, "tensor"),
            P(None, "tensor"),
            P(),
            P(),
            P(None, "tensor"),
            P(),
            P(),
            P("expert", None, "tensor"),
            P("expert", None, "tensor"),
            P("expert", "tensor", None),
            P("expert", None),
        ),
        out_specs=(
            P("expert", None),
            P("expert", None),
            P("expert"),
            P("expert", "tensor"),
            P("expert", "tensor"),
            P("expert", "tensor"),
            P("expert"),
            P("expert"),
            P("expert", "tensor"),
            P("expert"),
            P("expert", None),
            P("expert", None, "tensor"),
            P("expert", None, "tensor"),
            P("expert", "tensor", None),
        ),
        check_vma=False,
    )
```

```python
import functools

import jax
import jax.numpy as jnp
from jax import lax
from jax.experimental import pallas as pl
from jax.experimental.pallas import tpu as pltpu
from jax.sharding import PartitionSpec as P

EPSILON = 1e-06
THETA = 1000000.0
NEGATIVE = -1e30


def rms_scale(values):
    return lax.rsqrt(jnp.mean(values * values, axis=-1, keepdims=True) + EPSILON)


def rope_tables(count, width):
    half = width // 2
    freqs = THETA ** (-(jnp.arange(half, dtype=jnp.float32) * 2.0 / width))
    angles = jnp.arange(count, dtype=jnp.float32)[:, None] * freqs[None, :]
    cosine = jnp.concatenate([jnp.cos(angles), jnp.cos(angles)], axis=1)
    sine = jnp.concatenate([jnp.sin(angles), jnp.sin(angles)], axis=1)
    return (cosine, sine)


def rotate(values, cosine, sine):
    half = values.shape[-1] // 2
    turned = jnp.concatenate([-values[..., half:], values[..., :half]], axis=-1)
    return values * cosine[:, None, :] + turned * sine[:, None, :]


def rotate_back(grads, cosine, sine):
    half = grads.shape[-1] // 2
    scaled = grads * sine[:, None, :]
    turned = jnp.concatenate([scaled[..., half:], -scaled[..., :half]], axis=-1)
    return grads * cosine[:, None, :] + turned


def head_norm(values, gain):
    scale = rms_scale(values)
    normed = values * scale
    return (normed * gain, normed, scale)


def head_norm_back(grads, normed, scale, gain):
    gain_grad = jnp.sum(grads * normed, axis=(0, 1))
    inner = grads * gain
    values_grad = scale * (inner - normed * jnp.mean(inner * normed, axis=-1, keepdims=True))
    return (values_grad, gain_grad)


def contract(left, right, left_dim, right_dim):
    return lax.dot_general(
        left, right, (((left_dim,), (right_dim,)), ((), ())), preferred_element_type=jnp.float32
    )


def block_scores(qblock, start, keys, length):
    block = qblock.shape[0]
    count = keys.shape[0]
    factor = qblock.shape[-1] ** (-0.5)
    rows = start + jnp.arange(block, dtype=jnp.int32)
    columns = jnp.arange(count, dtype=jnp.int32)
    allowed = (columns[None, :] <= rows[:, None]) & (columns[None, :] < length)
    scores = jnp.einsum("qagh,kah->agqk", qblock, keys, preferred_element_type=jnp.float32) * factor
    return (jnp.where(allowed[None, None, :, :], scores, NEGATIVE), factor)


def attend_block(qblock, start, keys, values, length):
    scores, factor = block_scores(qblock, start, keys, length)
    peak = jnp.max(scores, axis=-1, keepdims=True)
    expo = jnp.exp(scores - peak)
    total = jnp.sum(expo, axis=-1, keepdims=True)
    probs_low = (expo / total).astype(jnp.bfloat16)
    output = jnp.einsum("agqk,kah->qagh", probs_low, values, preferred_element_type=jnp.float32)
    return (output, (peak + jnp.log(total))[..., 0])


def attend_back(qblock, dblock, lse_block, start, keys, values, length):
    scores, factor = block_scores(qblock, start, keys, length)
    probs = jnp.exp(scores - lse_block[..., None])
    probs_grad = jnp.einsum("qagh,kah->agqk", dblock, values, preferred_element_type=jnp.float32)
    delta = jnp.sum(probs * probs_grad, axis=-1, keepdims=True)
    score_grad = (probs * (probs_grad - delta)).astype(jnp.bfloat16)
    query_grad = (
        jnp.einsum("agqk,kah->qagh", score_grad, keys, preferred_element_type=jnp.float32) * factor
    )
    key_grad = (
        jnp.einsum("agqk,qagh->kah", score_grad, qblock, preferred_element_type=jnp.float32)
        * factor
    )
    value_grad = jnp.einsum(
        "agqk,qagh->kah", probs.astype(jnp.bfloat16), dblock, preferred_element_type=jnp.float32
    )
    return (query_grad, key_grad, value_grad)


def routed_shards(
    tokens,
    seq_length,
    expert_routes,
    attention_gain,
    query_weight,
    key_weight,
    value_weight,
    query_gain,
    key_gain,
    output_weight,
    routing_gain,
    router_weight,
    gate_weight,
    up_weight,
    down_weight,
    cotangent,
):
    count = tokens.shape[0]
    width = tokens.shape[1]
    head_size = query_gain.shape[0]
    local_heads = query_weight.shape[1] // head_size
    local_groups = key_weight.shape[1] // head_size
    ratio = local_heads // local_groups
    length = seq_length[0]
    experts = router_weight.shape[1]
    top = expert_routes.shape[1]
    owned = gate_weight.shape[0]
    sources = experts // owned
    parts = lax.axis_size("tensor")
    part = lax.axis_index("tensor")
    quarter = (count * top * 5 + 16 * experts - 1) // (16 * experts)
    inputs = tokens.astype(jnp.float32)
    scale1 = rms_scale(inputs)
    normed1 = inputs * scale1
    xnorm1 = (normed1 * attention_gain).astype(jnp.bfloat16)
    query_raw = jnp.dot(xnorm1, query_weight, preferred_element_type=jnp.float32).reshape(
        count, local_heads, head_size
    )
    key_raw = jnp.dot(xnorm1, key_weight, preferred_element_type=jnp.float32).reshape(
        count, local_groups, head_size
    )
    value_low = (
        jnp.dot(xnorm1, value_weight, preferred_element_type=jnp.float32)
        .astype(jnp.bfloat16)
        .reshape(count, local_groups, head_size)
    )
    query_gained, query_normed, query_scale = head_norm(query_raw, query_gain)
    key_gained, key_normed, key_scale = head_norm(key_raw, key_gain)
    cosine, sine = rope_tables(count, head_size)
    query_low = rotate(query_gained, cosine, sine).astype(jnp.bfloat16)
    key_low = rotate(key_gained, cosine, sine).astype(jnp.bfloat16)
    block = min(512, count)
    blocks = count // block
    starts = jnp.arange(blocks, dtype=jnp.int32) * block
    query_blocks = query_low.reshape(blocks, block, local_groups, ratio, head_size)

    def forward_block(item):
        qblock, start = item
        return attend_block(qblock, start, key_low, value_low, length)

    outputs, lse = lax.map(forward_block, (query_blocks, starts))
    valid = (jnp.arange(count, dtype=jnp.int32) < length)[:, None]
    heads_low = jnp.where(valid, outputs.reshape(count, local_heads * head_size), 0.0).astype(
        jnp.bfloat16
    )
    attention_part = contract(heads_low, output_weight, 1, 1)
    attention_full = lax.psum(attention_part, "tensor")
    hidden = inputs + attention_full
    scale2 = rms_scale(hidden)
    normed2 = hidden * scale2
    xnorm2 = (normed2 * routing_gain).astype(jnp.bfloat16)
    logits = jnp.dot(xnorm2, router_weight, preferred_element_type=jnp.float32)
    peak = jnp.max(logits, axis=1, keepdims=True)
    expo = jnp.exp(logits - peak)
    router = expo / jnp.sum(expo, axis=1, keepdims=True)
    onehot = expert_routes[:, :, None] == jnp.arange(experts, dtype=jnp.int32)[None, None, :]
    chosen = jnp.sum(jnp.where(onehot, router[:, None, :], 0.0), axis=-1)
    chosen_total = jnp.sum(chosen, axis=1, keepdims=True)
    route_weight = chosen / chosen_total
    flat_routes = expert_routes.reshape(-1)
    hits = (flat_routes[:, None] == jnp.arange(experts, dtype=jnp.int32)[None, :]).astype(jnp.int32)
    ranks = jnp.sum((jnp.cumsum(hits, axis=0) - 1) * hits, axis=1)
    mine = ranks % parts == part
    slot_index = jnp.where(mine, ranks // parts * experts + flat_routes, quarter * experts)
    table = (
        jnp.full((quarter * experts,), count * top, jnp.int32)
        .at[slot_index]
        .set(jnp.arange(count * top, dtype=jnp.int32), mode="drop")
    )
    slot_token = table // top
    send_rows = jnp.take(xnorm2, slot_token, axis=0, mode="fill", fill_value=0).reshape(
        quarter, experts, width
    )
    arrived = lax.all_to_all(send_rows, "expert", split_axis=1, concat_axis=1, tiled=True)
    gate_full, up_full, down_full = (
        lax.all_gather(gate_weight, "tensor", axis=2, tiled=True),
        lax.all_gather(up_weight, "tensor", axis=2, tiled=True),
        lax.all_gather(down_weight, "tensor", axis=1, tiled=True),
    )
    rows_own = arrived.reshape(quarter, sources, owned, width)
    gate_val = jnp.einsum("csjd,jdf->csjf", rows_own, gate_full, preferred_element_type=jnp.float32)
    up_val = jnp.einsum("csjd,jdf->csjf", rows_own, up_full, preferred_element_type=jnp.float32)
    sigmoid_gate = jax.nn.sigmoid(gate_val)
    activated = gate_val * sigmoid_gate
    inner_low = (activated * up_val).astype(jnp.bfloat16)
    expert_total = jnp.einsum(
        "csjf,jfd->csjd", inner_low, down_full, preferred_element_type=jnp.float32
    )
    expert_low = expert_total.astype(jnp.bfloat16).reshape(quarter, experts, width)
    returned = lax.all_to_all(
        expert_low, "expert", split_axis=1, concat_axis=1, tiled=True
    ).reshape(quarter * experts, width)
    picked = jnp.take(returned, slot_index, axis=0, mode="fill", fill_value=0).reshape(
        count, top, width
    )
    mine_rows = mine.reshape(count, top)
    mine_weight = jnp.where(mine_rows, route_weight, 0.0)
    moe_part = jnp.sum(mine_weight[:, :, None] * picked, axis=1)
    moe_full = lax.psum(moe_part.astype(jnp.bfloat16), "tensor").astype(jnp.float32)
    mixed = (hidden + moe_full).astype(jnp.bfloat16)
    upstream = cotangent.astype(jnp.float32)
    route_grad_part = jnp.where(mine_rows, jnp.sum(picked * upstream[:, None, :], axis=-1), 0.0)
    slot_weight = jnp.take(route_weight.reshape(-1), table, mode="fill", fill_value=0.0)
    grad_send = (
        jnp.take(cotangent, slot_token, axis=0, mode="fill", fill_value=0) * slot_weight[:, None]
    ).astype(jnp.bfloat16)
    grad_arrived = lax.all_to_all(
        grad_send.reshape(quarter, experts, width),
        "expert",
        split_axis=1,
        concat_axis=1,
        tiled=True,
    )
    grad_own = grad_arrived.reshape(quarter, sources, owned, width)
    down_part = jnp.einsum(
        "csjf,csjd->jfd", inner_low, grad_own, preferred_element_type=jnp.float32
    )
    inner_grad = jnp.einsum(
        "csjd,jfd->csjf", grad_own, down_full, preferred_element_type=jnp.float32
    )
    gate_grad_low = (
        inner_grad * up_val * sigmoid_gate * (1.0 + gate_val * (1.0 - sigmoid_gate))
    ).astype(jnp.bfloat16)
    up_grad_low = (inner_grad * activated).astype(jnp.bfloat16)
    gate_part = jnp.einsum(
        "csjd,csjf->jdf", rows_own, gate_grad_low, preferred_element_type=jnp.float32
    )
    up_part = jnp.einsum(
        "csjd,csjf->jdf", rows_own, up_grad_low, preferred_element_type=jnp.float32
    )
    rows_grad = jnp.einsum(
        "csjf,jdf->csjd", gate_grad_low, gate_full, preferred_element_type=jnp.float32
    )
    rows_grad = rows_grad + jnp.einsum(
        "csjf,jdf->csjd", up_grad_low, up_full, preferred_element_type=jnp.float32
    )
    gate_grad, up_grad, down_grad = (
        lax.psum_scatter(
            gate_part.astype(jnp.bfloat16), "tensor", scatter_dimension=2, tiled=True
        ).astype(jnp.float32),
        lax.psum_scatter(
            up_part.astype(jnp.bfloat16), "tensor", scatter_dimension=2, tiled=True
        ).astype(jnp.float32),
        lax.psum_scatter(
            down_part.astype(jnp.bfloat16), "tensor", scatter_dimension=1, tiled=True
        ).astype(jnp.float32),
    )
    rows_grad_low = rows_grad.astype(jnp.bfloat16).reshape(quarter, experts, width)
    returned_grad = lax.all_to_all(
        rows_grad_low, "expert", split_axis=1, concat_axis=1, tiled=True
    ).reshape(quarter * experts, width)
    route_rows = jnp.take(returned_grad, slot_index, axis=0, mode="fill", fill_value=0).reshape(
        count, top, width
    )
    xnorm2_part = jnp.sum(route_rows, axis=1, dtype=jnp.float32)
    xnorm2_moe, route_grad = (
        lax.psum(xnorm2_part.astype(jnp.bfloat16), "tensor").astype(jnp.float32),
        lax.psum(route_grad_part.astype(jnp.bfloat16), "tensor").astype(jnp.float32),
    )
    inner_total = jnp.sum(route_grad * route_weight, axis=1, keepdims=True)
    chosen_grad = (route_grad - inner_total) / chosen_total
    prob_grad = jnp.sum(jnp.where(onehot, chosen_grad[:, :, None], 0.0), axis=1)
    logit_low = (router * (prob_grad - jnp.sum(router * prob_grad, axis=1, keepdims=True))).astype(
        jnp.bfloat16
    )
    router_grad = contract(xnorm2, logit_low, 0, 0)
    xnorm2_grad = xnorm2_moe + contract(logit_low, router_weight, 1, 1)
    routing_gain_part = jnp.sum(xnorm2_grad * normed2, axis=0)
    inner2 = xnorm2_grad * routing_gain
    hidden_grad = upstream + scale2 * (
        inner2 - normed2 * jnp.mean(inner2 * normed2, axis=1, keepdims=True)
    )
    hidden_low = hidden_grad.astype(jnp.bfloat16)
    output_grad = contract(hidden_low, heads_low, 0, 0)
    heads_grad = jnp.where(
        valid,
        jnp.dot(hidden_low, output_weight, preferred_element_type=jnp.float32).astype(jnp.bfloat16),
        jnp.zeros((), jnp.bfloat16),
    )
    grad_blocks = heads_grad.reshape(blocks, block, local_groups, ratio, head_size)

    def backward_block(carry, item):
        key_acc, value_acc = carry
        qblock, dblock, lse_block, start = item
        query_piece, key_piece, value_piece = attend_back(
            qblock, dblock, lse_block, start, key_low, value_low, length
        )
        return ((key_acc + key_piece, value_acc + value_piece), query_piece)

    empty = jnp.zeros((count, local_groups, head_size), jnp.float32)
    (key_rot_grad, value_grad), query_rot_grad = lax.scan(
        backward_block, (empty, empty), (query_blocks, grad_blocks, lse, starts)
    )
    query_back, query_gain_part = head_norm_back(
        rotate_back(query_rot_grad.reshape(count, local_heads, head_size), cosine, sine),
        query_normed,
        query_scale,
        query_gain,
    )
    key_back, key_gain_part = head_norm_back(
        rotate_back(key_rot_grad, cosine, sine), key_normed, key_scale, key_gain
    )
    query_grad_low = query_back.reshape(count, local_heads * head_size).astype(jnp.bfloat16)
    key_grad_low = key_back.reshape(count, local_groups * head_size).astype(jnp.bfloat16)
    value_grad_low = value_grad.reshape(count, local_groups * head_size).astype(jnp.bfloat16)
    query_wgrad = contract(xnorm1, query_grad_low, 0, 0)
    key_wgrad = contract(xnorm1, key_grad_low, 0, 0)
    value_wgrad = contract(xnorm1, value_grad_low, 0, 0)
    xnorm1_part = contract(query_grad_low, query_weight, 1, 1) + contract(
        key_grad_low, key_weight, 1, 1
    )
    xnorm1_part = xnorm1_part + contract(value_grad_low, value_weight, 1, 1)
    xnorm1_grad, query_gain_sum, key_gain_sum = (
        lax.psum(xnorm1_part.astype(jnp.bfloat16), "tensor").astype(jnp.float32),
        lax.psum(query_gain_part.astype(jnp.bfloat16), "tensor").astype(jnp.float32),
        lax.psum(key_gain_part.astype(jnp.bfloat16), "tensor").astype(jnp.float32),
    )
    attention_gain_part = jnp.sum(xnorm1_grad * normed1, axis=0)
    inner1 = xnorm1_grad * attention_gain
    tokens_grad = (
        hidden_grad
        + scale1 * (inner1 - normed1 * jnp.mean(inner1 * normed1, axis=1, keepdims=True))
    ).astype(jnp.bfloat16)
    summed = (
        lax.psum_scatter(
            attention_gain_part.astype(jnp.bfloat16), "expert", scatter_dimension=0, tiled=True
        ).astype(jnp.float32),
        lax.psum_scatter(
            query_wgrad.astype(jnp.bfloat16), "expert", scatter_dimension=0, tiled=True
        ).astype(jnp.float32),
        lax.psum_scatter(
            key_wgrad.astype(jnp.bfloat16), "expert", scatter_dimension=0, tiled=True
        ).astype(jnp.float32),
        lax.psum_scatter(
            value_wgrad.astype(jnp.bfloat16), "expert", scatter_dimension=0, tiled=True
        ).astype(jnp.float32),
        lax.psum_scatter(
            query_gain_sum.astype(jnp.bfloat16), "expert", scatter_dimension=0, tiled=True
        ).astype(jnp.float32),
        lax.psum_scatter(
            key_gain_sum.astype(jnp.bfloat16), "expert", scatter_dimension=0, tiled=True
        ).astype(jnp.float32),
        lax.psum_scatter(
            output_grad.astype(jnp.bfloat16), "expert", scatter_dimension=0, tiled=True
        ).astype(jnp.float32),
        lax.psum_scatter(
            routing_gain_part.astype(jnp.bfloat16), "expert", scatter_dimension=0, tiled=True
        ).astype(jnp.float32),
        lax.psum_scatter(
            router_grad.astype(jnp.bfloat16), "expert", scatter_dimension=0, tiled=True
        ).astype(jnp.float32),
    )
    return (
        mixed,
        tokens_grad,
        summed[0],
        summed[1],
        summed[2],
        summed[3],
        summed[4],
        summed[5],
        summed[6],
        summed[7],
        summed[8],
        gate_grad,
        up_grad,
        down_grad,
    )


MESH_ID = pl.DeviceIdType.MESH
DEPTH = 4
F32 = jnp.float32
LOW = jnp.bfloat16


class Place:
    def __init__(self):
        e, t = lax.axis_index("expert"), lax.axis_index("tensor")
        self.e, self.t = e, t
        self.z, self.y, self.x, self.c = e // 2, e % 2, t // 2, t % 2

    def at(self, z=None, y=None, x=None, c=None):
        z, y = self.z if z is None else z, self.y if y is None else y
        x, c = self.x if x is None else x, self.c if c is None else c
        return (z * 2 + y, x * 2 + c)

    def block(self, **where):
        e, t = self.at(**where)
        return e * 4 + t

    def near(self, k):
        table = ((0, 1, 2, 3), (1, 2, 0, 3), (2, 1, 3, 0), (3, 2, 1, 0))
        out = 0
        for z in range(DEPTH):
            if isinstance(k, int):
                column = table[z][k]
            else:
                column = table[z][0]
                for i in range(1, DEPTH):
                    column = jnp.where(k == i, table[z][i], column)
            out = jnp.where(self.z == z, column, out)
        return out

    def peers(self):
        line = [self.at(z=(self.z + d) % DEPTH) for d in range(1, DEPTH)]
        return line + [self.at(x=1 - self.x), self.at(y=1 - self.y), self.at(c=1 - self.c)]


class Copies:
    def __init__(self, send_sems, recv_sems):
        self.send_sems, self.recv_sems, self.used, self.made = send_sems, recv_sems, 0, []

    def make(self, src, dst, to):
        i = self.used
        self.used += 1
        copy = pltpu.make_async_remote_copy(
            src,
            dst,
            self.send_sems.at[i],
            self.recv_sems.at[i],
            device_id=to,
            device_id_type=MESH_ID,
        )
        self.made.append(copy)
        return copy

    def along(self, pieces, to, mine):
        base = self.used
        self.used += DEPTH
        out = []
        for (peer, src, dst), device in zip(pieces, to):
            there = pltpu.make_async_remote_copy(
                src,
                dst,
                self.send_sems.at[base + peer],
                self.recv_sems.at[base + mine],
                device_id=device,
                device_id_type=MESH_ID,
            )
            back = pltpu.make_async_remote_copy(
                src,
                dst,
                self.send_sems.at[base + peer],
                self.recv_sems.at[base + peer],
                device_id=device,
                device_id_type=MESH_ID,
            )
            self.made.append(there)
            out.append((there, back))
        return out

    def between(self, src, dst, to, send, recv):
        return pltpu.make_async_remote_copy(
            src,
            dst,
            self.send_sems.at[send],
            self.recv_sems.at[recv],
            device_id=to,
            device_id_type=MESH_ID,
        )

    def finish(self):
        for copy in self.made:
            copy.wait_send()


class LineSend:
    SEMS = DEPTH

    def __init__(self, p, copies, src, slot):
        others = [p.near(k) for k in range(1, DEPTH)]
        self.pairs = copies.along(
            [(z, src, slot(p.z)) for z in others], [p.at(z=z) for z in others], p.z
        )

    def start(self):
        for there, _ in self.pairs:
            there.start()

    def wait(self, k):
        self.pairs[k - 1][1].wait_recv()


class LineSum:
    SEMS = 4

    def __init__(self, p, copies, terms, arrived):
        base = copies.used
        copies.used += self.SEMS
        near = {k: p.at(z=p.near(k)) for k in range(1, DEPTH)}
        self.inner = (p.z == 1) | (p.z == 2)
        arrived = [arrived.at[i] for i in range(DEPTH)]
        self.terms, self.arrived = terms, arrived
        self.outer_to = {
            1: copies.between(terms[1], arrived[0], near[1], base, base),
            2: copies.between(terms[2], arrived[2], near[1], base + 1, base + 2),
            3: copies.between(terms[3], arrived[3], near[1], base + 2, base + 3),
        }
        self.inner_to = {
            2: copies.between(terms[2], arrived[0], near[2], base, base),
            1: copies.between(terms[1], arrived[1], near[1], base + 1, base + 1),
            3: copies.between(terms[3], arrived[1], near[3], base + 2, base + 1),
        }
        copies.made += self.outer_to.values()

    def send(self, k):
        pl.when(jnp.logical_not(self.inner))(self.outer_to[k].start)
        if k == 2:
            pl.when(self.inner)(self.inner_to[2].start)

    def relay(self):
        @pl.when(self.inner)
        def _():
            for k, behind in ((3, 3), (1, 2)):
                self.outer_to[behind].wait_recv()
                term = self.terms[k]
                term[...] = (term[...].astype(F32) + self.arrived[behind][...].astype(F32)).astype(
                    LOW
                )
                self.inner_to[k].start()

    def wait(self):
        self.inner_to[2].wait_recv()
        self.inner_to[1].wait_recv()
        return self.arrived[:2]


class StraightSum:
    SEMS = DEPTH

    def __init__(self, p, copies, terms, arrived):
        others = [p.near(k) for k in range(1, DEPTH)]
        slots = [arrived.at[p.near(k)] for k in range(1, DEPTH)]
        self.slots = slots
        self.pairs = copies.along(
            [(z, terms[k], arrived.at[p.z]) for k, z in enumerate(others, 1)],
            [p.at(z=z) for z in others],
            p.z,
        )

    def send(self, k):
        self.pairs[k - 1][0].start()

    def relay(self):
        pass

    def wait(self):
        for _, back in self.pairs:
            back.wait_recv()
        return self.slots


def enter(peers):
    barrier = pltpu.get_barrier_semaphore()
    for peer in peers:
        pl.semaphore_signal(barrier, inc=1, device_id=peer, device_id_type=MESH_ID)
    pl.semaphore_wait(barrier, len(peers))


def pieces_of(ref, rows):
    half = rows // 2

    def whole(b):
        return ref.at[pl.ds(pl.multiple_of(b * rows, rows), rows)]

    def first(b):
        return ref.at[pl.ds(pl.multiple_of(b * rows, rows), half)]

    def second(b):
        return ref.at[pl.ds(pl.multiple_of(b * rows + half, half), half)]

    return whole, first, second


GATHER_SEMS = LineSend.SEMS + 3 * DEPTH + 4 * DEPTH + 2 * DEPTH


def gather_steps(p, copies, rows, own_ref, all_ref, own_copy):
    whole, first, second = pieces_of(all_ref, rows)
    me = p.block()
    xn, yn, cn = p.at(x=1 - p.x), p.at(y=1 - p.y), p.at(c=1 - p.c)
    order = [p.near(k) for k in range(DEPTH)]
    line = LineSend(p, copies, own_ref, lambda z: whole(p.block(z=z)))
    to_x, to_y, near, far, diagonal = [], [], [], [], []
    for d in range(DEPTH):
        b = p.block(z=order[d])
        src = own_ref if d == 0 else whole(b)
        to_x.append(copies.make(src, whole(b), xn))
        to_y.append(copies.make(src, whole(b), yn))
        bx, by = p.block(z=order[d], x=1 - p.x), p.block(z=order[d], y=1 - p.y)
        bd = p.block(z=order[d], x=1 - p.x, y=1 - p.y)
        near.append([copies.make(src, whole(b), cn), copies.make(whole(bx), whole(bx), cn)])
        diagonal.append(
            (copies.make(first(bx), first(bx), yn), copies.make(second(by), second(by), xn))
        )
        far.append(
            [
                copies.make(whole(by), whole(by), cn),
                copies.make(first(bd), first(bd), cn),
                copies.make(second(bd), second(bd), cn),
            ]
        )

    def onward(d):
        if d:
            line.wait(d)
        to_x[d].start()
        to_y[d].start()
        near[d][0].start()

    def pair(d):
        to_x[d].wait_recv()
        diagonal[d][0].start()
        near[d][1].start()
        to_y[d].wait_recv()
        diagonal[d][1].start()
        far[d][0].start()

    def corner(d):
        for i in range(2):
            diagonal[d][i].wait_recv()
            far[d][1 + i].start()

    def arrived(group):
        for copy in group:
            copy.wait_recv()

    def begin():
        own_copy.start()
        line.start()
        onward(0)

    def step0():
        onward(1)
        pair(0)
        own_copy.wait()
        arrived(near[0])

    def step1():
        onward(2)
        pair(1)
        corner(0)
        arrived(far[0])

    def step3():
        onward(3)
        pair(2)
        corner(1)
        arrived(far[1])

    def step5():
        pair(3)
        corner(2)
        arrived(far[2])

    def step6():
        corner(3)
        arrived(near[3])

    return [
        begin,
        step0,
        step1,
        lambda: arrived(near[1]),
        step3,
        lambda: arrived(near[2]),
        step5,
        step6,
        lambda: arrived(far[3]),
    ]


SCATTER_SEMS = 16 + 8 + 8 + LineSum.SEMS


def scatter_scratch(rows, width):
    return [
        pltpu.VMEM((16, rows, width), LOW),
        pltpu.VMEM((2, DEPTH, rows // 2, width), LOW),
        pltpu.VMEM((2, DEPTH, rows, width), LOW),
        pltpu.VMEM((DEPTH, rows, width), LOW),
    ]


class Scatter:
    def __init__(self, p, copies, rows, part, core_in, diag_in, side_in, line_in, order, kind):
        whole, first, second = pieces_of(part, rows)
        positions = [p.near(k) for k in order]
        xn, yn, cn = p.at(x=1 - p.x), p.at(y=1 - p.y), p.at(c=1 - p.c)
        kinds = [dict(y=1 - p.y, x=1 - p.x), dict(x=1 - p.x), dict(y=1 - p.y), dict()]
        self.core_in, self.diag_in, self.side_in = core_in, diag_in, side_in
        self.order = order
        blocks = [[p.block(z=z, **kind) for kind in kinds] for z in positions]
        self.wholes = [[whole(b) for b in row] for row in blocks]
        self.first = [first(row[1]) for row in blocks]
        self.second = [second(row[2]) for row in blocks]
        self.core = [
            [
                copies.make(whole(p.block(z=z, c=1 - p.c, **kind)), core_in.at[k * 4 + j], cn)
                for j, kind in enumerate(kinds)
            ]
            for k, z in enumerate(positions)
        ]
        self.corners = [
            (
                copies.make(first(row[0]), diag_in.at[0, k], yn),
                copies.make(second(row[0]), diag_in.at[1, k], xn),
            )
            for k, row in enumerate(blocks)
        ]
        self.sides = [
            (
                copies.make(whole(row[1]), side_in.at[0, k], xn),
                copies.make(whole(row[2]), side_in.at[1, k], yn),
            )
            for k, row in enumerate(blocks)
        ]
        self.line = kind(
            p, copies, {order[k]: self.wholes[k][3] for k in range(DEPTH)}, line_in
        )

    def add(self, ref, *more):
        total = ref[...].astype(F32)
        for other in more:
            total = total + other[...].astype(F32)
        ref[...] = total.astype(LOW)

    def start(self, k):
        for copy in self.core[k]:
            copy.start()

    def corner(self, k):
        self.core[k][0].wait_recv()
        self.add(self.wholes[k][0], self.core_in.at[k * 4])
        for copy in self.corners[k]:
            copy.start()
        for j in (1, 2):
            self.core[k][j].wait_recv()
            self.add(self.wholes[k][j], self.core_in.at[k * 4 + j])

    def side(self, k):
        self.corners[k][0].wait_recv()
        self.add(self.first[k], self.diag_in.at[0, k])
        self.sides[k][0].start()
        self.corners[k][1].wait_recv()
        self.add(self.second[k], self.diag_in.at[1, k])
        self.sides[k][1].start()
        self.core[k][3].wait_recv()

    def close(self, k):
        for copy in self.sides[k]:
            copy.wait_recv()
        self.add(
            self.wholes[k][3],
            self.core_in.at[k * 4 + 3],
            self.side_in.at[0, k],
            self.side_in.at[1, k],
        )
        if self.order[k]:
            self.line.send(self.order[k])

    def relay(self, _):
        self.line.relay()

    def finish(self):
        total = self.wholes[self.order.index(0)][3][...].astype(F32)
        for term in self.line.wait():
            total = total + term[...].astype(F32)
        return total


def dot(left, right, left_dim, right_dim):
    return lax.dot_general(
        left, right, (((left_dim,), (right_dim,)), ((), ())), preferred_element_type=F32
    )


def semaphores(*counts):
    return [pltpu.SemaphoreType.DMA((n,)) for n in counts]


VMEM_SPEC = pl.BlockSpec(memory_space=pltpu.VMEM)
ANY_SPEC = pl.BlockSpec(memory_space=pl.ANY)


def experts_kernel(
    rows,
    width,
    experts,
    owned,
    own_ref,
    upstream_ref,
    gate_ref,
    up_ref,
    down_ref,
    grad_ref,
    moe_ref,
    gate_grad_ref,
    up_grad_ref,
    down_grad_ref,
    all_ref,
    upstream,
    outgoing,
    part,
    back_rows,
    core_in,
    diag_in,
    side_in,
    line_in,
    local_sems,
    gather_send,
    gather_recv,
    scatter_send,
    scatter_recv,
):
    p = Place()
    group = rows * 4
    units = down_ref.shape[0]
    hidden = units // owned
    extra = all_ref.shape[1] - width
    enter(p.peers())
    whole, _, _ = pieces_of(all_ref, rows)
    own_copy = pltpu.make_async_copy(own_ref, whole(p.block()), local_sems.at[0])
    gather_copies = Copies(gather_send, gather_recv)
    scatter_copies = Copies(scatter_send, scatter_recv)
    gathering = gather_steps(p, gather_copies, rows, own_ref, all_ref, own_copy)
    sums = Scatter(
        p,
        scatter_copies,
        rows,
        part,
        core_in,
        diag_in,
        side_in,
        line_in,
        list(range(DEPTH)),
        StraightSum,
    )

    def finish():
        grad_ref[...] = sums.finish()

    beside_work = {
        2: [(sums.start, 0)],
        3: [(sums.corner, 0)],
        4: [(sums.start, 1)],
        5: [(sums.corner, 1), (sums.side, 0)],
        6: [(sums.start, 2)],
        7: [(sums.corner, 2), (sums.side, 1), (sums.close, 0)],
    }
    beside_tiles = {
        0: [(sums.start, 3), (sums.side, 2), (sums.close, 1), (sums.corner, 3)],
        2: [(sums.side, 3)],
        3: [(sums.close, 2)],
        5: [(sums.close, 3)],
    }

    def run(actions):
        for stage, k in actions:
            stage(k)

    count = 2 * DEPTH

    def rows_of(i):
        side = jnp.where(i % 2 == 0, p.y, 1 - p.y)
        return pl.ds(pl.multiple_of((p.near(i // 2) * 2 + side) * group, group), group)

    def fetch(i):
        return pltpu.make_async_copy(
            upstream_ref.at[rows_of(i)], upstream.at[i % 2], local_sems.at[1 + i % 2]
        )

    def store(i):
        return pltpu.make_async_copy(
            outgoing.at[i % 2], moe_ref.at[rows_of(i)], local_sems.at[3 + i % 2]
        )

    fetch(0).start()
    gathering[0]()
    down_grad_ref[...] = jnp.zeros_like(down_grad_ref)
    first = p.e * owned
    lane = lax.broadcasted_iota(jnp.int32, (group, extra), 1)
    unit = lax.broadcasted_iota(jnp.int32, (group, units), 1)

    @pl.loop(0, count)
    def _(i):
        for k, actions in beside_work.items():
            pl.when(i == k)(functools.partial(run, actions))
        for k, step in enumerate(gathering[1:]):
            pl.when(i == k)(step)
        at = rows_of(i)
        x = all_ref[at, :width]
        gate = dot(x, gate_ref[...], 1, 1)
        up = dot(x, up_ref[...], 1, 1)
        tail = all_ref[at, width:].astype(F32)
        weights = [
            jnp.sum(
                jnp.where((lane == first + j) | (lane == experts + first + j), tail, 0.0),
                axis=1,
                keepdims=True,
            )
            for j in range(owned)
        ]
        weight = weights[0]
        for j in range(1, owned):
            weight = jnp.where(unit >= j * hidden, weights[j], weight)
        sigmoid = 1.0 / (1.0 + jnp.exp(-gate))
        activated = gate * sigmoid
        inner = activated * up
        weighted = (inner * weight).astype(LOW)

        @pl.when(i >= 2)
        def _():
            store(i - 2).wait()

        outgoing[i % 2] = dot(weighted, down_ref[...], 1, 0).astype(LOW)
        store(i).start()
        fetch(i).wait()

        @pl.when(i + 1 < count)
        def _():
            fetch(i + 1).start()

        u = upstream[i % 2]
        down_back = dot(u, down_ref[...], 1, 1)
        down_grad_ref[...] += dot(weighted, u, 0, 0)
        product = inner * down_back
        note = jnp.zeros((group, extra), F32)
        for j in range(owned):
            mine = (unit >= j * hidden) & (unit < (j + 1) * hidden)
            route_grad = jnp.sum(jnp.where(mine, product, 0.0), axis=1, keepdims=True)
            note = jnp.where(lane == first + j, route_grad, note)
        inner_grad = down_back * weight
        gate_back = (inner_grad * up * sigmoid * (1.0 + gate * (1.0 - sigmoid))).astype(LOW)
        up_back = (inner_grad * activated).astype(LOW)
        back_rows[at, :units] = gate_back
        back_rows[at, units:] = up_back
        part[at, :width] = (
            dot(gate_back, gate_ref[...], 1, 0) + dot(up_back, up_ref[...], 1, 0)
        ).astype(LOW)
        part[at, width:] = note.astype(LOW)

    tile = width // count

    @pl.loop(0, count)
    def _(i):
        for k, actions in beside_tiles.items():
            pl.when(i == k)(functools.partial(run, actions))
        at = pl.ds(pl.multiple_of(i * tile, tile), tile)
        x = all_ref[:, at]
        gate_grad_ref[:, at] = dot(back_rows[:, :units], x, 0, 0)
        up_grad_ref[:, at] = dot(back_rows[:, units:], x, 0, 0)

    finish()
    gather_copies.finish()
    scatter_copies.finish()
    store(count - 2).wait()
    store(count - 1).wait()


def run_experts(own, upstream_all, gate, up, down, owned, experts, width, collective_id):
    rows, full = own.shape
    total = upstream_all.shape[0]
    units = down.shape[0]
    group = rows * lax.axis_size("tensor")
    return pl.pallas_call(
        functools.partial(experts_kernel, rows, width, experts, owned),
        out_shape=(
            jax.ShapeDtypeStruct((rows, full), F32),
            jax.ShapeDtypeStruct((total, width), LOW),
            *[jax.ShapeDtypeStruct((units, width), F32)] * 3,
        ),
        in_specs=[VMEM_SPEC, ANY_SPEC, VMEM_SPEC, VMEM_SPEC, VMEM_SPEC],
        out_specs=(VMEM_SPEC, ANY_SPEC, VMEM_SPEC, VMEM_SPEC, VMEM_SPEC),
        scratch_shapes=[
            pltpu.VMEM((total, full), LOW),
            pltpu.VMEM((2, group, width), LOW),
            pltpu.VMEM((2, group, width), LOW),
            pltpu.VMEM((total, full), LOW),
            pltpu.VMEM((total, 2 * units), LOW),
        ]
        + scatter_scratch(rows, full)
        + semaphores(5, GATHER_SEMS, GATHER_SEMS, SCATTER_SEMS, SCATTER_SEMS),
        compiler_params=pltpu.CompilerParams(
            collective_id=collective_id, has_side_effects=True, vmem_limit_bytes=64000000
        ),
        name="experts",
    )(own, upstream_all, gate, up, down)


def normed_rows(values):
    scale = lax.rsqrt(jnp.mean(values * values, axis=-1, keepdims=True) + EPSILON)
    return values * scale, scale


def turned(values):
    return pltpu.roll(values, values.shape[-1] // 2, values.ndim - 1)


def allowed_keys(count, length):
    row = lax.broadcasted_iota(jnp.int32, (count, count), 0)
    column = lax.broadcasted_iota(jnp.int32, (count, count), 1)
    return (column <= row) & (column < length)


def attention_probs(query, key, allowed):
    factor = query.shape[-1] ** (-0.5)
    scores = jnp.where(allowed, dot(query, key, 1, 1) * factor, NEGATIVE)
    expo = jnp.exp(scores - jnp.max(scores, axis=-1, keepdims=True))
    return expo / jnp.sum(expo, axis=-1, keepdims=True)


class Spread:
    def __init__(self, p, copies, slot):
        other = (1 - p.x) * 2 + p.c
        self.to_x = copies.make(slot(p.t), slot(p.t), p.at(x=1 - p.x))
        self.to_c = copies.make(slot(p.t), slot(p.t), p.at(c=1 - p.c))
        self.onward = copies.make(slot(other), slot(other), p.at(c=1 - p.c))

    def start(self):
        self.to_x.start()
        self.to_c.start()

    def forward(self):
        self.to_x.wait_recv()
        self.onward.start()

    def finish(self):
        self.to_c.wait_recv()
        self.onward.wait_recv()


class Fold:
    def __init__(self, p, copies, rows, part, arrived):
        def block(t):
            return part.at[pl.ds(pl.multiple_of(t * rows, rows), rows)]

        cn, xn = p.at(c=1 - p.c), p.at(x=1 - p.x)
        self.arrived, self.own, self.other = arrived, block(p.t), block((1 - p.x) * 2 + p.c)
        self.to_c = [
            copies.make(block((1 - p.x) * 2 + 1 - p.c), arrived.at[0], cn),
            copies.make(block(p.x * 2 + 1 - p.c), arrived.at[1], cn),
        ]
        self.to_x = copies.make(self.other, arrived.at[2], xn)

    def start(self):
        for copy in self.to_c:
            copy.start()

    def forward(self):
        self.to_c[0].wait_recv()
        self.other[...] = (self.other[...].astype(F32) + self.arrived[0].astype(F32)).astype(LOW)
        self.to_x.start()

    def finish(self):
        self.to_c[1].wait_recv()
        self.to_x.wait_recv()
        return (
            self.own[...].astype(F32) + self.arrived[1].astype(F32) + self.arrived[2].astype(F32)
        )


FOLD_SEMS = 3
FRONT_SEMS = FOLD_SEMS + 2 * LineSend.SEMS


def front_kernel(
    rows,
    experts,
    length_ref,
    tokens_ref,
    cotangent_ref,
    routes_ref,
    attention_gain_ref,
    query_gain_ref,
    key_gain_ref,
    routing_gain_ref,
    cosine_ref,
    sine_ref,
    query_weight_ref,
    key_weight_ref,
    value_weight_ref,
    output_weight_ref,
    router_weight_ref,
    upstream_ref,
    xnorm1_ref,
    query_ref,
    key_ref,
    value_ref,
    heads_ref,
    line_heads_ref,
    hidden_ref,
    own_ref,
    router_ref,
    part,
    part_in,
    local_sems,
    gather_send,
    gather_recv,
    send_sems,
    recv_sems,
):
    p = Place()
    group, width = tokens_ref.shape
    units = query_ref.shape[1]
    size = cosine_ref.shape[1]
    count = units // size
    length = length_ref[0]
    enter(p.peers())
    copies = Copies(send_sems, recv_sems)
    gather_copies = Copies(gather_send, gather_recv)
    mine = pl.ds(pl.multiple_of(p.t * rows, rows), rows)
    whole, _, _ = pieces_of(upstream_ref, rows)
    own_cotangent = cotangent_ref.at[mine]
    own_copy = pltpu.make_async_copy(own_cotangent, whole(p.block()), local_sems.at[0])
    gathering = gather_steps(p, gather_copies, rows, own_cotangent, upstream_ref, own_copy)
    fold = Fold(p, copies, rows, part, part_in)
    line = [
        LineSend(
            p,
            copies,
            heads_ref.at[:, a:b],
            lambda z, a=a, b=b: line_heads_ref.at[z, :, a:b],
        )
        for a, b in ((0, units // 2), (units // 2, units))
    ]

    def send_heads(i):
        line[i].start()

    gathering[0]()

    normed1, _ = normed_rows(tokens_ref[...].astype(F32))
    xnorm1_ref[...] = (normed1 * attention_gain_ref[...]).astype(LOW)
    query_ref[...] = dot(xnorm1_ref[...], query_weight_ref[...], 1, 0)
    key_ref[...] = dot(xnorm1_ref[...], key_weight_ref[...], 1, 0)
    value_ref[...] = dot(xnorm1_ref[...], value_weight_ref[...], 1, 0).astype(LOW)
    gathering[1]()
    cosine, sine = cosine_ref[...], sine_ref[...]
    query_gain = query_gain_ref[...]
    valid = lax.broadcasted_iota(jnp.int32, (group, 1), 0) < length
    allowed = allowed_keys(group, length)
    key_hat, _ = normed_rows(key_ref[...])
    key_gained = key_hat * key_gain_ref[...]
    key_low = (key_gained * cosine + turned(key_gained) * sine).astype(LOW)

    @pl.loop(0, count)
    def _(h):
        pl.when(h == count // 2)(functools.partial(send_heads, 0))
        for k in (2, 3):
            pl.when(h == 2 * k)(gathering[k])
        at = pl.ds(pl.multiple_of(h * size, size), size)
        hat, _ = normed_rows(query_ref[:, at])
        gained = hat * query_gain
        query_low = (gained * cosine + turned(gained) * sine).astype(LOW)
        probs = attention_probs(query_low, key_low, allowed).astype(LOW)
        heads_ref[:, at] = jnp.where(valid, dot(probs, value_ref[...], 1, 0), 0.0).astype(LOW)

    send_heads(1)
    part[...] = dot(heads_ref[...], output_weight_ref[...], 1, 1).astype(LOW)
    fold.start()
    gathering[4]()
    fold.forward()
    gathering[5]()
    hidden = tokens_ref[mine, :].astype(F32) + fold.finish()
    hidden_ref[...] = hidden
    normed2, _ = normed_rows(hidden)
    xnorm2 = (normed2 * routing_gain_ref[...]).astype(LOW)
    own_ref[:, :width] = xnorm2
    gathering[6]()
    logits = dot(xnorm2, router_weight_ref[...], 1, 1)
    lanes = logits.shape[1]
    lane = lax.broadcasted_iota(jnp.int32, logits.shape, 1)
    peak = jnp.max(jnp.where(lane < experts, logits, NEGATIVE), axis=1, keepdims=True)
    expo = jnp.where(lane < experts, jnp.exp(jnp.minimum(logits - peak, 0.0)), 0.0)
    router = expo / jnp.sum(expo, axis=1, keepdims=True)
    named = jnp.zeros(logits.shape, F32)
    for k in range(routes_ref.shape[1]):
        named = jnp.where(routes_ref[:, k : k + 1] == lane, 1.0, named)
    chosen = router * named
    route_weight = chosen / jnp.sum(chosen, axis=1, keepdims=True)
    high = route_weight.astype(LOW).astype(F32)
    own_ref[:, width:] = (high + pltpu.roll(route_weight - high, experts, 1)).astype(LOW)
    router_ref[:, :lanes] = router
    router_ref[:, lanes : 2 * lanes] = route_weight
    router_ref[:, 2 * lanes :] = named
    gathering[7]()
    gathering[8]()
    for half in line:
        for k in range(1, DEPTH):
            half.wait(k)
    gather_copies.finish()
    copies.finish()


def run_front(
    length,
    tokens,
    cotangent,
    routes,
    attention_gain,
    query_gain,
    key_gain,
    routing_gain,
    cosine,
    sine,
    query_weight,
    key_weight,
    value_weight,
    output_weight,
    router_weight,
    experts,
    collective_id,
):
    group, width = tokens.shape
    rows = routes.shape[0]
    lanes = router_weight.shape[0]
    total = group * lax.axis_size("expert")
    struct = jax.ShapeDtypeStruct
    return pl.pallas_call(
        functools.partial(front_kernel, rows, experts),
        out_shape=(
            struct((total, width), LOW),
            struct((group, width), LOW),
            struct((group, query_weight.shape[1]), F32),
            struct((group, key_weight.shape[1]), F32),
            struct((group, value_weight.shape[1]), LOW),
            struct((group, query_weight.shape[1]), LOW),
            struct((DEPTH, group, query_weight.shape[1]), LOW),
            struct((rows, width), F32),
            struct((rows, width + lanes), LOW),
            struct((rows, 3 * lanes), F32),
        ),
        in_specs=[pl.BlockSpec(memory_space=pltpu.SMEM), VMEM_SPEC, ANY_SPEC] + [VMEM_SPEC] * 12,
        out_specs=[ANY_SPEC] + [VMEM_SPEC] * 5 + [ANY_SPEC] + [VMEM_SPEC] * 3,
        scratch_shapes=[pltpu.VMEM((group, width), LOW), pltpu.VMEM((3, rows, width), LOW)]
        + semaphores(1, GATHER_SEMS, GATHER_SEMS, FRONT_SEMS, FRONT_SEMS),
        compiler_params=pltpu.CompilerParams(
            collective_id=collective_id, has_side_effects=True, vmem_limit_bytes=60000000
        ),
        name="front",
    )(
        length,
        tokens,
        cotangent,
        routes,
        attention_gain,
        query_gain,
        key_gain,
        routing_gain,
        cosine,
        sine,
        query_weight,
        key_weight,
        value_weight,
        output_weight,
        router_weight,
    )


SPREAD_SEMS = 3
TAIL_SEMS = 4 * SPREAD_SEMS + DEPTH + DEPTH + 2 + 2 * LineSum.SEMS + 1 + 3 + 3 + DEPTH


def tail_kernel(
    rows,
    experts,
    length_ref,
    summed_ref,
    own_ref,
    router_ref,
    hidden_ref,
    cotangent_ref,
    tokens_ref,
    xnorm1_ref,
    moe_ref,
    heads_ref,
    line_heads_ref,
    query_ref,
    key_ref,
    value_ref,
    cosine_ref,
    sine_ref,
    attention_gain_ref,
    routing_gain_ref,
    query_gain_ref,
    key_gain_ref,
    query_weight_ref,
    key_weight_ref,
    value_weight_ref,
    output_weight_ref,
    router_weight_ref,
    mixed_ref,
    tokens_grad_ref,
    output_grad_ref,
    packed_grad_ref,
    small_out_ref,
    hidden_grad_ref,
    hidden_low_ref,
    hidden_all,
    hidden_line,
    line_heads,
    heads_grad,
    packed,
    packed_in,
    xnorm_in,
    weight_out,
    weight_in,
    output_out,
    output_in,
    key_sum,
    value_sum,
    back_part,
    back_in,
    moe,
    small,
    small_in,
    small_side,
    small_line,
    core_in,
    diag_in,
    side_in,
    line_in,
    local_sems,
    send_sems,
    recv_sems,
    scatter_send,
    scatter_recv,
):
    p = Place()
    group, width = xnorm1_ref.shape
    units = query_ref.shape[1]
    size = cosine_ref.shape[1]
    count = units // size
    packed_width = packed.shape[1]
    share = width // (2 * DEPTH)
    length = length_ref[0]
    fetch = [
        pltpu.make_async_copy(moe_ref, moe, local_sems.at[0]),
        *[
            pltpu.make_async_copy(
                line_heads_ref.at[p.near(k)], line_heads.at[p.near(k)], local_sems.at[k]
            )
            for k in range(1, DEPTH)
        ],
    ]
    for copy in fetch:
        copy.start()
    enter(p.peers())
    copies = Copies(send_sems, recv_sems)
    scatter_copies = Copies(scatter_send, scatter_recv)
    sums = Scatter(
        p,
        scatter_copies,
        rows,
        moe,
        core_in,
        diag_in,
        side_in,
        line_in,
        [3, 2, 1, 0],
        LineSum,
    )
    xn, yn, cn = p.at(x=1 - p.x), p.at(y=1 - p.y), p.at(c=1 - p.c)
    order = [p.near(k) for k in reversed(range(DEPTH))]
    along = [p.at(z=z) for z in order[: DEPTH - 1]]

    def columns(z, y):
        return pl.ds(pl.multiple_of((z * 2 + y) * share, share), share)

    def block(ref, t):
        return ref.at[pl.ds(pl.multiple_of(t * rows, rows), rows)]

    hidden_spread = Spread(p, copies, lambda t: block(hidden_all, t))
    line_spread = Spread(p, copies, lambda t: hidden_line.at[t])
    hidden_to = copies.along(
        [
            (
                z,
                hidden_low_ref.at[:, pl.ds(pl.multiple_of(z * 2 * share, share), 2 * share)],
                hidden_line.at[p.t, p.z],
            )
            for z in order[: DEPTH - 1]
        ],
        along,
        p.z,
    )
    xnorm_to = [
        copies.make(xnorm1_ref.at[:, columns(z, 1 - p.y)], xnorm_in.at[z], yn) for z in range(DEPTH)
    ]
    cuts = [(0, units // 2), (units // 2, packed_width)]
    packed_to = [copies.make(packed.at[:, a:b], packed_in.at[:, a:b], yn) for a, b in cuts]
    weight_sums = [
        LineSum(
            p,
            copies,
            {k: weight_out.at[k - 1, :, a:b] for k in range(1, DEPTH)},
            weight_in.at[:, :, a:b],
        )
        for a, b in cuts
    ]
    output_to = copies.make(output_out, output_in, yn)
    fold = Fold(p, copies, rows, back_part, back_in)
    tokens_spread = Spread(p, copies, lambda t: block(tokens_grad_ref, t))
    mixed_spread = Spread(p, copies, lambda t: block(mixed_ref, t))
    small_to_c = copies.make(small, small_in.at[0], cn)
    small_to_x = copies.make(small, small_in.at[1], xn)
    small_to_y = copies.make(small_side.at[0], small_side.at[1], yn)
    small_to = copies.along(
        [(z, small_side.at[2, z], small_line.at[p.z]) for z in order[: DEPTH - 1]], along, p.z
    )

    lanes = router_weight_ref.shape[0]
    gain_row = experts + 2
    route_grad = summed_ref[:, width:]
    router = router_ref[:, :lanes]
    route_weight = router_ref[:, lanes : 2 * lanes]
    named = router_ref[:, 2 * lanes :]
    chosen_total = jnp.sum(router * named, axis=1, keepdims=True)
    inner_total = jnp.sum(route_grad * route_weight, axis=1, keepdims=True)
    prob_grad = named * (route_grad - inner_total) / chosen_total
    logit_low = (router * (prob_grad - jnp.sum(router * prob_grad, axis=1, keepdims=True))).astype(
        LOW
    )
    small[...] = jnp.zeros_like(small)
    small[:experts, :] = dot(logit_low, own_ref[:, :width], 0, 0)[:experts]
    fetch[0].wait()
    for k in range(DEPTH):
        sums.start(k)
    xnorm2_grad = summed_ref[:, :width] + dot(logit_low, router_weight_ref[...], 1, 0)
    normed2, scale2 = normed_rows(hidden_ref[...])
    small[experts : experts + 1, :] = jnp.sum(xnorm2_grad * normed2, axis=0, keepdims=True)
    inner2 = xnorm2_grad * routing_gain_ref[...]
    hidden_grad_ref[...] = cotangent_ref[...].astype(F32) + scale2 * (
        inner2 - normed2 * jnp.mean(inner2 * normed2, axis=-1, keepdims=True)
    )
    hidden_low_ref[...] = hidden_grad_ref[...].astype(LOW)
    block(hidden_all, p.t)[...] = hidden_low_ref[...]
    hidden_line[p.t, p.z] = hidden_low_ref[
        :, pl.ds(pl.multiple_of(p.z * 2 * share, share), 2 * share)
    ]
    for there, _ in hidden_to:
        there.start()
    hidden_spread.start()
    for copy in xnorm_to:
        copy.start()
    key_sum[...] = jnp.zeros_like(key_sum)
    value_sum[...] = jnp.zeros_like(value_sum)
    sums.corner(0)
    hidden_spread.forward()
    sums.corner(1)
    sums.corner(2)
    hidden_spread.finish()

    valid = lax.broadcasted_iota(jnp.int32, (group, 1), 0) < length
    allowed = allowed_keys(group, length)
    heads_grad[...] = jnp.where(
        valid, dot(hidden_all[...], output_weight_ref[...], 1, 0), 0.0
    ).astype(LOW)
    cosine, sine = cosine_ref[...], sine_ref[...]
    query_gain, key_gain = query_gain_ref[...], key_gain_ref[...]
    factor = size ** (-0.5)
    key_hat, key_scale = normed_rows(key_ref[...])
    key_gained = key_hat * key_gain
    key_low = (key_gained * cosine + turned(key_gained) * sine).astype(LOW)

    def norm_back(grad, hat, scale, gain):
        grad = grad * cosine - turned(grad) * sine
        gain_part = jnp.sum(grad * hat, axis=0, keepdims=True)
        inner = grad * gain
        return scale * (inner - hat * jnp.mean(inner * hat, axis=-1, keepdims=True)), gain_part

    def one_head(h):
        at = pl.ds(pl.multiple_of(h * size, size), size)
        hat, scale = normed_rows(query_ref[:, at])
        gained = hat * query_gain
        query_low = (gained * cosine + turned(gained) * sine).astype(LOW)
        probs = attention_probs(query_low, key_low, allowed)
        grad = heads_grad[:, at]
        probs_grad = dot(grad, value_ref[...], 1, 1)
        delta = jnp.sum(probs * probs_grad, axis=-1, keepdims=True)
        score_grad = (probs * (probs_grad - delta)).astype(LOW)
        key_sum[...] += dot(score_grad, query_low, 0, 0)
        value_sum[...] += dot(probs.astype(LOW), grad, 0, 0)
        back, gain_part = norm_back(
            dot(score_grad, key_low, 1, 0) * factor, hat, scale, query_gain
        )
        packed[:, at] = back.astype(LOW)
        small[gain_row : gain_row + 1, :size] += gain_part

    pl.loop(0, count // 2)(one_head)
    packed_to[0].start()
    sums.corner(3)
    sums.side(0)
    for _, back in hidden_to:
        back.wait_recv()
    line_spread.start()
    pl.loop(count // 2, count)(one_head)
    key_back, key_part = norm_back(key_sum[...] * factor, key_hat, key_scale, key_gain)
    packed[:, units : units + size] = key_back.astype(LOW)
    packed[:, units + size :] = value_sum[...].astype(LOW)
    packed_to[1].start()
    small[gain_row + 1 : gain_row + 2, :size] = key_part
    for row in (gain_row, gain_row + 1):
        part = small[row : row + 1, :size]
        for i in range(1, width // size):
            small[row : row + 1, i * size : (i + 1) * size] = part
    line_spread.forward()
    sums.side(1)
    back_part[...] = (
        dot(packed[:, :units], query_weight_ref[...], 1, 1)
        + dot(packed[:, units : units + size], key_weight_ref[...], 1, 1)
        + dot(packed[:, units + size :], value_weight_ref[...], 1, 1)
    ).astype(LOW)
    fold.start()
    for copy in xnorm_to:
        copy.wait_recv()

    def weight_piece(i):
        a, b = cuts[i]
        packed_to[i].wait_recv()
        for k in reversed(range(DEPTH)):
            z = p.near(k)
            grad = dot(xnorm1_ref[:, columns(z, p.y)], packed[:, a:b], 0, 0) + dot(
                xnorm_in[z], packed_in[:, a:b], 0, 0
            )
            if k:
                weight_out[k - 1, :, a:b] = grad.astype(LOW)
                weight_sums[i].send(k)
            else:
                packed_grad_ref[:, a:b] = grad

    weight_piece(0)
    fold.forward()
    sums.side(2)
    weight_sums[0].relay()
    weight_piece(1)
    sums.side(3)
    sums.close(0)

    xnorm1_grad = fold.finish()
    normed1, scale1 = normed_rows(tokens_ref[...].astype(F32))
    small[gain_row - 1 : gain_row, :] = jnp.sum(xnorm1_grad * normed1, axis=0, keepdims=True)
    small_to_c.start()
    inner = xnorm1_grad * attention_gain_ref[...]
    block(tokens_grad_ref, p.t)[...] = (
        hidden_grad_ref[...]
        + scale1 * (inner - normed1 * jnp.mean(inner * normed1, axis=-1, keepdims=True))
    ).astype(LOW)
    tokens_spread.start()

    line_spread.finish()
    for copy in fetch[1:]:
        copy.wait()

    def output_piece(y):
        at = pl.ds(pl.multiple_of(y * share, share), share)
        grad = dot(hidden_line[:, p.z, :, at].reshape(group, share), heads_ref[...], 0, 0)
        for k in range(1, DEPTH):
            z = p.near(k)
            grad += dot(hidden_line[:, z, :, at].reshape(group, share), line_heads[z], 0, 0)
        return grad

    output_out[...] = output_piece(1 - p.y).astype(LOW)
    output_to.start()
    output_grad_ref[...] = output_piece(p.y)
    weight_sums[1].relay()
    sums.close(1)
    small_to_c.wait_recv()
    small_to_c.wait_send()
    small[...] += small_in[0]
    small_to_x.start()
    tokens_spread.forward()
    sums.close(2)
    sums.close(3)
    sums.relay(0)
    small_to_x.wait_recv()
    small_to_x.wait_send()
    small[...] += small_in[1]
    for z in range(DEPTH):
        small_side[0, z] = small[:, columns(z, 1 - p.y)]
        small_side[2, z] = small[:, columns(z, p.y)]
    small_to_y.start()
    output_to.wait_recv()
    output_grad_ref[...] += output_in[...].astype(F32)
    small_to_y.wait_recv()
    small_side[2] += small_side[1]
    for there, _ in small_to:
        there.start()
    tokens_spread.finish()
    block(mixed_ref, p.t)[...] = (hidden_ref[...] + sums.finish()).astype(LOW)
    mixed_spread.start()
    small_total = small_side[2, p.z]
    for (_, back), z in zip(small_to, order):
        back.wait_recv()
        small_total += small_line[z]
    small_out_ref[...] = small_total
    mixed_spread.forward()
    mixed_spread.finish()
    for i, (a, b) in enumerate(cuts):
        for term in weight_sums[i].wait():
            packed_grad_ref[:, a:b] += term[...].astype(F32)
    for copy in copies.made:
        if copy is not small_to_c and copy is not small_to_x:
            copy.wait_send()
    scatter_copies.finish()


def run_tail(
    length,
    summed,
    own,
    router,
    hidden,
    cotangent,
    tokens,
    xnorm1,
    moe,
    heads,
    line_heads,
    query,
    key,
    value,
    cosine,
    sine,
    attention_gain,
    routing_gain,
    query_gain,
    key_gain,
    query_weight,
    key_weight,
    value_weight,
    output_weight,
    router_weight,
    experts,
    collective_id,
):
    group, width = xnorm1.shape
    rows = hidden.shape[0]
    units, size = query.shape[1], cosine.shape[1]
    packed_width = units + 2 * size
    share = width // (2 * DEPTH)
    tensors = group // rows
    smalls = (experts + 4 + 7) // 8 * 8
    vmem = pltpu.VMEM
    return pl.pallas_call(
        functools.partial(tail_kernel, rows, experts),
        out_shape=(
            jax.ShapeDtypeStruct((group, width), LOW),
            jax.ShapeDtypeStruct((group, width), LOW),
            jax.ShapeDtypeStruct((share, units), F32),
            jax.ShapeDtypeStruct((share, packed_width), F32),
            jax.ShapeDtypeStruct((smalls, share), F32),
        ),
        in_specs=[pl.BlockSpec(memory_space=pltpu.SMEM)]
        + [VMEM_SPEC] * 7
        + [ANY_SPEC, VMEM_SPEC, ANY_SPEC]
        + [VMEM_SPEC] * 14,
        out_specs=[VMEM_SPEC] * 5,
        scratch_shapes=[
            vmem((rows, width), F32),
            vmem((rows, width), LOW),
            vmem((group, width), LOW),
            vmem((tensors, DEPTH, rows, 2 * share), LOW),
            vmem((DEPTH, group, units), LOW),
            vmem((group, units), LOW),
            vmem((group, packed_width), LOW),
            vmem((group, packed_width), LOW),
            vmem((DEPTH, group, share), LOW),
            vmem((DEPTH - 1, share, packed_width), LOW),
            vmem((DEPTH, share, packed_width), LOW),
            vmem((share, units), LOW),
            vmem((share, units), LOW),
            vmem((group, size), F32),
            vmem((group, size), F32),
            vmem((group, width), LOW),
            vmem((3, rows, width), LOW),
            vmem(moe.shape, LOW),
            vmem((smalls, width), F32),
            vmem((2, smalls, width), F32),
            vmem((3, DEPTH, smalls, share), F32),
            vmem((DEPTH, smalls, share), F32),
        ]
        + scatter_scratch(rows, width)
        + semaphores(DEPTH, TAIL_SEMS, TAIL_SEMS, SCATTER_SEMS, SCATTER_SEMS),
        compiler_params=pltpu.CompilerParams(
            collective_id=collective_id, has_side_effects=True, vmem_limit_bytes=64000000
        ),
        name="tail",
    )(
        length,
        summed,
        own,
        router,
        hidden,
        cotangent,
        tokens,
        xnorm1,
        moe,
        heads,
        line_heads,
        query,
        key,
        value,
        cosine,
        sine,
        attention_gain,
        routing_gain,
        query_gain,
        key_gain,
        query_weight,
        key_weight,
        value_weight,
        output_weight,
        router_weight,
    )


def gathered_shards(
    tokens,
    seq_length,
    expert_routes,
    attention_gain,
    query_weight,
    key_weight,
    value_weight,
    query_gain,
    key_gain,
    output_weight,
    routing_gain,
    router_weight,
    gate_weight,
    up_weight,
    down_weight,
    cotangent,
):
    count, width = tokens.shape
    head_size = query_gain.shape[0]
    experts = router_weight.shape[1]
    owned = gate_weight.shape[0]
    part = lax.axis_index("tensor")
    owner = lax.axis_index("expert")
    rows = count // lax.axis_size("tensor")

    def own_rows(values):
        return lax.dynamic_slice_in_dim(values, part * rows, rows, 0)

    cosine, sine = rope_tables(count, head_size)
    half = head_size // 2
    sine = jnp.concatenate([-sine[:, :half], sine[:, half:]], axis=1)
    router_wide = jnp.pad(router_weight.T, ((0, 128 - experts), (0, 0)))
    upstream_all, xnorm1, query, key, value, heads, line_heads, hidden, own, router = run_front(
        seq_length,
        tokens,
        cotangent,
        own_rows(expert_routes),
        attention_gain[None],
        query_gain[None],
        key_gain[None],
        routing_gain[None],
        cosine,
        sine,
        query_weight,
        key_weight,
        value_weight,
        output_weight,
        router_wide,
        experts,
        0,
    )

    def by_unit(weight):
        return weight.transpose(0, 2, 1).reshape(-1, width)

    def from_units(grad):
        return grad.reshape(owned, -1, width).transpose(0, 2, 1)

    summed, moe_part, gate_grad, up_grad, down_grad = run_experts(
        own,
        upstream_all,
        by_unit(gate_weight),
        by_unit(up_weight),
        down_weight.reshape(-1, width),
        owned,
        experts,
        width,
        1,
    )
    mixed, tokens_grad, output_grad, packed_grad, small_sum = run_tail(
        seq_length,
        summed,
        own,
        router,
        hidden,
        own_rows(cotangent),
        own_rows(tokens),
        xnorm1,
        moe_part,
        heads,
        line_heads,
        query,
        key,
        value,
        cosine,
        sine,
        attention_gain[None],
        routing_gain[None],
        query_gain[None],
        key_gain[None],
        query_weight,
        key_weight,
        value_weight,
        output_weight,
        router_wide,
        experts,
        2,
    )
    query_end = query_weight.shape[1]
    key_end = query_end + key_weight.shape[1]
    share = head_size // lax.axis_size("expert")

    def own_gain(row):
        return lax.dynamic_slice_in_dim(small_sum[row], owner * share, share, 0)

    return (
        mixed,
        tokens_grad,
        small_sum[experts + 1],
        packed_grad[:, :query_end],
        packed_grad[:, query_end:key_end],
        packed_grad[:, key_end:],
        own_gain(experts + 2),
        own_gain(experts + 3),
        output_grad,
        small_sum[experts],
        small_sum[:experts].T,
        from_units(gate_grad),
        from_units(up_grad),
        down_grad.reshape(down_weight.shape),
    )


def solution(mesh):
    sizes = dict(mesh.shape)
    fits = sizes["expert"] == 2 * DEPTH and sizes["tensor"] == 4
    return jax.shard_map(
        gathered_shards if fits else routed_shards,
        mesh=mesh,
        in_specs=(
            P("expert", None),
            P("expert"),
            P("expert", None),
            P(),
            P(None, "tensor"),
            P(None, "tensor"),
            P(None, "tensor"),
            P(),
            P(),
            P(None, "tensor"),
            P(),
            P(),
            P("expert", None, "tensor"),
            P("expert", None, "tensor"),
            P("expert", "tensor", None),
            P("expert", None),
        ),
        out_specs=(
            P("expert", None),
            P("expert", None),
            P("expert"),
            P("expert", "tensor"),
            P("expert", "tensor"),
            P("expert", "tensor"),
            P("expert"),
            P("expert"),
            P("expert", "tensor"),
            P("expert"),
            P("expert", None),
            P("expert", None, "tensor"),
            P("expert", None, "tensor"),
            P("expert", "tensor", None),
        ),
        check_vma=False,
    )
```

```python
import functools

import jax
import jax.numpy as jnp
from jax import lax
from jax.experimental import pallas as pl
from jax.experimental.pallas import tpu as pltpu
from jax.sharding import PartitionSpec as P

EPSILON = 1e-06
THETA = 1000000.0
NEGATIVE = -1e30


def rms_scale(values):
    return lax.rsqrt(jnp.mean(values * values, axis=-1, keepdims=True) + EPSILON)


def rope_tables(count, width):
    half = width // 2
    freqs = THETA ** (-(jnp.arange(half, dtype=jnp.float32) * 2.0 / width))
    angles = jnp.arange(count, dtype=jnp.float32)[:, None] * freqs[None, :]
    cosine = jnp.concatenate([jnp.cos(angles), jnp.cos(angles)], axis=1)
    sine = jnp.concatenate([jnp.sin(angles), jnp.sin(angles)], axis=1)
    return (cosine, sine)


def rotate(values, cosine, sine):
    half = values.shape[-1] // 2
    turned = jnp.concatenate([-values[..., half:], values[..., :half]], axis=-1)
    return values * cosine[:, None, :] + turned * sine[:, None, :]


def rotate_back(grads, cosine, sine):
    half = grads.shape[-1] // 2
    scaled = grads * sine[:, None, :]
    turned = jnp.concatenate([scaled[..., half:], -scaled[..., :half]], axis=-1)
    return grads * cosine[:, None, :] + turned


def head_norm(values, gain):
    scale = rms_scale(values)
    normed = values * scale
    return (normed * gain, normed, scale)


def head_norm_back(grads, normed, scale, gain):
    gain_grad = jnp.sum(grads * normed, axis=(0, 1))
    inner = grads * gain
    values_grad = scale * (inner - normed * jnp.mean(inner * normed, axis=-1, keepdims=True))
    return (values_grad, gain_grad)


def contract(left, right, left_dim, right_dim):
    return lax.dot_general(
        left, right, (((left_dim,), (right_dim,)), ((), ())), preferred_element_type=jnp.float32
    )


def block_scores(qblock, start, keys, length):
    block = qblock.shape[0]
    count = keys.shape[0]
    factor = qblock.shape[-1] ** (-0.5)
    rows = start + jnp.arange(block, dtype=jnp.int32)
    columns = jnp.arange(count, dtype=jnp.int32)
    allowed = (columns[None, :] <= rows[:, None]) & (columns[None, :] < length)
    scores = jnp.einsum("qagh,kah->agqk", qblock, keys, preferred_element_type=jnp.float32) * factor
    return (jnp.where(allowed[None, None, :, :], scores, NEGATIVE), factor)


def attend_block(qblock, start, keys, values, length):
    scores, factor = block_scores(qblock, start, keys, length)
    peak = jnp.max(scores, axis=-1, keepdims=True)
    expo = jnp.exp(scores - peak)
    total = jnp.sum(expo, axis=-1, keepdims=True)
    probs_low = (expo / total).astype(jnp.bfloat16)
    output = jnp.einsum("agqk,kah->qagh", probs_low, values, preferred_element_type=jnp.float32)
    return (output, (peak + jnp.log(total))[..., 0])


def attend_back(qblock, dblock, lse_block, start, keys, values, length):
    scores, factor = block_scores(qblock, start, keys, length)
    probs = jnp.exp(scores - lse_block[..., None])
    probs_grad = jnp.einsum("qagh,kah->agqk", dblock, values, preferred_element_type=jnp.float32)
    delta = jnp.sum(probs * probs_grad, axis=-1, keepdims=True)
    score_grad = (probs * (probs_grad - delta)).astype(jnp.bfloat16)
    query_grad = (
        jnp.einsum("agqk,kah->qagh", score_grad, keys, preferred_element_type=jnp.float32) * factor
    )
    key_grad = (
        jnp.einsum("agqk,qagh->kah", score_grad, qblock, preferred_element_type=jnp.float32)
        * factor
    )
    value_grad = jnp.einsum(
        "agqk,qagh->kah", probs.astype(jnp.bfloat16), dblock, preferred_element_type=jnp.float32
    )
    return (query_grad, key_grad, value_grad)


def routed_shards(
    tokens,
    seq_length,
    expert_routes,
    attention_gain,
    query_weight,
    key_weight,
    value_weight,
    query_gain,
    key_gain,
    output_weight,
    routing_gain,
    router_weight,
    gate_weight,
    up_weight,
    down_weight,
    cotangent,
):
    count = tokens.shape[0]
    width = tokens.shape[1]
    head_size = query_gain.shape[0]
    local_heads = query_weight.shape[1] // head_size
    local_groups = key_weight.shape[1] // head_size
    ratio = local_heads // local_groups
    length = seq_length[0]
    experts = router_weight.shape[1]
    top = expert_routes.shape[1]
    owned = gate_weight.shape[0]
    sources = experts // owned
    parts = lax.axis_size("tensor")
    part = lax.axis_index("tensor")
    quarter = (count * top * 5 + 16 * experts - 1) // (16 * experts)
    inputs = tokens.astype(jnp.float32)
    scale1 = rms_scale(inputs)
    normed1 = inputs * scale1
    xnorm1 = (normed1 * attention_gain).astype(jnp.bfloat16)
    query_raw = jnp.dot(xnorm1, query_weight, preferred_element_type=jnp.float32).reshape(
        count, local_heads, head_size
    )
    key_raw = jnp.dot(xnorm1, key_weight, preferred_element_type=jnp.float32).reshape(
        count, local_groups, head_size
    )
    value_low = (
        jnp.dot(xnorm1, value_weight, preferred_element_type=jnp.float32)
        .astype(jnp.bfloat16)
        .reshape(count, local_groups, head_size)
    )
    query_gained, query_normed, query_scale = head_norm(query_raw, query_gain)
    key_gained, key_normed, key_scale = head_norm(key_raw, key_gain)
    cosine, sine = rope_tables(count, head_size)
    query_low = rotate(query_gained, cosine, sine).astype(jnp.bfloat16)
    key_low = rotate(key_gained, cosine, sine).astype(jnp.bfloat16)
    block = min(512, count)
    blocks = count // block
    starts = jnp.arange(blocks, dtype=jnp.int32) * block
    query_blocks = query_low.reshape(blocks, block, local_groups, ratio, head_size)

    def forward_block(item):
        qblock, start = item
        return attend_block(qblock, start, key_low, value_low, length)

    outputs, lse = lax.map(forward_block, (query_blocks, starts))
    valid = (jnp.arange(count, dtype=jnp.int32) < length)[:, None]
    heads_low = jnp.where(valid, outputs.reshape(count, local_heads * head_size), 0.0).astype(
        jnp.bfloat16
    )
    attention_part = contract(heads_low, output_weight, 1, 1)
    attention_full = lax.psum(attention_part, "tensor")
    hidden = inputs + attention_full
    scale2 = rms_scale(hidden)
    normed2 = hidden * scale2
    xnorm2 = (normed2 * routing_gain).astype(jnp.bfloat16)
    logits = jnp.dot(xnorm2, router_weight, preferred_element_type=jnp.float32)
    peak = jnp.max(logits, axis=1, keepdims=True)
    expo = jnp.exp(logits - peak)
    router = expo / jnp.sum(expo, axis=1, keepdims=True)
    onehot = expert_routes[:, :, None] == jnp.arange(experts, dtype=jnp.int32)[None, None, :]
    chosen = jnp.sum(jnp.where(onehot, router[:, None, :], 0.0), axis=-1)
    chosen_total = jnp.sum(chosen, axis=1, keepdims=True)
    route_weight = chosen / chosen_total
    flat_routes = expert_routes.reshape(-1)
    hits = (flat_routes[:, None] == jnp.arange(experts, dtype=jnp.int32)[None, :]).astype(jnp.int32)
    ranks = jnp.sum((jnp.cumsum(hits, axis=0) - 1) * hits, axis=1)
    mine = ranks % parts == part
    slot_index = jnp.where(mine, ranks // parts * experts + flat_routes, quarter * experts)
    table = (
        jnp.full((quarter * experts,), count * top, jnp.int32)
        .at[slot_index]
        .set(jnp.arange(count * top, dtype=jnp.int32), mode="drop")
    )
    slot_token = table // top
    send_rows = jnp.take(xnorm2, slot_token, axis=0, mode="fill", fill_value=0).reshape(
        quarter, experts, width
    )
    arrived = lax.all_to_all(send_rows, "expert", split_axis=1, concat_axis=1, tiled=True)
    gate_full, up_full, down_full = (
        lax.all_gather(gate_weight, "tensor", axis=2, tiled=True),
        lax.all_gather(up_weight, "tensor", axis=2, tiled=True),
        lax.all_gather(down_weight, "tensor", axis=1, tiled=True),
    )
    rows_own = arrived.reshape(quarter, sources, owned, width)
    gate_val = jnp.einsum("csjd,jdf->csjf", rows_own, gate_full, preferred_element_type=jnp.float32)
    up_val = jnp.einsum("csjd,jdf->csjf", rows_own, up_full, preferred_element_type=jnp.float32)
    sigmoid_gate = jax.nn.sigmoid(gate_val)
    activated = gate_val * sigmoid_gate
    inner_low = (activated * up_val).astype(jnp.bfloat16)
    expert_total = jnp.einsum(
        "csjf,jfd->csjd", inner_low, down_full, preferred_element_type=jnp.float32
    )
    expert_low = expert_total.astype(jnp.bfloat16).reshape(quarter, experts, width)
    returned = lax.all_to_all(
        expert_low, "expert", split_axis=1, concat_axis=1, tiled=True
    ).reshape(quarter * experts, width)
    picked = jnp.take(returned, slot_index, axis=0, mode="fill", fill_value=0).reshape(
        count, top, width
    )
    mine_rows = mine.reshape(count, top)
    mine_weight = jnp.where(mine_rows, route_weight, 0.0)
    moe_part = jnp.sum(mine_weight[:, :, None] * picked, axis=1)
    moe_full = lax.psum(moe_part.astype(jnp.bfloat16), "tensor").astype(jnp.float32)
    mixed = (hidden + moe_full).astype(jnp.bfloat16)
    upstream = cotangent.astype(jnp.float32)
    route_grad_part = jnp.where(mine_rows, jnp.sum(picked * upstream[:, None, :], axis=-1), 0.0)
    slot_weight = jnp.take(route_weight.reshape(-1), table, mode="fill", fill_value=0.0)
    grad_send = (
        jnp.take(cotangent, slot_token, axis=0, mode="fill", fill_value=0) * slot_weight[:, None]
    ).astype(jnp.bfloat16)
    grad_arrived = lax.all_to_all(
        grad_send.reshape(quarter, experts, width),
        "expert",
        split_axis=1,
        concat_axis=1,
        tiled=True,
    )
    grad_own = grad_arrived.reshape(quarter, sources, owned, width)
    down_part = jnp.einsum(
        "csjf,csjd->jfd", inner_low, grad_own, preferred_element_type=jnp.float32
    )
    inner_grad = jnp.einsum(
        "csjd,jfd->csjf", grad_own, down_full, preferred_element_type=jnp.float32
    )
    gate_grad_low = (
        inner_grad * up_val * sigmoid_gate * (1.0 + gate_val * (1.0 - sigmoid_gate))
    ).astype(jnp.bfloat16)
    up_grad_low = (inner_grad * activated).astype(jnp.bfloat16)
    gate_part = jnp.einsum(
        "csjd,csjf->jdf", rows_own, gate_grad_low, preferred_element_type=jnp.float32
    )
    up_part = jnp.einsum(
        "csjd,csjf->jdf", rows_own, up_grad_low, preferred_element_type=jnp.float32
    )
    rows_grad = jnp.einsum(
        "csjf,jdf->csjd", gate_grad_low, gate_full, preferred_element_type=jnp.float32
    )
    rows_grad = rows_grad + jnp.einsum(
        "csjf,jdf->csjd", up_grad_low, up_full, preferred_element_type=jnp.float32
    )
    gate_grad, up_grad, down_grad = (
        lax.psum_scatter(
            gate_part.astype(jnp.bfloat16), "tensor", scatter_dimension=2, tiled=True
        ).astype(jnp.float32),
        lax.psum_scatter(
            up_part.astype(jnp.bfloat16), "tensor", scatter_dimension=2, tiled=True
        ).astype(jnp.float32),
        lax.psum_scatter(
            down_part.astype(jnp.bfloat16), "tensor", scatter_dimension=1, tiled=True
        ).astype(jnp.float32),
    )
    rows_grad_low = rows_grad.astype(jnp.bfloat16).reshape(quarter, experts, width)
    returned_grad = lax.all_to_all(
        rows_grad_low, "expert", split_axis=1, concat_axis=1, tiled=True
    ).reshape(quarter * experts, width)
    route_rows = jnp.take(returned_grad, slot_index, axis=0, mode="fill", fill_value=0).reshape(
        count, top, width
    )
    xnorm2_part = jnp.sum(route_rows, axis=1, dtype=jnp.float32)
    xnorm2_moe, route_grad = (
        lax.psum(xnorm2_part.astype(jnp.bfloat16), "tensor").astype(jnp.float32),
        lax.psum(route_grad_part.astype(jnp.bfloat16), "tensor").astype(jnp.float32),
    )
    inner_total = jnp.sum(route_grad * route_weight, axis=1, keepdims=True)
    chosen_grad = (route_grad - inner_total) / chosen_total
    prob_grad = jnp.sum(jnp.where(onehot, chosen_grad[:, :, None], 0.0), axis=1)
    logit_low = (router * (prob_grad - jnp.sum(router * prob_grad, axis=1, keepdims=True))).astype(
        jnp.bfloat16
    )
    router_grad = contract(xnorm2, logit_low, 0, 0)
    xnorm2_grad = xnorm2_moe + contract(logit_low, router_weight, 1, 1)
    routing_gain_part = jnp.sum(xnorm2_grad * normed2, axis=0)
    inner2 = xnorm2_grad * routing_gain
    hidden_grad = upstream + scale2 * (
        inner2 - normed2 * jnp.mean(inner2 * normed2, axis=1, keepdims=True)
    )
    hidden_low = hidden_grad.astype(jnp.bfloat16)
    output_grad = contract(hidden_low, heads_low, 0, 0)
    heads_grad = jnp.where(
        valid,
        jnp.dot(hidden_low, output_weight, preferred_element_type=jnp.float32).astype(jnp.bfloat16),
        jnp.zeros((), jnp.bfloat16),
    )
    grad_blocks = heads_grad.reshape(blocks, block, local_groups, ratio, head_size)

    def backward_block(carry, item):
        key_acc, value_acc = carry
        qblock, dblock, lse_block, start = item
        query_piece, key_piece, value_piece = attend_back(
            qblock, dblock, lse_block, start, key_low, value_low, length
        )
        return ((key_acc + key_piece, value_acc + value_piece), query_piece)

    empty = jnp.zeros((count, local_groups, head_size), jnp.float32)
    (key_rot_grad, value_grad), query_rot_grad = lax.scan(
        backward_block, (empty, empty), (query_blocks, grad_blocks, lse, starts)
    )
    query_back, query_gain_part = head_norm_back(
        rotate_back(query_rot_grad.reshape(count, local_heads, head_size), cosine, sine),
        query_normed,
        query_scale,
        query_gain,
    )
    key_back, key_gain_part = head_norm_back(
        rotate_back(key_rot_grad, cosine, sine), key_normed, key_scale, key_gain
    )
    query_grad_low = query_back.reshape(count, local_heads * head_size).astype(jnp.bfloat16)
    key_grad_low = key_back.reshape(count, local_groups * head_size).astype(jnp.bfloat16)
    value_grad_low = value_grad.reshape(count, local_groups * head_size).astype(jnp.bfloat16)
    query_wgrad = contract(xnorm1, query_grad_low, 0, 0)
    key_wgrad = contract(xnorm1, key_grad_low, 0, 0)
    value_wgrad = contract(xnorm1, value_grad_low, 0, 0)
    xnorm1_part = contract(query_grad_low, query_weight, 1, 1) + contract(
        key_grad_low, key_weight, 1, 1
    )
    xnorm1_part = xnorm1_part + contract(value_grad_low, value_weight, 1, 1)
    xnorm1_grad, query_gain_sum, key_gain_sum = (
        lax.psum(xnorm1_part.astype(jnp.bfloat16), "tensor").astype(jnp.float32),
        lax.psum(query_gain_part.astype(jnp.bfloat16), "tensor").astype(jnp.float32),
        lax.psum(key_gain_part.astype(jnp.bfloat16), "tensor").astype(jnp.float32),
    )
    attention_gain_part = jnp.sum(xnorm1_grad * normed1, axis=0)
    inner1 = xnorm1_grad * attention_gain
    tokens_grad = (
        hidden_grad
        + scale1 * (inner1 - normed1 * jnp.mean(inner1 * normed1, axis=1, keepdims=True))
    ).astype(jnp.bfloat16)
    summed = (
        lax.psum_scatter(
            attention_gain_part.astype(jnp.bfloat16), "expert", scatter_dimension=0, tiled=True
        ).astype(jnp.float32),
        lax.psum_scatter(
            query_wgrad.astype(jnp.bfloat16), "expert", scatter_dimension=0, tiled=True
        ).astype(jnp.float32),
        lax.psum_scatter(
            key_wgrad.astype(jnp.bfloat16), "expert", scatter_dimension=0, tiled=True
        ).astype(jnp.float32),
        lax.psum_scatter(
            value_wgrad.astype(jnp.bfloat16), "expert", scatter_dimension=0, tiled=True
        ).astype(jnp.float32),
        lax.psum_scatter(
            query_gain_sum.astype(jnp.bfloat16), "expert", scatter_dimension=0, tiled=True
        ).astype(jnp.float32),
        lax.psum_scatter(
            key_gain_sum.astype(jnp.bfloat16), "expert", scatter_dimension=0, tiled=True
        ).astype(jnp.float32),
        lax.psum_scatter(
            output_grad.astype(jnp.bfloat16), "expert", scatter_dimension=0, tiled=True
        ).astype(jnp.float32),
        lax.psum_scatter(
            routing_gain_part.astype(jnp.bfloat16), "expert", scatter_dimension=0, tiled=True
        ).astype(jnp.float32),
        lax.psum_scatter(
            router_grad.astype(jnp.bfloat16), "expert", scatter_dimension=0, tiled=True
        ).astype(jnp.float32),
    )
    return (
        mixed,
        tokens_grad,
        summed[0],
        summed[1],
        summed[2],
        summed[3],
        summed[4],
        summed[5],
        summed[6],
        summed[7],
        summed[8],
        gate_grad,
        up_grad,
        down_grad,
    )


MESH_ID = pl.DeviceIdType.MESH
DEPTH = 4
F32 = jnp.float32
LOW = jnp.bfloat16


class Place:
    def __init__(self):
        e, t = lax.axis_index("expert"), lax.axis_index("tensor")
        self.e, self.t = e, t
        self.z, self.y, self.x, self.c = e // 2, e % 2, t // 2, t % 2

    def at(self, z=None, y=None, x=None, c=None):
        z, y = self.z if z is None else z, self.y if y is None else y
        x, c = self.x if x is None else x, self.c if c is None else c
        return (z * 2 + y, x * 2 + c)

    def block(self, **where):
        e, t = self.at(**where)
        return e * 4 + t

    def near(self, k):
        table = ((0, 1, 2, 3), (1, 2, 0, 3), (2, 1, 3, 0), (3, 2, 1, 0))
        out = 0
        for z in range(DEPTH):
            if isinstance(k, int):
                column = table[z][k]
            else:
                column = table[z][0]
                for i in range(1, DEPTH):
                    column = jnp.where(k == i, table[z][i], column)
            out = jnp.where(self.z == z, column, out)
        return out

    def peers(self):
        line = [self.at(z=(self.z + d) % DEPTH) for d in range(1, DEPTH)]
        return line + [self.at(x=1 - self.x), self.at(y=1 - self.y), self.at(c=1 - self.c)]


class Copies:
    def __init__(self, send_sems, recv_sems):
        self.send_sems, self.recv_sems, self.used, self.made = send_sems, recv_sems, 0, []

    def make(self, src, dst, to):
        i = self.used
        self.used += 1
        copy = pltpu.make_async_remote_copy(
            src,
            dst,
            self.send_sems.at[i],
            self.recv_sems.at[i],
            device_id=to,
            device_id_type=MESH_ID,
        )
        self.made.append(copy)
        return copy

    def along(self, pieces, to, mine):
        base = self.used
        self.used += DEPTH
        out = []
        for (peer, src, dst), device in zip(pieces, to):
            there = pltpu.make_async_remote_copy(
                src,
                dst,
                self.send_sems.at[base + peer],
                self.recv_sems.at[base + mine],
                device_id=device,
                device_id_type=MESH_ID,
            )
            back = pltpu.make_async_remote_copy(
                src,
                dst,
                self.send_sems.at[base + peer],
                self.recv_sems.at[base + peer],
                device_id=device,
                device_id_type=MESH_ID,
            )
            self.made.append(there)
            out.append((there, back))
        return out

    def between(self, src, dst, to, send, recv):
        return pltpu.make_async_remote_copy(
            src,
            dst,
            self.send_sems.at[send],
            self.recv_sems.at[recv],
            device_id=to,
            device_id_type=MESH_ID,
        )

    def finish(self):
        for copy in self.made:
            copy.wait_send()


class LineSend:
    SEMS = DEPTH

    def __init__(self, p, copies, src, slot):
        others = [p.near(k) for k in range(1, DEPTH)]
        self.pairs = copies.along(
            [(z, src, slot(p.z)) for z in others], [p.at(z=z) for z in others], p.z
        )

    def start(self):
        for there, _ in self.pairs:
            there.start()

    def wait(self, k):
        self.pairs[k - 1][1].wait_recv()


class LineSum:
    SEMS = 4

    def __init__(self, p, copies, terms, arrived):
        base = copies.used
        copies.used += self.SEMS
        near = {k: p.at(z=p.near(k)) for k in range(1, DEPTH)}
        self.inner = (p.z == 1) | (p.z == 2)
        arrived = [arrived.at[i] for i in range(DEPTH)]
        self.terms, self.arrived = terms, arrived
        self.outer_to = {
            1: copies.between(terms[1], arrived[0], near[1], base, base),
            2: copies.between(terms[2], arrived[2], near[1], base + 1, base + 2),
            3: copies.between(terms[3], arrived[3], near[1], base + 2, base + 3),
        }
        self.inner_to = {
            2: copies.between(terms[2], arrived[0], near[2], base, base),
            1: copies.between(terms[1], arrived[1], near[1], base + 1, base + 1),
            3: copies.between(terms[3], arrived[1], near[3], base + 2, base + 1),
        }
        copies.made += self.outer_to.values()

    def send(self, k):
        pl.when(jnp.logical_not(self.inner))(self.outer_to[k].start)
        if k == 2:
            pl.when(self.inner)(self.inner_to[2].start)

    def relay(self):
        @pl.when(self.inner)
        def _():
            for k, behind in ((3, 3), (1, 2)):
                self.outer_to[behind].wait_recv()
                term = self.terms[k]
                term[...] = (term[...].astype(F32) + self.arrived[behind][...].astype(F32)).astype(
                    LOW
                )
                self.inner_to[k].start()

    def wait(self):
        self.inner_to[2].wait_recv()
        self.inner_to[1].wait_recv()
        return self.arrived[:2]


class StraightSum:
    SEMS = DEPTH

    def __init__(self, p, copies, terms, arrived):
        others = [p.near(k) for k in range(1, DEPTH)]
        slots = [arrived.at[p.near(k)] for k in range(1, DEPTH)]
        self.slots = slots
        self.pairs = copies.along(
            [(z, terms[k], arrived.at[p.z]) for k, z in enumerate(others, 1)],
            [p.at(z=z) for z in others],
            p.z,
        )

    def send(self, k):
        self.pairs[k - 1][0].start()

    def relay(self):
        pass

    def wait(self):
        for _, back in self.pairs:
            back.wait_recv()
        return self.slots


def enter(peers):
    barrier = pltpu.get_barrier_semaphore()
    for peer in peers:
        pl.semaphore_signal(barrier, inc=1, device_id=peer, device_id_type=MESH_ID)
    pl.semaphore_wait(barrier, len(peers))


def pieces_of(ref, rows):
    half = rows // 2

    def whole(b):
        return ref.at[pl.ds(pl.multiple_of(b * rows, rows), rows)]

    def first(b):
        return ref.at[pl.ds(pl.multiple_of(b * rows, rows), half)]

    def second(b):
        return ref.at[pl.ds(pl.multiple_of(b * rows + half, half), half)]

    return whole, first, second


GATHER_SEMS = LineSend.SEMS + 3 * DEPTH + 4 * DEPTH + 2 * DEPTH


def gather_steps(p, copies, rows, own_ref, all_ref, own_copy):
    whole, first, second = pieces_of(all_ref, rows)
    me = p.block()
    xn, yn, cn = p.at(x=1 - p.x), p.at(y=1 - p.y), p.at(c=1 - p.c)
    order = [p.near(k) for k in range(DEPTH)]
    line = LineSend(p, copies, own_ref, lambda z: whole(p.block(z=z)))
    to_x, to_y, near, far, diagonal = [], [], [], [], []
    for d in range(DEPTH):
        b = p.block(z=order[d])
        src = own_ref if d == 0 else whole(b)
        to_x.append(copies.make(src, whole(b), xn))
        to_y.append(copies.make(src, whole(b), yn))
        bx, by = p.block(z=order[d], x=1 - p.x), p.block(z=order[d], y=1 - p.y)
        bd = p.block(z=order[d], x=1 - p.x, y=1 - p.y)
        near.append([copies.make(src, whole(b), cn), copies.make(whole(bx), whole(bx), cn)])
        diagonal.append(
            (copies.make(first(bx), first(bx), yn), copies.make(second(by), second(by), xn))
        )
        far.append(
            [
                copies.make(whole(by), whole(by), cn),
                copies.make(first(bd), first(bd), cn),
                copies.make(second(bd), second(bd), cn),
            ]
        )

    def onward(d):
        if d:
            line.wait(d)
        to_x[d].start()
        to_y[d].start()
        near[d][0].start()

    def pair(d):
        to_x[d].wait_recv()
        diagonal[d][0].start()
        near[d][1].start()
        to_y[d].wait_recv()
        diagonal[d][1].start()
        far[d][0].start()

    def corner(d):
        for i in range(2):
            diagonal[d][i].wait_recv()
            far[d][1 + i].start()

    def arrived(group):
        for copy in group:
            copy.wait_recv()

    def begin():
        own_copy.start()
        line.start()
        onward(0)

    def step0():
        onward(1)
        pair(0)
        own_copy.wait()
        arrived(near[0])

    def step1():
        onward(2)
        pair(1)
        corner(0)
        arrived(far[0])

    def step3():
        onward(3)
        pair(2)
        corner(1)
        arrived(far[1])

    def step5():
        pair(3)
        corner(2)
        arrived(far[2])

    def step6():
        corner(3)
        arrived(near[3])

    return [
        begin,
        step0,
        step1,
        lambda: arrived(near[1]),
        step3,
        lambda: arrived(near[2]),
        step5,
        step6,
        lambda: arrived(far[3]),
    ]


SCATTER_SEMS = 16 + 8 + 8 + LineSum.SEMS


def scatter_scratch(rows, width):
    return [
        pltpu.VMEM((16, rows, width), LOW),
        pltpu.VMEM((2, DEPTH, rows // 2, width), LOW),
        pltpu.VMEM((2, DEPTH, rows, width), LOW),
        pltpu.VMEM((DEPTH, rows, width), LOW),
    ]


class Scatter:
    def __init__(self, p, copies, rows, part, core_in, diag_in, side_in, line_in, order, kind):
        whole, first, second = pieces_of(part, rows)
        positions = [p.near(k) for k in order]
        xn, yn, cn = p.at(x=1 - p.x), p.at(y=1 - p.y), p.at(c=1 - p.c)
        kinds = [dict(y=1 - p.y, x=1 - p.x), dict(x=1 - p.x), dict(y=1 - p.y), dict()]
        self.core_in, self.diag_in, self.side_in = core_in, diag_in, side_in
        self.order = order
        blocks = [[p.block(z=z, **kind) for kind in kinds] for z in positions]
        self.wholes = [[whole(b) for b in row] for row in blocks]
        self.first = [first(row[1]) for row in blocks]
        self.second = [second(row[2]) for row in blocks]
        self.core = [
            [
                copies.make(whole(p.block(z=z, c=1 - p.c, **kind)), core_in.at[k * 4 + j], cn)
                for j, kind in enumerate(kinds)
            ]
            for k, z in enumerate(positions)
        ]
        self.corners = [
            (
                copies.make(first(row[0]), diag_in.at[0, k], yn),
                copies.make(second(row[0]), diag_in.at[1, k], xn),
            )
            for k, row in enumerate(blocks)
        ]
        self.sides = [
            (
                copies.make(whole(row[1]), side_in.at[0, k], xn),
                copies.make(whole(row[2]), side_in.at[1, k], yn),
            )
            for k, row in enumerate(blocks)
        ]
        self.line = kind(
            p, copies, {order[k]: self.wholes[k][3] for k in range(DEPTH)}, line_in
        )

    def add(self, ref, *more):
        total = ref[...].astype(F32)
        for other in more:
            total = total + other[...].astype(F32)
        ref[...] = total.astype(LOW)

    def start(self, k):
        for copy in self.core[k]:
            copy.start()

    def corner(self, k):
        self.core[k][0].wait_recv()
        self.add(self.wholes[k][0], self.core_in.at[k * 4])
        for copy in self.corners[k]:
            copy.start()
        for j in (1, 2):
            self.core[k][j].wait_recv()
            self.add(self.wholes[k][j], self.core_in.at[k * 4 + j])

    def side(self, k):
        self.corners[k][0].wait_recv()
        self.add(self.first[k], self.diag_in.at[0, k])
        self.sides[k][0].start()
        self.corners[k][1].wait_recv()
        self.add(self.second[k], self.diag_in.at[1, k])
        self.sides[k][1].start()
        self.core[k][3].wait_recv()

    def close(self, k):
        for copy in self.sides[k]:
            copy.wait_recv()
        self.add(
            self.wholes[k][3],
            self.core_in.at[k * 4 + 3],
            self.side_in.at[0, k],
            self.side_in.at[1, k],
        )
        if self.order[k]:
            self.line.send(self.order[k])

    def relay(self, _):
        self.line.relay()

    def finish(self):
        total = self.wholes[self.order.index(0)][3][...].astype(F32)
        for term in self.line.wait():
            total = total + term[...].astype(F32)
        return total


def dot(left, right, left_dim, right_dim):
    return lax.dot_general(
        left, right, (((left_dim,), (right_dim,)), ((), ())), preferred_element_type=F32
    )


def semaphores(*counts):
    return [pltpu.SemaphoreType.DMA((n,)) for n in counts]


VMEM_SPEC = pl.BlockSpec(memory_space=pltpu.VMEM)
ANY_SPEC = pl.BlockSpec(memory_space=pl.ANY)


def experts_kernel(
    rows,
    width,
    experts,
    owned,
    own_ref,
    upstream_ref,
    gate_from,
    up_from,
    down_from,
    heads_ref,
    grad_ref,
    moe_ref,
    line_heads_ref,
    gate_grad_to,
    up_grad_to,
    down_grad_to,
    gate_ref,
    up_ref,
    down_ref,
    gate_grad_ref,
    up_grad_ref,
    down_grad_ref,
    all_ref,
    upstream,
    outgoing,
    part,
    back_rows,
    core_in,
    diag_in,
    side_in,
    line_in,
    local_sems,
    gather_send,
    gather_recv,
    scatter_send,
    scatter_recv,
    heads_send,
    heads_recv,
    store_sems,
):
    p = Place()
    group = rows * 4
    units = down_ref.shape[0]
    hidden = units // owned
    extra = all_ref.shape[1] - width
    loads = [
        pltpu.make_async_copy(src, dst, local_sems.at[5 + i])
        for i, (src, dst) in enumerate(
            ((gate_from, gate_ref), (up_from, up_ref), (down_from, down_ref))
        )
    ]
    for copy in loads:
        copy.start()
    enter(p.peers())
    whole, _, _ = pieces_of(all_ref, rows)
    own_copy = pltpu.make_async_copy(own_ref, whole(p.block()), local_sems.at[0])
    gather_copies = Copies(gather_send, gather_recv)
    scatter_copies = Copies(scatter_send, scatter_recv)
    gathering = gather_steps(p, gather_copies, rows, own_ref, all_ref, own_copy)
    sums = Scatter(
        p,
        scatter_copies,
        rows,
        part,
        core_in,
        diag_in,
        side_in,
        line_in,
        list(range(DEPTH)),
        StraightSum,
    )

    def finish():
        grad_ref[...] = sums.finish()

    beside_work = {
        2: [(sums.start, 0)],
        3: [(sums.corner, 0)],
        4: [(sums.start, 1)],
        5: [(sums.corner, 1), (sums.side, 0)],
        6: [(sums.start, 2)],
        7: [(sums.corner, 2), (sums.side, 1), (sums.close, 0)],
    }
    beside_tiles = {
        0: [(sums.start, 3), (sums.side, 2), (sums.close, 1), (sums.corner, 3)],
        2: [(sums.side, 3)],
        3: [(sums.close, 2)],
        5: [(sums.close, 3)],
    }

    def run(actions):
        for stage, k in actions:
            stage(k)

    count = 2 * DEPTH

    def rows_of(i):
        side = jnp.where(i % 2 == 0, p.y, 1 - p.y)
        return pl.ds(pl.multiple_of((p.near(i // 2) * 2 + side) * group, group), group)

    def fetch(i):
        return pltpu.make_async_copy(
            upstream_ref.at[rows_of(i)], upstream.at[i % 2], local_sems.at[1 + i % 2]
        )

    def store(i):
        return pltpu.make_async_copy(
            outgoing.at[i % 2], moe_ref.at[rows_of(i)], local_sems.at[3 + i % 2]
        )

    fetch(0).start()
    gathering[0]()
    heads_copies = Copies(heads_send, heads_recv)
    half = heads_ref.shape[1] // 2
    heads_line = LineSend(
        p, heads_copies, heads_ref.at[:, half:], lambda z: line_heads_ref.at[z]
    )
    heads_line.start()
    down_grad_ref[...] = jnp.zeros_like(down_grad_ref)
    first = p.e * owned
    lane = lax.broadcasted_iota(jnp.int32, (group, extra), 1)
    unit = lax.broadcasted_iota(jnp.int32, (group, units), 1)
    for copy in loads:
        copy.wait()

    @pl.loop(0, count)
    def _(i):
        for k, actions in beside_work.items():
            pl.when(i == k)(functools.partial(run, actions))
        for k, step in enumerate(gathering[1:]):
            pl.when(i == k)(step)
        at = rows_of(i)
        x = all_ref[at, :width]
        gate = dot(x, gate_ref[...], 1, 1)
        up = dot(x, up_ref[...], 1, 1)
        tail = all_ref[at, width:].astype(F32)
        weights = [
            jnp.sum(
                jnp.where((lane == first + j) | (lane == experts + first + j), tail, 0.0),
                axis=1,
                keepdims=True,
            )
            for j in range(owned)
        ]
        weight = weights[0]
        for j in range(1, owned):
            weight = jnp.where(unit >= j * hidden, weights[j], weight)
        sigmoid = 1.0 / (1.0 + jnp.exp(-gate))
        activated = gate * sigmoid
        inner = activated * up
        weighted = (inner * weight).astype(LOW)

        @pl.when(i >= 2)
        def _():
            store(i - 2).wait()

        outgoing[i % 2] = dot(weighted, down_ref[...], 1, 0).astype(LOW)
        store(i).start()
        fetch(i).wait()

        @pl.when(i + 1 < count)
        def _():
            fetch(i + 1).start()

        u = upstream[i % 2]
        down_back = dot(u, down_ref[...], 1, 1)
        down_grad_ref[...] += dot(weighted, u, 0, 0)
        product = inner * down_back
        note = jnp.zeros((group, extra), F32)
        for j in range(owned):
            mine = (unit >= j * hidden) & (unit < (j + 1) * hidden)
            route_grad = jnp.sum(jnp.where(mine, product, 0.0), axis=1, keepdims=True)
            note = jnp.where(lane == first + j, route_grad, note)
        inner_grad = down_back * weight
        gate_back = (inner_grad * up * sigmoid * (1.0 + gate * (1.0 - sigmoid))).astype(LOW)
        up_back = (inner_grad * activated).astype(LOW)
        back_rows[at, :units] = gate_back
        back_rows[at, units:] = up_back
        part[at, :width] = (
            dot(gate_back, gate_ref[...], 1, 0) + dot(up_back, up_ref[...], 1, 0)
        ).astype(LOW)
        part[at, width:] = note.astype(LOW)

    tile = width // count

    def store_tile(i):
        at = pl.ds(pl.multiple_of(i * tile, tile), tile)
        return [
            pltpu.make_async_copy(ref.at[:, at], to.at[:, at], store_sems.at[i, j])
            for j, (ref, to) in enumerate(
                ((gate_grad_ref, gate_grad_to), (up_grad_ref, up_grad_to))
            )
        ]

    store_down = pltpu.make_async_copy(down_grad_ref, down_grad_to, local_sems.at[5])
    store_down.start()

    @pl.loop(0, count)
    def _(i):
        for k, actions in beside_tiles.items():
            pl.when(i == k)(functools.partial(run, actions))
        at = pl.ds(pl.multiple_of(i * tile, tile), tile)
        x = all_ref[:, at]
        gate_grad_ref[:, at] = dot(back_rows[:, :units], x, 0, 0)
        up_grad_ref[:, at] = dot(back_rows[:, units:], x, 0, 0)
        for copy in store_tile(i):
            copy.start()

    finish()
    gather_copies.finish()
    scatter_copies.finish()
    for k in range(1, DEPTH):
        heads_line.wait(k)
    heads_copies.finish()
    store(count - 2).wait()
    store(count - 1).wait()
    store_down.wait()
    for i in range(count):
        for copy in store_tile(i):
            copy.wait()


def run_experts(own, upstream_all, gate, up, down, heads, owned, experts, width, collective_id):
    rows, full = own.shape
    total = upstream_all.shape[0]
    units = down.shape[0]
    group = rows * lax.axis_size("tensor")
    return pl.pallas_call(
        functools.partial(experts_kernel, rows, width, experts, owned),
        out_shape=(
            jax.ShapeDtypeStruct((rows, full), F32),
            jax.ShapeDtypeStruct((total, width), LOW),
            jax.ShapeDtypeStruct((DEPTH, group, heads.shape[1] // 2), LOW),
            *[jax.ShapeDtypeStruct((units, width), F32)] * 3,
        ),
        in_specs=[VMEM_SPEC] + [ANY_SPEC] * 5,
        out_specs=[VMEM_SPEC] + [ANY_SPEC] * 5,
        scratch_shapes=[pltpu.VMEM((units, width), LOW)] * 3
        + [pltpu.VMEM((units, width), F32)] * 3
        + [
            pltpu.VMEM((total, full), LOW),
            pltpu.VMEM((2, group, width), LOW),
            pltpu.VMEM((2, group, width), LOW),
            pltpu.VMEM((total, full), LOW),
            pltpu.VMEM((total, 2 * units), LOW),
        ]
        + scatter_scratch(rows, full)
        + semaphores(8, GATHER_SEMS, GATHER_SEMS, SCATTER_SEMS, SCATTER_SEMS, DEPTH, DEPTH)
        + [pltpu.SemaphoreType.DMA((2 * DEPTH, 2))],
        compiler_params=pltpu.CompilerParams(
            collective_id=collective_id, has_side_effects=True, vmem_limit_bytes=64000000
        ),
        name="experts",
    )(own, upstream_all, gate, up, down, heads)


def normed_rows(values):
    scale = lax.rsqrt(jnp.mean(values * values, axis=-1, keepdims=True) + EPSILON)
    return values * scale, scale


def turned(values):
    return pltpu.roll(values, values.shape[-1] // 2, values.ndim - 1)


def allowed_keys(count, length):
    row = lax.broadcasted_iota(jnp.int32, (count, count), 0)
    column = lax.broadcasted_iota(jnp.int32, (count, count), 1)
    return (column <= row) & (column < length)


def attention_probs(query, key, allowed):
    factor = query.shape[-1] ** (-0.5)
    scores = jnp.where(allowed, dot(query, key, 1, 1) * factor, NEGATIVE)
    expo = jnp.exp(scores - jnp.max(scores, axis=-1, keepdims=True))
    return expo / jnp.sum(expo, axis=-1, keepdims=True)


class Spread:
    def __init__(self, p, copies, slot):
        other = (1 - p.x) * 2 + p.c
        self.to_x = copies.make(slot(p.t), slot(p.t), p.at(x=1 - p.x))
        self.to_c = copies.make(slot(p.t), slot(p.t), p.at(c=1 - p.c))
        self.onward = copies.make(slot(other), slot(other), p.at(c=1 - p.c))

    def start(self):
        self.to_x.start()
        self.to_c.start()

    def forward(self):
        self.to_x.wait_recv()
        self.onward.start()

    def finish(self):
        self.to_c.wait_recv()
        self.onward.wait_recv()


class Fold:
    def __init__(self, p, copies, rows, part, arrived):
        def block(t):
            return part.at[pl.ds(pl.multiple_of(t * rows, rows), rows)]

        cn, xn = p.at(c=1 - p.c), p.at(x=1 - p.x)
        self.arrived, self.own, self.other = arrived, block(p.t), block((1 - p.x) * 2 + p.c)
        self.to_c = [
            copies.make(block((1 - p.x) * 2 + 1 - p.c), arrived.at[0], cn),
            copies.make(block(p.x * 2 + 1 - p.c), arrived.at[1], cn),
        ]
        self.to_x = copies.make(self.other, arrived.at[2], xn)

    def start(self):
        for copy in self.to_c:
            copy.start()

    def forward(self):
        self.to_c[0].wait_recv()
        self.other[...] = (self.other[...].astype(F32) + self.arrived[0].astype(F32)).astype(LOW)
        self.to_x.start()

    def finish(self):
        self.to_c[1].wait_recv()
        self.to_x.wait_recv()
        return (
            self.own[...].astype(F32) + self.arrived[1].astype(F32) + self.arrived[2].astype(F32)
        )


FOLD_SEMS = 3
FRONT_SEMS = FOLD_SEMS + LineSend.SEMS
LANES = 128


def widen(wide_ref, router_weight_ref):
    experts, width = router_weight_ref.shape
    wide_ref[:experts, :] = router_weight_ref[...]
    wide_ref[experts:, :] = jnp.zeros((LANES - experts, width), LOW)


def front_kernel(
    rows,
    experts,
    length_ref,
    tokens_ref,
    cotangent_ref,
    routes_ref,
    attention_gain_ref,
    query_gain_ref,
    key_gain_ref,
    routing_gain_ref,
    cosine_ref,
    sine_ref,
    query_weight_ref,
    key_weight_ref,
    value_weight_ref,
    output_weight_from,
    router_weight_from,
    upstream_ref,
    xnorm1_ref,
    query_ref,
    key_ref,
    value_ref,
    heads_ref,
    line_heads_ref,
    hidden_ref,
    own_ref,
    router_ref,
    output_weight_ref,
    router_weight_ref,
    part,
    part_in,
    local_sems,
    gather_send,
    gather_recv,
    send_sems,
    recv_sems,
):
    p = Place()
    group, width = tokens_ref.shape
    units = query_ref.shape[1]
    size = cosine_ref.shape[1]
    count = units // size
    length = length_ref[0]
    load = pltpu.make_async_copy(output_weight_from, output_weight_ref, local_sems.at[1])
    load.start()
    enter(p.peers())
    copies = Copies(send_sems, recv_sems)
    gather_copies = Copies(gather_send, gather_recv)
    mine = pl.ds(pl.multiple_of(p.t * rows, rows), rows)
    whole, _, _ = pieces_of(upstream_ref, rows)
    own_cotangent = cotangent_ref.at[mine]
    own_copy = pltpu.make_async_copy(own_cotangent, whole(p.block()), local_sems.at[0])
    gathering = gather_steps(p, gather_copies, rows, own_cotangent, upstream_ref, own_copy)
    fold = Fold(p, copies, rows, part, part_in)
    line = LineSend(
        p, copies, heads_ref.at[:, : units // 2], lambda z: line_heads_ref.at[z]
    )
    gathering[0]()

    normed1, _ = normed_rows(tokens_ref[...].astype(F32))
    xnorm1_ref[...] = (normed1 * attention_gain_ref[...]).astype(LOW)
    query_ref[...] = dot(xnorm1_ref[...], query_weight_ref[...], 1, 0)
    key_ref[...] = dot(xnorm1_ref[...], key_weight_ref[...], 1, 0)
    value_ref[...] = dot(xnorm1_ref[...], value_weight_ref[...], 1, 0).astype(LOW)
    gathering[1]()
    cosine, sine = cosine_ref[...], sine_ref[...]
    query_gain = query_gain_ref[...]
    valid = lax.broadcasted_iota(jnp.int32, (group, 1), 0) < length
    allowed = allowed_keys(group, length)
    key_hat, _ = normed_rows(key_ref[...])
    key_gained = key_hat * key_gain_ref[...]
    key_low = (key_gained * cosine + turned(key_gained) * sine).astype(LOW)

    @pl.loop(0, count)
    def _(h):
        pl.when(h == count // 2)(line.start)
        for k in (2, 3):
            pl.when(h == 2 * k)(gathering[k])
        at = pl.ds(pl.multiple_of(h * size, size), size)
        hat, _ = normed_rows(query_ref[:, at])
        gained = hat * query_gain
        query_low = (gained * cosine + turned(gained) * sine).astype(LOW)
        probs = attention_probs(query_low, key_low, allowed).astype(LOW)
        heads_ref[:, at] = jnp.where(valid, dot(probs, value_ref[...], 1, 0), 0.0).astype(LOW)

    load.wait()
    part[...] = dot(heads_ref[...], output_weight_ref[...], 1, 1).astype(LOW)
    fold.start()
    gathering[4]()
    fold.forward()
    gathering[5]()
    hidden = tokens_ref[mine, :].astype(F32) + fold.finish()
    hidden_ref[...] = hidden
    normed2, _ = normed_rows(hidden)
    xnorm2 = (normed2 * routing_gain_ref[...]).astype(LOW)
    own_ref[:, :width] = xnorm2
    gathering[6]()
    widen(router_weight_ref, router_weight_from)
    logits = dot(xnorm2, router_weight_ref[...], 1, 1)
    lanes = logits.shape[1]
    lane = lax.broadcasted_iota(jnp.int32, logits.shape, 1)
    peak = jnp.max(jnp.where(lane < experts, logits, NEGATIVE), axis=1, keepdims=True)
    expo = jnp.where(lane < experts, jnp.exp(jnp.minimum(logits - peak, 0.0)), 0.0)
    router = expo / jnp.sum(expo, axis=1, keepdims=True)
    named = jnp.zeros(logits.shape, F32)
    for k in range(routes_ref.shape[1]):
        named = jnp.where(routes_ref[:, k : k + 1] == lane, 1.0, named)
    chosen = router * named
    route_weight = chosen / jnp.sum(chosen, axis=1, keepdims=True)
    high = route_weight.astype(LOW).astype(F32)
    own_ref[:, width:] = (high + pltpu.roll(route_weight - high, experts, 1)).astype(LOW)
    router_ref[:, :lanes] = router
    router_ref[:, lanes : 2 * lanes] = route_weight
    router_ref[:, 2 * lanes :] = named
    gathering[7]()
    gathering[8]()
    for k in range(1, DEPTH):
        line.wait(k)
    gather_copies.finish()
    copies.finish()


def run_front(
    length,
    tokens,
    cotangent,
    routes,
    attention_gain,
    query_gain,
    key_gain,
    routing_gain,
    cosine,
    sine,
    query_weight,
    key_weight,
    value_weight,
    output_weight,
    router_weight,
    experts,
    collective_id,
):
    group, width = tokens.shape
    rows = routes.shape[0]
    lanes = LANES
    total = group * lax.axis_size("expert")
    struct = jax.ShapeDtypeStruct
    return pl.pallas_call(
        functools.partial(front_kernel, rows, experts),
        out_shape=(
            struct((total, width), LOW),
            struct((group, width), LOW),
            struct((group, query_weight.shape[1]), F32),
            struct((group, key_weight.shape[1]), F32),
            struct((group, value_weight.shape[1]), LOW),
            struct((group, query_weight.shape[1]), LOW),
            struct((DEPTH, group, query_weight.shape[1] // 2), LOW),
            struct((rows, width), F32),
            struct((rows, width + lanes), LOW),
            struct((rows, 3 * lanes), F32),
        ),
        in_specs=[pl.BlockSpec(memory_space=pltpu.SMEM), VMEM_SPEC, ANY_SPEC]
        + [VMEM_SPEC] * 10
        + [ANY_SPEC, VMEM_SPEC],
        out_specs=[ANY_SPEC] + [VMEM_SPEC] * 5 + [ANY_SPEC] + [VMEM_SPEC] * 3,
        scratch_shapes=[
            pltpu.VMEM(output_weight.shape, LOW),
            pltpu.VMEM((lanes, width), LOW),
            pltpu.VMEM((group, width), LOW),
            pltpu.VMEM((3, rows, width), LOW),
        ]
        + semaphores(2, GATHER_SEMS, GATHER_SEMS, FRONT_SEMS, FRONT_SEMS),
        compiler_params=pltpu.CompilerParams(
            collective_id=collective_id, has_side_effects=True, vmem_limit_bytes=60000000
        ),
        name="front",
    )(
        length,
        tokens,
        cotangent,
        routes,
        attention_gain,
        query_gain,
        key_gain,
        routing_gain,
        cosine,
        sine,
        query_weight,
        key_weight,
        value_weight,
        output_weight,
        router_weight,
    )


SPREAD_SEMS = 3
PIECES = 4
TAIL_SEMS = 4 * SPREAD_SEMS + DEPTH * 3 + PIECES * (1 + LineSum.SEMS) + 1 + FOLD_SEMS + 3


def tail_kernel(
    rows,
    experts,
    length_ref,
    summed_ref,
    own_ref,
    router_ref,
    hidden_ref,
    cotangent_from,
    tokens_from,
    xnorm1_ref,
    moe_ref,
    heads_ref,
    line_first_ref,
    line_second_ref,
    query_ref,
    key_ref,
    value_ref,
    cosine_ref,
    sine_ref,
    attention_gain_ref,
    routing_gain_ref,
    query_gain_ref,
    key_gain_ref,
    query_weight_from,
    key_weight_from,
    value_weight_from,
    output_weight_from,
    router_weight_from,
    mixed_ref,
    tokens_grad_ref,
    output_grad_ref,
    query_grad_ref,
    key_grad_ref,
    value_grad_ref,
    small_out_ref,
    cotangent_ref,
    tokens_ref,
    query_weight_ref,
    key_weight_ref,
    value_weight_ref,
    output_weight_ref,
    router_weight_ref,
    packed_grad_ref,
    hidden_grad_ref,
    hidden_low_ref,
    hidden_all,
    hidden_line,
    line_heads,
    heads_grad,
    packed,
    packed_in,
    xnorm_in,
    weight_out,
    weight_in,
    output_out,
    output_in,
    key_sum,
    value_sum,
    back_part,
    back_in,
    moe,
    small,
    small_in,
    small_side,
    small_line,
    core_in,
    diag_in,
    side_in,
    line_in,
    local_sems,
    send_sems,
    recv_sems,
    scatter_send,
    scatter_recv,
):
    p = Place()
    group, width = xnorm1_ref.shape
    units = query_ref.shape[1]
    size = cosine_ref.shape[1]
    count = units // size
    packed_width = packed.shape[1]
    share = width // (2 * DEPTH)
    length = length_ref[0]
    mine = pl.ds(pl.multiple_of(p.t * rows, rows), rows)
    pairs = [
        (cotangent_from.at[mine], cotangent_ref),
        (moe_ref, moe),
        (output_weight_from, output_weight_ref),
        (tokens_from.at[mine], tokens_ref),
        (query_weight_from, query_weight_ref),
        (key_weight_from, key_weight_ref),
        (value_weight_from, value_weight_ref),
    ]
    for i in range(1, DEPTH):
        z = p.near(i)
        pairs += [
            (line_first_ref.at[z], line_heads.at[z, :, : units // 2]),
            (line_second_ref.at[z], line_heads.at[z, :, units // 2 :]),
        ]
    fetch = [
        pltpu.make_async_copy(src, dst, local_sems.at[i]) for i, (src, dst) in enumerate(pairs)
    ]
    for copy in fetch:
        copy.start()
    enter(p.peers())
    copies = Copies(send_sems, recv_sems)
    scatter_copies = Copies(scatter_send, scatter_recv)
    sums = Scatter(
        p,
        scatter_copies,
        rows,
        moe,
        core_in,
        diag_in,
        side_in,
        line_in,
        [3, 2, 1, 0],
        LineSum,
    )
    xn, yn, cn = p.at(x=1 - p.x), p.at(y=1 - p.y), p.at(c=1 - p.c)
    order = [p.near(k) for k in reversed(range(DEPTH))]
    along = [p.at(z=z) for z in order[: DEPTH - 1]]

    def columns(z, y):
        return pl.ds(pl.multiple_of((z * 2 + y) * share, share), share)

    def block(ref, t):
        return ref.at[pl.ds(pl.multiple_of(t * rows, rows), rows)]

    hidden_spread = Spread(p, copies, lambda t: block(hidden_all, t))
    line_spread = Spread(p, copies, lambda t: hidden_line.at[t])
    hidden_to = copies.along(
        [
            (
                z,
                hidden_low_ref.at[:, pl.ds(pl.multiple_of(z * 2 * share, share), 2 * share)],
                hidden_line.at[p.t, p.z],
            )
            for z in order[: DEPTH - 1]
        ],
        along,
        p.z,
    )
    xnorm_to = [
        copies.make(xnorm1_ref.at[:, columns(z, 1 - p.y)], xnorm_in.at[z], yn) for z in range(DEPTH)
    ]
    cut = units // PIECES
    cuts = [(i * cut, (i + 1) * cut) for i in range(PIECES - 1)]
    cuts.append((cuts[-1][1], packed_width))
    packed_to = [copies.make(packed.at[:, a:b], packed_in.at[:, a:b], yn) for a, b in cuts]
    weight_sums = [
        LineSum(
            p,
            copies,
            {k: weight_out.at[k - 1, :, a:b] for k in range(1, DEPTH)},
            weight_in.at[:, :, a:b],
        )
        for a, b in cuts
    ]
    output_to = copies.make(output_out, output_in, yn)
    fold = Fold(p, copies, rows, back_part, back_in)
    tokens_spread = Spread(p, copies, lambda t: block(tokens_grad_ref, t))
    mixed_spread = Spread(p, copies, lambda t: block(mixed_ref, t))
    small_to_c = copies.make(small, small_in.at[0], cn)
    small_to_x = copies.make(small, small_in.at[1], xn)
    small_to_y = copies.make(small_side.at[0], small_side.at[1], yn)
    small_to = copies.along(
        [(z, small_side.at[2, z], small_line.at[p.z]) for z in order[: DEPTH - 1]], along, p.z
    )

    widen(router_weight_ref, router_weight_from)
    lanes = router_weight_ref.shape[0]
    gain_row = experts + 2
    route_grad = summed_ref[:, width:]
    router = router_ref[:, :lanes]
    route_weight = router_ref[:, lanes : 2 * lanes]
    named = router_ref[:, 2 * lanes :]
    chosen_total = jnp.sum(router * named, axis=1, keepdims=True)
    inner_total = jnp.sum(route_grad * route_weight, axis=1, keepdims=True)
    prob_grad = named * (route_grad - inner_total) / chosen_total
    logit_low = (router * (prob_grad - jnp.sum(router * prob_grad, axis=1, keepdims=True))).astype(
        LOW
    )
    small[...] = jnp.zeros_like(small)
    small[:experts, :] = dot(logit_low, own_ref[:, :width], 0, 0)[:experts]
    fetch[1].wait()
    for k in range(DEPTH):
        sums.start(k)
    fetch[0].wait()
    xnorm2_grad = summed_ref[:, :width] + dot(logit_low, router_weight_ref[...], 1, 0)
    normed2, scale2 = normed_rows(hidden_ref[...])
    small[experts : experts + 1, :] = jnp.sum(xnorm2_grad * normed2, axis=0, keepdims=True)
    inner2 = xnorm2_grad * routing_gain_ref[...]
    hidden_grad_ref[...] = cotangent_ref[...].astype(F32) + scale2 * (
        inner2 - normed2 * jnp.mean(inner2 * normed2, axis=-1, keepdims=True)
    )
    hidden_low_ref[...] = hidden_grad_ref[...].astype(LOW)
    block(hidden_all, p.t)[...] = hidden_low_ref[...]
    hidden_line[p.t, p.z] = hidden_low_ref[
        :, pl.ds(pl.multiple_of(p.z * 2 * share, share), 2 * share)
    ]
    for there, _ in hidden_to:
        there.start()
    hidden_spread.start()
    for copy in xnorm_to:
        copy.start()
    key_sum[...] = jnp.zeros_like(key_sum)
    value_sum[...] = jnp.zeros_like(value_sum)
    sums.corner(0)
    hidden_spread.forward()
    sums.corner(1)
    sums.corner(2)
    hidden_spread.finish()

    valid = lax.broadcasted_iota(jnp.int32, (group, 1), 0) < length
    allowed = allowed_keys(group, length)
    fetch[2].wait()
    heads_grad[...] = jnp.where(
        valid, dot(hidden_all[...], output_weight_ref[...], 1, 0), 0.0
    ).astype(LOW)
    cosine, sine = cosine_ref[...], sine_ref[...]
    query_gain, key_gain = query_gain_ref[...], key_gain_ref[...]
    factor = size ** (-0.5)
    key_hat, key_scale = normed_rows(key_ref[...])
    key_gained = key_hat * key_gain
    key_low = (key_gained * cosine + turned(key_gained) * sine).astype(LOW)

    def norm_back(grad, hat, scale, gain):
        grad = grad * cosine - turned(grad) * sine
        gain_part = jnp.sum(grad * hat, axis=0, keepdims=True)
        inner = grad * gain
        return scale * (inner - hat * jnp.mean(inner * hat, axis=-1, keepdims=True)), gain_part

    def one_head(h):
        at = pl.ds(pl.multiple_of(h * size, size), size)
        hat, scale = normed_rows(query_ref[:, at])
        gained = hat * query_gain
        query_low = (gained * cosine + turned(gained) * sine).astype(LOW)
        probs = attention_probs(query_low, key_low, allowed)
        grad = heads_grad[:, at]
        probs_grad = dot(grad, value_ref[...], 1, 1)
        delta = jnp.sum(probs * probs_grad, axis=-1, keepdims=True)
        score_grad = (probs * (probs_grad - delta)).astype(LOW)
        key_sum[...] += dot(score_grad, query_low, 0, 0)
        value_sum[...] += dot(probs.astype(LOW), grad, 0, 0)
        back, gain_part = norm_back(
            dot(score_grad, key_low, 1, 0) * factor, hat, scale, query_gain
        )
        packed[:, at] = back.astype(LOW)
        small[gain_row : gain_row + 1, :size] += gain_part

    def heads_piece(i):
        pl.loop(i * count // PIECES, (i + 1) * count // PIECES)(one_head)

    def weight_piece(i):
        a, b = cuts[i]
        packed_to[i].wait_recv()
        for k in reversed(range(DEPTH)):
            z = p.near(k)
            grad = dot(xnorm1_ref[:, columns(z, p.y)], packed[:, a:b], 0, 0) + dot(
                xnorm_in[z], packed_in[:, a:b], 0, 0
            )
            if k:
                weight_out[k - 1, :, a:b] = grad.astype(LOW)
                weight_sums[i].send(k)
            else:
                packed_grad_ref[:, a:b] = grad

    heads_piece(0)
    packed_to[0].start()
    sums.corner(3)
    heads_piece(1)
    packed_to[1].start()
    for copy in xnorm_to:
        copy.wait_recv()
    weight_piece(0)
    sums.side(0)
    for _, back in hidden_to:
        back.wait_recv()
    line_spread.start()
    heads_piece(2)
    packed_to[2].start()
    weight_piece(1)
    weight_sums[0].relay()
    sums.side(1)
    heads_piece(3)
    key_back, key_part = norm_back(key_sum[...] * factor, key_hat, key_scale, key_gain)
    packed[:, units : units + size] = key_back.astype(LOW)
    packed[:, units + size :] = value_sum[...].astype(LOW)
    packed_to[3].start()
    small[gain_row + 1 : gain_row + 2, :size] = key_part
    for row in (gain_row, gain_row + 1):
        part = small[row : row + 1, :size]
        for i in range(1, width // size):
            small[row : row + 1, i * size : (i + 1) * size] = part
    line_spread.forward()
    weight_piece(2)
    weight_sums[1].relay()
    for copy in fetch[3:7]:
        copy.wait()
    back_part[...] = (
        dot(packed[:, :units], query_weight_ref[...], 1, 1)
        + dot(packed[:, units : units + size], key_weight_ref[...], 1, 1)
        + dot(packed[:, units + size :], value_weight_ref[...], 1, 1)
    ).astype(LOW)
    fold.start()
    weight_piece(3)
    fold.forward()
    weight_sums[2].relay()
    sums.side(2)
    sums.side(3)
    sums.close(0)

    xnorm1_grad = fold.finish()
    normed1, scale1 = normed_rows(tokens_ref[...].astype(F32))
    small[gain_row - 1 : gain_row, :] = jnp.sum(xnorm1_grad * normed1, axis=0, keepdims=True)
    small_to_c.start()
    inner = xnorm1_grad * attention_gain_ref[...]
    block(tokens_grad_ref, p.t)[...] = (
        hidden_grad_ref[...]
        + scale1 * (inner - normed1 * jnp.mean(inner * normed1, axis=-1, keepdims=True))
    ).astype(LOW)
    tokens_spread.start()

    line_spread.finish()
    for copy in fetch[7:]:
        copy.wait()

    def output_piece(y):
        at = pl.ds(pl.multiple_of(y * share, share), share)
        grad = dot(hidden_line[:, p.z, :, at].reshape(group, share), heads_ref[...], 0, 0)
        for k in range(1, DEPTH):
            z = p.near(k)
            grad += dot(hidden_line[:, z, :, at].reshape(group, share), line_heads[z], 0, 0)
        return grad

    output_out[...] = output_piece(1 - p.y).astype(LOW)
    output_to.start()
    output_grad_ref[...] = output_piece(p.y)
    weight_sums[3].relay()
    sums.close(1)
    small_to_c.wait_recv()
    small_to_c.wait_send()
    small[...] += small_in[0]
    small_to_x.start()
    tokens_spread.forward()
    sums.close(2)
    sums.close(3)
    sums.relay(0)
    small_to_x.wait_recv()
    small_to_x.wait_send()
    small[...] += small_in[1]
    for z in range(DEPTH):
        small_side[0, z] = small[:, columns(z, 1 - p.y)]
        small_side[2, z] = small[:, columns(z, p.y)]
    small_to_y.start()
    output_to.wait_recv()
    output_grad_ref[...] += output_in[...].astype(F32)
    small_to_y.wait_recv()
    small_side[2] += small_side[1]
    for there, _ in small_to:
        there.start()
    tokens_spread.finish()
    block(mixed_ref, p.t)[...] = (hidden_ref[...] + sums.finish()).astype(LOW)
    mixed_spread.start()
    small_total = small_side[2, p.z]
    for (_, back), z in zip(small_to, order):
        back.wait_recv()
        small_total += small_line[z]
    small_out_ref[...] = small_total
    mixed_spread.forward()
    mixed_spread.finish()
    for i, (a, b) in enumerate(cuts):
        grad = packed_grad_ref[:, a:b]
        for term in weight_sums[i].wait():
            grad += term[...].astype(F32)
        query_grad_ref[:, a : min(b, units)] = grad[:, : min(b, units) - a]
    key_grad_ref[...] = grad[:, -2 * size : -size]
    value_grad_ref[...] = grad[:, -size:]
    for copy in copies.made:
        if copy is not small_to_c and copy is not small_to_x:
            copy.wait_send()
    scatter_copies.finish()


def run_tail(
    length,
    summed,
    own,
    router,
    hidden,
    cotangent,
    tokens,
    xnorm1,
    moe,
    heads,
    line_first,
    line_second,
    query,
    key,
    value,
    cosine,
    sine,
    attention_gain,
    routing_gain,
    query_gain,
    key_gain,
    query_weight,
    key_weight,
    value_weight,
    output_weight,
    router_weight,
    experts,
    collective_id,
):
    group, width = xnorm1.shape
    rows = hidden.shape[0]
    units, size = query.shape[1], cosine.shape[1]
    packed_width = units + 2 * size
    share = width // (2 * DEPTH)
    tensors = group // rows
    smalls = (experts + 4 + 7) // 8 * 8
    vmem = pltpu.VMEM
    return pl.pallas_call(
        functools.partial(tail_kernel, rows, experts),
        out_shape=(
            jax.ShapeDtypeStruct((group, width), LOW),
            jax.ShapeDtypeStruct((group, width), LOW),
            jax.ShapeDtypeStruct((share, units), F32),
            jax.ShapeDtypeStruct((share, units), F32),
            jax.ShapeDtypeStruct((share, size), F32),
            jax.ShapeDtypeStruct((share, size), F32),
            jax.ShapeDtypeStruct((smalls, share), F32),
        ),
        in_specs=[pl.BlockSpec(memory_space=pltpu.SMEM)]
        + [VMEM_SPEC] * 4
        + [ANY_SPEC, ANY_SPEC, VMEM_SPEC]
        + [ANY_SPEC, VMEM_SPEC, ANY_SPEC, ANY_SPEC]
        + [VMEM_SPEC] * 9
        + [ANY_SPEC] * 4
        + [VMEM_SPEC],
        out_specs=[VMEM_SPEC] * 7,
        scratch_shapes=[
            vmem((rows, width), LOW),
            vmem((rows, width), LOW),
            vmem(query_weight.shape, LOW),
            vmem(key_weight.shape, LOW),
            vmem(value_weight.shape, LOW),
            vmem(output_weight.shape, LOW),
            vmem((LANES, width), LOW),
            vmem((share, packed_width), F32),
            vmem((rows, width), F32),
            vmem((rows, width), LOW),
            vmem((group, width), LOW),
            vmem((tensors, DEPTH, rows, 2 * share), LOW),
            vmem((DEPTH, group, units), LOW),
            vmem((group, units), LOW),
            vmem((group, packed_width), LOW),
            vmem((group, packed_width), LOW),
            vmem((DEPTH, group, share), LOW),
            vmem((DEPTH - 1, share, packed_width), LOW),
            vmem((DEPTH, share, packed_width), LOW),
            vmem((share, units), LOW),
            vmem((share, units), LOW),
            vmem((group, size), F32),
            vmem((group, size), F32),
            vmem((group, width), LOW),
            vmem((3, rows, width), LOW),
            vmem(moe.shape, LOW),
            vmem((smalls, width), F32),
            vmem((2, smalls, width), F32),
            vmem((3, DEPTH, smalls, share), F32),
            vmem((DEPTH, smalls, share), F32),
        ]
        + scatter_scratch(rows, width)
        + semaphores(7 + 2 * (DEPTH - 1), TAIL_SEMS, TAIL_SEMS, SCATTER_SEMS, SCATTER_SEMS),
        compiler_params=pltpu.CompilerParams(
            collective_id=collective_id, has_side_effects=True, vmem_limit_bytes=64000000
        ),
        name="tail",
    )(
        length,
        summed,
        own,
        router,
        hidden,
        cotangent,
        tokens,
        xnorm1,
        moe,
        heads,
        line_first,
        line_second,
        query,
        key,
        value,
        cosine,
        sine,
        attention_gain,
        routing_gain,
        query_gain,
        key_gain,
        query_weight,
        key_weight,
        value_weight,
        output_weight,
        router_weight,
    )


def gathered_shards(
    tokens,
    seq_length,
    expert_routes,
    attention_gain,
    query_weight,
    key_weight,
    value_weight,
    query_gain,
    key_gain,
    output_weight,
    routing_gain,
    router_weight,
    gate_weight,
    up_weight,
    down_weight,
    cotangent,
):
    count, width = tokens.shape
    head_size = query_gain.shape[0]
    experts = router_weight.shape[1]
    owned = gate_weight.shape[0]
    part = lax.axis_index("tensor")
    owner = lax.axis_index("expert")
    rows = count // lax.axis_size("tensor")

    def own_rows(values):
        return lax.dynamic_slice_in_dim(values, part * rows, rows, 0)

    cosine, sine = rope_tables(count, head_size)
    half = head_size // 2
    sine = jnp.concatenate([-sine[:, :half], sine[:, half:]], axis=1)
    upstream_all, xnorm1, query, key, value, heads, line_first, hidden, own, router = run_front(
        seq_length,
        tokens,
        cotangent,
        own_rows(expert_routes),
        attention_gain[None],
        query_gain[None],
        key_gain[None],
        routing_gain[None],
        cosine,
        sine,
        query_weight,
        key_weight,
        value_weight,
        output_weight,
        router_weight.T,
        experts,
        0,
    )

    def by_unit(weight):
        return weight.transpose(0, 2, 1).reshape(-1, width)

    def from_units(grad):
        return grad.reshape(owned, -1, width).transpose(0, 2, 1)

    summed, moe_part, line_second, gate_grad, up_grad, down_grad = run_experts(
        own,
        upstream_all,
        by_unit(gate_weight),
        by_unit(up_weight),
        down_weight.reshape(-1, width),
        heads,
        owned,
        experts,
        width,
        1,
    )
    mixed, tokens_grad, output_grad, query_grad, key_grad, value_grad, small_sum = run_tail(
        seq_length,
        summed,
        own,
        router,
        hidden,
        cotangent,
        tokens,
        xnorm1,
        moe_part,
        heads,
        line_first,
        line_second,
        query,
        key,
        value,
        cosine,
        sine,
        attention_gain[None],
        routing_gain[None],
        query_gain[None],
        key_gain[None],
        query_weight,
        key_weight,
        value_weight,
        output_weight,
        router_weight.T,
        experts,
        2,
    )
    share = head_size // lax.axis_size("expert")

    def own_gain(row):
        return lax.dynamic_slice_in_dim(small_sum[row], owner * share, share, 0)

    return (
        mixed,
        tokens_grad,
        small_sum[experts + 1],
        query_grad,
        key_grad,
        value_grad,
        own_gain(experts + 2),
        own_gain(experts + 3),
        output_grad,
        small_sum[experts],
        small_sum[:experts].T,
        from_units(gate_grad),
        from_units(up_grad),
        down_grad.reshape(down_weight.shape),
    )


def solution(mesh):
    sizes = dict(mesh.shape)
    fits = sizes["expert"] == 2 * DEPTH and sizes["tensor"] == 4
    return jax.shard_map(
        gathered_shards if fits else routed_shards,
        mesh=mesh,
        in_specs=(
            P("expert", None),
            P("expert"),
            P("expert", None),
            P(),
            P(None, "tensor"),
            P(None, "tensor"),
            P(None, "tensor"),
            P(),
            P(),
            P(None, "tensor"),
            P(),
            P(),
            P("expert", None, "tensor"),
            P("expert", None, "tensor"),
            P("expert", "tensor", None),
            P("expert", None),
        ),
        out_specs=(
            P("expert", None),
            P("expert", None),
            P("expert"),
            P("expert", "tensor"),
            P("expert", "tensor"),
            P("expert", "tensor"),
            P("expert"),
            P("expert"),
            P("expert", "tensor"),
            P("expert"),
            P("expert", None),
            P("expert", None, "tensor"),
            P("expert", None, "tensor"),
            P("expert", "tensor", None),
        ),
        check_vma=False,
    )
```
